32 devices in a mesh: shard: 4 (over y, x), seq: 8 (over z, core).
Axes of the slice: x: 2, y: 2, z: 4, core: 2. Of those that a mesh axis runs over, the one named last changes fastest.
Arguments:
- inputs: bfloat16 [4, 1024, 2048], P('shard', 'seq'), may hold values from -6 to 6
- attn_gain: bfloat16 [2048], P(('shard', 'seq')), may hold values from 0.25 to 1.75
- query_project_weight: bfloat16 [2048, 3072], P('shard', 'seq'), may hold values from -0.25 to 0.25
- latent_project_weight: bfloat16 [2048, 576], P(('shard', 'seq')), may hold values from -0.125 to 0.125
- latent_gain: bfloat16 [512], P(('shard', 'seq')), may hold values from 0.25 to 1.75
- latent_keyval_weight: bfloat16 [512, 4096], P('shard', 'seq'), may hold values from -0.25 to 0.25
- attention_output_weight: bfloat16 [2048, 2048], P('seq', 'shard'), may hold values from -0.5 to 0.5
- ffn_gain: bfloat16 [2048], P(('shard', 'seq')), may hold values from 0.25 to 1.75
- shared_gate: bfloat16 [2048, 2816], P('shard', 'seq'), may hold values from -0.125 to 0.125
- shared_up: bfloat16 [2048, 2816], P('shard', 'seq'), may hold values from -0.125 to 0.125
- shared_down: bfloat16 [2816, 2048], P('seq', 'shard'), may hold values from -0.109375 to 0.109375
- expert_gate: bfloat16 [8, 2048, 1408], P('seq', 'shard'), may hold values from -0.125 to 0.125
- expert_up: bfloat16 [8, 2048, 1408], P('seq', 'shard'), may hold values from -0.125 to 0.125
- expert_down: bfloat16 [8, 1408, 2048], P('seq', None, 'shard'), may hold values from -0.15625 to 0.15625
- routes: int32 [4, 1024, 6], P('shard', 'seq'), may hold values from 0 to 7, as said below
- slots: int32 [4, 1024, 6], P('shard', 'seq'), may hold values from 0 to 108, as said below
- gates: bfloat16 [4, 1024, 6], P('shard', 'seq'), may hold values from 0.099609375 to 0.5
- cotangent: bfloat16 [4, 1024, 2048], P('shard', 'seq'), may hold values from -6 to 6
Outputs:
- output: bfloat16 [4, 1024, 2048], P('shard', 'seq')
- input_grad: float32 [4, 1024, 2048], P('shard', 'seq')
- attn_gain_grad: float32 [2048], P(('shard', 'seq'))
- query_grad: float32 [2048, 3072], P('shard', 'seq')
- latent_grad: float32 [2048, 576], P(('shard', 'seq'))
- latent_gain_grad: float32 [512], P(('shard', 'seq'))
- kvup_grad: float32 [512, 4096], P('shard', 'seq')
- out_grad: float32 [2048, 2048], P('seq', 'shard')
- ffn_gain_grad: float32 [2048], P(('shard', 'seq'))
- shared_gate_grad: float32 [2048, 2816], P('shard', 'seq')
- shared_up_grad: float32 [2048, 2816], P('shard', 'seq')
- shared_down_grad: float32 [2816, 2048], P('seq', 'shard')
- expert_gate_grad: float32 [8, 2048, 1408], P('seq', 'shard')
- expert_up_grad: float32 [8, 2048, 1408], P('seq', 'shard')
- expert_down_grad: float32 [8, 1408, 2048], P('seq', None, 'shard')
The draws below stay inside these ranges and needn't reach their ends.
Inputs may be any that keep to these rules, and one draw needn't show every extreme that they name: `routes`: each token names 6 different experts. In each device's block of 128 tokens one expert is named by more than 108 tokens. `slots`: within each device's block of 128 tokens, the routes to one expert carry the numbers 0, 1, 2 and so on, each once, in an order drawn from the seed, except that every number from 108 on is written as 108; such routes are dropped.
All inputs are finite; a program needn't handle non-finite values.
Results may differ from the reference program's by a relative error of at most 0.025.
Values may be sent and summed in bfloat16 or wider, within the bound.
A program may use at most 256 MiB of HBM per device.

```python
import jax
import jax.numpy as jnp
from jax import lax

D = 2048
HEADS = 16
NOPE = 128
ROPE = 64
VDIM = 128
RANK = 512
FF = 1408
SHARED_FF = 2816
TOPK = 6
TOK_DEV = 128
EXPERTS = 8
SEQS = 4
LEN = 1024
CAP = 108


def route_plan(key):
    blocks = SEQS * LEN // TOK_DEV
    base = jax.random.fold_in(key, 1201)
    key_popular, key_noise, key_hot, key_order = jax.random.split(base, 4)
    popular = jax.random.randint(key_popular, (EXPERTS,), 0, 3) * 262144
    noise = jax.random.randint(key_noise, (blocks, TOK_DEV, EXPERTS), 0, 1048576)
    hottest = jax.random.randint(key_hot, (blocks,), 0, EXPERTS)
    forced = (jnp.arange(TOK_DEV)[None, :, None] <= CAP) & (jnp.arange(EXPERTS)[None, None, :] == hottest[:, None, None])
    scores = (noise + popular[None, None, :] + forced.astype(jnp.int32) * 4194304) * EXPERTS + jnp.arange(EXPERTS)[None, None, :]
    unused, chosen = lax.top_k(scores, TOPK)
    chosen = chosen.astype(jnp.int32)
    count = TOK_DEV * TOPK
    priority = jax.random.randint(key_order, (blocks, count), 0, 65536) * count + jnp.arange(count)[None, :]
    flat = chosen.reshape(blocks, count)
    same = flat[:, :, None] == flat[:, None, :]
    before = priority[:, None, :] < priority[:, :, None]
    ranking = jnp.sum((same & before).astype(jnp.int32), 2)
    placed = jnp.minimum(ranking, CAP).astype(jnp.int32)
    return (chosen.reshape(SEQS, LEN, TOPK), placed.reshape(SEQS, LEN, TOPK))


def draw_routes(key, part):
    return route_plan(key)[0]


def draw_slots(key, part):
    return route_plan(key)[1]


def levels(stream_key, dims, cuts, low, top_value):
    def one(dim, blocks):
        steps = jax.random.uniform(jax.random.fold_in(jax.random.fold_in(stream_key, 6), dim), (blocks,), jnp.float32, low / len(cuts), top_value / len(cuts))
        return jnp.repeat(jnp.exp(steps), dims[dim] // blocks).reshape((-1,) + (1,) * (len(dims) - dim - 1))

    level = one(*cuts[0])
    for cut in cuts[1:]:
        level = level * one(*cut)
    return level


def centred(stream_key, dims, scale, limit, pieces=(), kind=jnp.bfloat16):
    values = jax.random.normal(stream_key, dims, jnp.float32) * scale
    if len(pieces) > 0:
        values = levels(stream_key, dims, pieces, -0.22, 0.18) * values
    return jnp.clip(values, min=-limit, max=limit).astype(kind)


def setup_inputs(seed: int = 0) -> dict:
    streams_of = jax.random.split(jax.random.key(seed), 19)
    inputs = centred(streams_of[0], (SEQS, LEN, D), 1.0, 6.0, ((0, 4), (1, 8)))
    attn_gain = jnp.clip(1.0 + 0.15 * jax.random.normal(streams_of[1], (D,), jnp.float32), 0.25, 1.75).astype(jnp.bfloat16)
    query_project_weight = centred(streams_of[2], (D, HEADS * (NOPE + ROPE)), (D // 4) ** -0.5, 0.25, ((0, 4), (1, 8)))
    latent_project_weight = centred(streams_of[3], (D, RANK + ROPE), D ** -0.5, 0.125, ((0, 32),))
    latent_gain = jnp.clip(1.0 + 0.15 * jax.random.normal(streams_of[4], (RANK,), jnp.float32), 0.25, 1.75).astype(jnp.bfloat16)
    latent_keyval_weight = centred(streams_of[5], (RANK, HEADS * (NOPE + VDIM)), RANK ** -0.5, 0.25, ((0, 4), (1, 8)))
    attention_output_weight = centred(streams_of[6], (HEADS * VDIM, D), (HEADS * VDIM // 16) ** -0.5, 0.5, ((0, 8), (1, 4)))
    ffn_gain = jnp.clip(1.0 + 0.15 * jax.random.normal(streams_of[7], (D,), jnp.float32), 0.25, 1.75).astype(jnp.bfloat16)
    shared_gate = centred(streams_of[8], (D, SHARED_FF), D ** -0.5, 0.125, ((0, 4), (1, 8)))
    shared_up = centred(streams_of[9], (D, SHARED_FF), D ** -0.5, 0.125, ((0, 4), (1, 8)))
    shared_down = centred(streams_of[10], (SHARED_FF, D), SHARED_FF ** -0.5, 0.109375, ((0, 8), (1, 4)))
    expert_gate = centred(streams_of[11], (EXPERTS, D, FF), D ** -0.5, 0.125, ((0, 8), (1, 4)))
    expert_up = centred(streams_of[12], (EXPERTS, D, FF), D ** -0.5, 0.125, ((0, 8), (1, 4)))
    expert_down = centred(streams_of[13], (EXPERTS, FF, D), FF ** -0.5, 0.15625, ((0, 8), (2, 4)))
    routes = draw_routes(jax.random.fold_in(streams_of[18], 71), 0)
    slots = draw_slots(jax.random.fold_in(streams_of[18], 71), 0)
    gates = jnp.clip(0.099609375 + 0.40039062 * jax.random.uniform(streams_of[16], (SEQS, LEN, TOPK), jnp.float32) ** levels(streams_of[16], (SEQS, LEN, TOPK), ((0, 4), (1, 8)), -0.2, 0.2), 0.099609375, 0.5).astype(jnp.bfloat16)
    cotangent = centred(streams_of[17], (SEQS, LEN, D), 1.0, 6.0, ((0, 4), (1, 8)))
    return {"inputs": inputs, "attn_gain": attn_gain, "query_project_weight": query_project_weight, "latent_project_weight": latent_project_weight, "latent_gain": latent_gain, "latent_keyval_weight": latent_keyval_weight, "attention_output_weight": attention_output_weight, "ffn_gain": ffn_gain, "shared_gate": shared_gate, "shared_up": shared_up, "shared_down": shared_down, "expert_gate": expert_gate, "expert_up": expert_up, "expert_down": expert_down, "routes": routes, "slots": slots, "gates": gates, "cotangent": cotangent}


EPSILON = 1e-06
THETA = 10000.0
MASKED = -1e+30

@jax.custom_vjp
def low(v):
    return lax.optimization_barrier(v.astype(jnp.bfloat16)).astype(jnp.float32)

@jax.custom_vjp
def low_back(v):
    return v

def low_keep(v):
    return (low(v), None)

def low_pass(kept, grad):
    return (grad,)

def back_keep(v):
    return (v, None)

def back_low(kept, grad):
    return (low(grad),)
low.defvjp(low_keep, low_pass)
low_back.defvjp(back_keep, back_low)

def matmul_high(left, right):
    return jnp.matmul(left, right, precision=lax.Precision.HIGHEST)

def rms_norm(values, scaling):
    return values * lax.rsqrt(lax.optimization_barrier(jnp.mean(values * values, -1, keepdims=True)) + EPSILON) * scaling

def rope_tables(positions, depth):
    half_depth = depth // 2
    frequency = THETA ** (-(2.0 * jnp.arange(half_depth, dtype=jnp.float32)) / depth)
    angles = positions.astype(jnp.float32)[:, None] * frequency[None, :]
    return (jnp.cos(angles), jnp.sin(angles))

def rotate(values, cosine, sine):
    half_depth = values.shape[-1] // 2
    first = values[..., :half_depth]
    second = values[..., half_depth:]
    return jnp.concatenate([first * cosine - second * sine, second * cosine + first * sine], -1)

def attend(parts):
    queries, keys, values = parts
    length = queries.shape[0]
    scores = jnp.einsum('qhd,khd->hqk', queries, keys, precision=lax.Precision.HIGHEST)
    scores = low_back(scores * (NOPE + ROPE) ** (-0.5))
    seen = jnp.arange(length)[None, :] <= jnp.arange(length)[:, None]
    scores = jnp.where(seen[None], scores, MASKED)
    top = lax.optimization_barrier(jnp.max(scores, -1, keepdims=True))
    expo = jnp.exp(scores - top)
    weights = expo / lax.optimization_barrier(jnp.sum(expo, -1, keepdims=True))
    return jnp.einsum('hqk,khd->qhd', low(weights), values, precision=lax.Precision.HIGHEST)

def expert_feedforward(parts):
    tokens, w_gate, w_up, w_down = parts
    gate_pre = low_back(matmul_high(tokens, w_gate))
    up_pre = low_back(matmul_high(tokens, w_up))
    hidden = low(jax.nn.silu(gate_pre) * up_pre)
    return low(low_back(matmul_high(hidden, w_down)))

def layer_forward(residual_stream, first_norm_weight, query_project_weight, latent_project_weight, latent_norm_weight, latent_keyval_weight, attention_output_weight, second_norm_weight, shared_gate_weight, shared_up_weight, shared_down_weight, expert_gate_weight, expert_up_weight, expert_down_weight, routes, slots, gates):
    seqs = residual_stream.shape[0]
    length = residual_stream.shape[1]
    model_width = residual_stream.shape[2]
    first = low(rms_norm(residual_stream, first_norm_weight))
    cosine, sine = rope_tables(jnp.arange(length), ROPE)
    query = low_back(matmul_high(first, query_project_weight)).reshape(seqs, length, HEADS, NOPE + ROPE)
    query = low(jnp.concatenate([query[..., :NOPE], rotate(query[..., NOPE:], cosine[:, None], sine[:, None])], -1))
    latent = low_back(matmul_high(first, latent_project_weight))
    compressed = low(rms_norm(latent[..., :RANK], latent_norm_weight))
    key_rope = low(rotate(latent[..., RANK:], cosine, sine))
    keyval = low(low_back(matmul_high(compressed, latent_keyval_weight))).reshape(seqs, length, HEADS, NOPE + VDIM)
    key_heads = low_back(jnp.broadcast_to(key_rope[:, :, None, :], (seqs, length, HEADS, ROPE)))
    keys = jnp.concatenate([keyval[..., :NOPE], key_heads], -1)
    values = keyval[..., NOPE:]
    attended = lax.map(jax.checkpoint(attend), (query, keys, values))
    attended = low(low_back(attended)).reshape(seqs, length, HEADS * VDIM)
    middle = residual_stream + low_back(matmul_high(attended, attention_output_weight))
    second = low(rms_norm(middle, second_norm_weight))
    shared_gate = low_back(matmul_high(second, shared_gate_weight))
    shared_up = low_back(matmul_high(second, shared_up_weight))
    shared_out = low_back(matmul_high(low(jax.nn.silu(shared_gate) * shared_up), shared_down_weight))
    blocks = seqs * length // TOK_DEV
    tokens = second.reshape(blocks, TOK_DEV, model_width)
    slot_ids = jnp.where(slots < CAP, routes * CAP + slots, -1).reshape(blocks, TOK_DEV, TOPK)
    columns = jnp.arange(EXPERTS * CAP)
    match = slot_ids[..., None] == columns[None, None, None, :]
    picks = lax.optimization_barrier(jnp.sum(match.astype(jnp.float32), 2))
    table = lax.optimization_barrier(jnp.sum(jnp.where(match, gates.reshape(blocks, TOK_DEV, TOPK)[..., None], 0.0), 2))
    buffer = low_back(jnp.einsum('btj,btd->bjd', picks, tokens, precision=lax.Precision.HIGHEST))
    rows_by_expert = buffer.reshape(blocks, EXPERTS, CAP, model_width).transpose(1, 0, 2, 3).reshape(EXPERTS, blocks * CAP, model_width)
    expert_result_rows = lax.map(jax.checkpoint(expert_feedforward), (rows_by_expert, expert_gate_weight, expert_up_weight, expert_down_weight))
    returned = expert_result_rows.reshape(EXPERTS, blocks, CAP, model_width).transpose(1, 0, 2, 3).reshape(blocks, EXPERTS * CAP, model_width)
    routed = jnp.einsum('btj,bjd->btd', table, returned, precision=lax.Precision.HIGHEST)
    return middle + shared_out + routed.reshape(seqs, length, model_width)

def reference(inputs, attn_gain, query_project_weight, latent_project_weight, latent_gain, latent_keyval_weight, attention_output_weight, ffn_gain, shared_gate, shared_up, shared_down, expert_gate, expert_up, expert_down, routes, slots, gates, cotangent):
    gates_full = gates.astype(jnp.float32)

    def apply_layer(residual_stream, first_norm_weight, wq, wl, gain_lat, wkv, wo, second_norm_weight, wsg, wsu, wsd, weg, weu, wed):
        return layer_forward(residual_stream, first_norm_weight, wq, wl, gain_lat, wkv, wo, second_norm_weight, wsg, wsu, wsd, weg, weu, wed, routes, slots, gates_full)
    output, pullback = jax.vjp(apply_layer, inputs.astype(jnp.float32), attn_gain.astype(jnp.float32), query_project_weight.astype(jnp.float32), latent_project_weight.astype(jnp.float32), latent_gain.astype(jnp.float32), latent_keyval_weight.astype(jnp.float32), attention_output_weight.astype(jnp.float32), ffn_gain.astype(jnp.float32), shared_gate.astype(jnp.float32), shared_up.astype(jnp.float32), shared_down.astype(jnp.float32), expert_gate.astype(jnp.float32), expert_up.astype(jnp.float32), expert_down.astype(jnp.float32))
    grads = pullback(cotangent.astype(jnp.float32))
    return (output.astype(jnp.bfloat16), grads[0], grads[1], grads[2], grads[3], grads[4], grads[5], grads[6], grads[7], grads[8], grads[9], grads[10], grads[11], grads[12], grads[13])
```

```python
import jax
import jax.numpy as jnp
from jax import lax
from jax.sharding import PartitionSpec as P

HEADS = 16
NOPE = 128
ROPE = 64
VDIM = 128
RANK = 512
TOPK = 6
EXP_DEV = 1


EPSILON = 1e-06
THETA = 10000.0
MASKED = -1e30


def rope_tables(positions, depth):
    half_depth = depth // 2
    frequency = THETA ** (-(2.0 * jnp.arange(half_depth, dtype=jnp.float32)) / depth)
    angles = positions.astype(jnp.float32)[:, None] * frequency[None, :]
    return (jnp.cos(angles), jnp.sin(angles))


def rotate(values, cosine, sine):
    half_depth = values.shape[-1] // 2
    first = values[..., :half_depth]
    second = values[..., half_depth:]
    return jnp.concatenate([first * cosine - second * sine, second * cosine + first * sine], -1)


def norm_forward(values, scaling):
    inverse = lax.rsqrt(jnp.mean(values * values, -1, keepdims=True) + EPSILON)
    return (values * inverse * scaling, inverse)


def norm_backward(values, inverse, scaling, upstream):
    weighted = upstream * scaling
    scaling_grad = jnp.sum(upstream * values * inverse, 0)
    centre = jnp.mean(weighted * values, -1, keepdims=True)
    return (inverse * weighted - values * inverse**3 * centre, scaling_grad)


def swish_gradient(gate_pre, upper, upstream):
    sigma = jax.nn.sigmoid(gate_pre)
    return (
        upstream * upper * sigma * (1.0 + gate_pre * (1.0 - sigma)),
        upstream * gate_pre * sigma,
    )


def inner_rows(left, right):
    return lax.dot_general(
        left, right, (((0,), (0,)), ((), ())), preferred_element_type=jnp.float32
    )


def times_transposed(left, right):
    return lax.dot_general(
        left, right, (((1,), (1,)), ((), ())), preferred_element_type=jnp.float32
    )


def masked_scores(queries, keys, offset, score_scale):
    scores = (
        jnp.einsum("qhd,khd->hqk", queries, keys, preferred_element_type=jnp.float32) * score_scale
    )
    query_pos = offset + jnp.arange(queries.shape[0])
    seen = jnp.arange(keys.shape[0])[None, :] <= query_pos[:, None]
    return jnp.where(seen[None], scores, MASKED)


def gather_seq(block):
    return lax.all_gather(block, "seq", axis=0, tiled=True)


def scatter_seq(partial):
    return lax.psum_scatter(partial, "seq", scatter_dimension=0, tiled=True)


def rows_dot(left, right):
    return jnp.dot(left, right, preferred_element_type=jnp.float32)


def on_device(
    inputs,
    attn_gain,
    query_project_weight,
    latent_project_weight,
    latent_gain,
    latent_keyval_weight,
    attention_output_weight,
    ffn_gain,
    shared_gate,
    shared_up,
    shared_down,
    expert_gate,
    expert_up,
    expert_down,
    routes,
    slots,
    gates,
    cotangent,
):
    tok_rows = inputs.shape[1]
    model_width = inputs.shape[2]
    groups = lax.axis_size("seq")
    shards = lax.axis_size("shard")
    me = lax.axis_index("seq")
    local_heads = HEADS // groups
    query_width = NOPE + ROPE
    experts = EXP_DEV * groups
    capacity = 9 * tok_rows * TOPK // (8 * experts)
    length = tok_rows * groups
    score_scale = (NOPE + ROPE) ** (-0.5)
    block_rows = min(512, length)
    starts = jnp.arange(length // block_rows) * block_rows
    own_start = me * tok_rows

    def gather_shard(weight, axis):
        return lax.all_gather(weight, "shard", axis=axis, tiled=True)

    own_inputs = inputs.reshape(tok_rows, model_width)
    upstream = cotangent.reshape(tok_rows, model_width)
    route_rows = routes.reshape(tok_rows, TOPK)
    slot_rows = slots.reshape(tok_rows, TOPK)
    kept = (route_rows[:, :, None] == jnp.arange(experts)[None, None, :]) & (
        slot_rows < capacity
    )[:, :, None]
    gate_table = jnp.sum(
        jnp.where(kept, gates.reshape(tok_rows, TOPK).astype(jnp.float32)[:, :, None], 0.0), 1
    ).astype(jnp.bfloat16)

    gains = lax.all_gather(
        jnp.concatenate([attn_gain, latent_gain, ffn_gain]), ("shard", "seq"), axis=0, tiled=False
    ).astype(jnp.float32)
    one_width = attn_gain.shape[0]
    lat_width = latent_gain.shape[0]
    first_norm_weight = gains[:, :one_width].reshape(-1)
    latent_norm_weight = gains[:, one_width : one_width + lat_width].reshape(-1)
    second_norm_weight = gains[:, one_width + lat_width :].reshape(-1)
    full_latent = lax.all_gather(latent_project_weight, ("shard", "seq"), axis=0, tiled=True)

    inputs_all = gather_seq(own_inputs)
    full_query = gather_shard(query_project_weight, 0)
    full_kvup = gather_shard(latent_keyval_weight, 0)
    full_out = gather_shard(attention_output_weight, 1)
    upstream_all = gather_seq(upstream)
    table_all = gather_seq(gate_table)
    full_sgate = gather_shard(shared_gate, 0)
    full_sup = gather_shard(shared_up, 0)
    full_sdown = gather_shard(shared_down, 1)
    full_egate = gather_shard(expert_gate[0], 0)
    full_eup = gather_shard(expert_up[0], 0)
    full_edown = gather_shard(expert_down[0], 1)
    gate_column = lax.dynamic_slice_in_dim(table_all, me, 1, 1).astype(jnp.float32)

    residual_stream = own_inputs.astype(jnp.float32)
    first_all = norm_forward(inputs_all.astype(jnp.float32), first_norm_weight)[0].astype(
        jnp.bfloat16
    )
    cos_all, sin_all = rope_tables(jnp.arange(length), ROPE)
    latent = rows_dot(first_all, full_latent)
    latent_all = norm_forward(latent[:, :RANK], latent_norm_weight)[0].astype(jnp.bfloat16)
    rope_all = rotate(latent[:, RANK:], cos_all, sin_all).astype(jnp.bfloat16)
    head_query = rows_dot(first_all, full_query).reshape(length, local_heads, query_width)
    head_query = jnp.concatenate(
        [
            head_query[..., :NOPE],
            rotate(head_query[..., NOPE:], cos_all[:, None], sin_all[:, None]),
        ],
        -1,
    ).astype(jnp.bfloat16)
    keyval = (
        rows_dot(latent_all, full_kvup)
        .astype(jnp.bfloat16)
        .reshape(length, local_heads, NOPE + VDIM)
    )
    head_keys = jnp.concatenate(
        [keyval[..., :NOPE], jnp.broadcast_to(rope_all[:, None, :], (length, local_heads, ROPE))],
        -1,
    )
    head_values = keyval[..., NOPE:]

    def forward_block(offset):
        queries = lax.dynamic_slice_in_dim(head_query, offset, block_rows, 0)
        scores = masked_scores(queries, head_keys, offset, score_scale)
        top = jnp.max(scores, -1, keepdims=True)
        expo = jnp.exp(scores - top)
        total = jnp.sum(expo, -1, keepdims=True)
        probs_low = (expo / total).astype(jnp.bfloat16)
        result = jnp.einsum(
            "hqk,khd->qhd", probs_low, head_values, preferred_element_type=jnp.float32
        ).astype(jnp.bfloat16)
        return (result, (top + jnp.log(total))[..., 0])

    attended_blocks, log_totals = lax.map(forward_block, starts)
    attended = attended_blocks.reshape(length, local_heads * VDIM)
    middle = residual_stream + scatter_seq(
        rows_dot(attended, full_out).astype(jnp.bfloat16)
    ).astype(jnp.float32)
    normed_two, inv_two = norm_forward(middle, second_norm_weight)
    second_all = gather_seq(normed_two.astype(jnp.bfloat16))

    sgate_pre = rows_dot(second_all, full_sgate)
    sup_pre = rows_dot(second_all, full_sup)
    shidden = (jax.nn.silu(sgate_pre) * sup_pre).astype(jnp.bfloat16)
    d_sdown = inner_rows(shidden, upstream_all).astype(jnp.bfloat16)
    d_sgate, d_sup = swish_gradient(sgate_pre, sup_pre, times_transposed(upstream_all, full_sdown))
    d_sgate = d_sgate.astype(jnp.bfloat16)
    d_sup = d_sup.astype(jnp.bfloat16)
    d_wsgate = inner_rows(second_all, d_sgate).astype(jnp.bfloat16)
    d_wsup = inner_rows(second_all, d_sup).astype(jnp.bfloat16)

    egate_pre = rows_dot(second_all, full_egate)
    eup_pre = rows_dot(second_all, full_eup)
    ehidden = (jax.nn.silu(egate_pre) * eup_pre).astype(jnp.bfloat16)
    d_eoutput = (gate_column * upstream_all.astype(jnp.float32)).astype(jnp.bfloat16)
    d_edown = inner_rows(ehidden, d_eoutput).astype(jnp.bfloat16)
    d_egate, d_eup = swish_gradient(egate_pre, eup_pre, times_transposed(d_eoutput, full_edown))
    d_egate = d_egate.astype(jnp.bfloat16)
    d_eup = d_eup.astype(jnp.bfloat16)
    d_second = scatter_seq(
        (
            times_transposed(d_sgate, full_sgate)
            + times_transposed(d_sup, full_sup)
            + times_transposed(d_egate, full_egate)
            + times_transposed(d_eup, full_eup)
        ).astype(jnp.bfloat16)
    ).astype(jnp.float32)
    d_wegate = inner_rows(second_all, d_egate).astype(jnp.bfloat16)
    d_weup = inner_rows(second_all, d_eup).astype(jnp.bfloat16)
    eoutput = rows_dot(ehidden, full_edown).astype(jnp.bfloat16).astype(jnp.float32)
    added = scatter_seq(
        (rows_dot(shidden, full_sdown) + gate_column * eoutput).astype(jnp.bfloat16)
    ).astype(jnp.float32)
    output = (middle + added).astype(jnp.bfloat16).reshape(1, tok_rows, model_width)

    d_middle_norm, d_gain_two = norm_backward(middle, inv_two, second_norm_weight, d_second)
    d_middle = upstream.astype(jnp.float32) + d_middle_norm
    d_branch_all = gather_seq(d_middle.astype(jnp.bfloat16))
    d_wout = inner_rows(attended, d_branch_all).astype(jnp.bfloat16)
    d_heads = (
        times_transposed(d_branch_all, full_out)
        .astype(jnp.bfloat16)
        .reshape(length, local_heads, VDIM)
    )

    def backward_block(carry, element):
        offset, block_lse = element
        key_sum, value_sum = carry
        queries = lax.dynamic_slice_in_dim(head_query, offset, block_rows, 0)
        d_out = lax.dynamic_slice_in_dim(d_heads, offset, block_rows, 0)
        scores = masked_scores(queries, head_keys, offset, score_scale)
        probs = jnp.exp(scores - block_lse[..., None])
        probs_low = probs.astype(jnp.bfloat16)
        d_probs = jnp.einsum("qhd,khd->hqk", d_out, head_values, preferred_element_type=jnp.float32)
        centre = jnp.sum(probs * d_probs, -1, keepdims=True)
        d_scores = (probs * (d_probs - centre)).astype(jnp.bfloat16)
        d_queries = (
            jnp.einsum("hqk,khd->qhd", d_scores, head_keys, preferred_element_type=jnp.float32)
            * score_scale
        )
        key_sum = (
            key_sum
            + jnp.einsum("hqk,qhd->khd", d_scores, queries, preferred_element_type=jnp.float32)
            * score_scale
        )
        value_sum = value_sum + jnp.einsum(
            "hqk,qhd->khd", probs_low, d_out, preferred_element_type=jnp.float32
        )
        return ((key_sum, value_sum), d_queries)

    zero_keys = jnp.zeros((length, local_heads, query_width), jnp.float32)
    zero_values = jnp.zeros((length, local_heads, VDIM), jnp.float32)
    (d_keys, d_values), d_queries = lax.scan(
        backward_block, (zero_keys, zero_values), (starts, log_totals)
    )
    d_queries = d_queries.reshape(length, local_heads, query_width)
    d_queries = jnp.concatenate(
        [d_queries[..., :NOPE], rotate(d_queries[..., NOPE:], cos_all[:, None], -sin_all[:, None])],
        -1,
    )
    d_queries = d_queries.astype(jnp.bfloat16).reshape(length, local_heads * query_width)
    d_keys = d_keys.astype(jnp.bfloat16)
    d_values = d_values.astype(jnp.bfloat16)
    d_keyval = jnp.concatenate([d_keys[..., :NOPE], d_values], -1).reshape(
        length, local_heads * (NOPE + VDIM)
    )
    d_wkvup = inner_rows(latent_all, d_keyval).astype(jnp.bfloat16)
    d_wquery = inner_rows(first_all, d_queries).astype(jnp.bfloat16)
    first_part = times_transposed(d_queries, full_query).astype(jnp.bfloat16)
    latent_part = times_transposed(d_keyval, full_kvup).astype(jnp.bfloat16)
    rope_part = jnp.sum(d_keys[..., NOPE:].astype(jnp.float32), 1).astype(jnp.bfloat16)
    latent_back = scatter_seq(jnp.concatenate([latent_part, rope_part], -1)).astype(jnp.float32)
    first_back = scatter_seq(first_part).astype(jnp.float32)

    own_latent = lax.dynamic_slice_in_dim(latent, own_start, tok_rows, 0)[:, :RANK]
    cos_own = lax.dynamic_slice_in_dim(cos_all, own_start, tok_rows, 0)
    sin_own = lax.dynamic_slice_in_dim(sin_all, own_start, tok_rows, 0)
    inv_latent = norm_forward(own_latent, latent_norm_weight)[1]
    d_rope = rotate(latent_back[:, RANK:], cos_own, -sin_own)
    d_compressed, d_gain_latent = norm_backward(
        own_latent, inv_latent, latent_norm_weight, latent_back[:, :RANK]
    )
    d_latent = jnp.concatenate([d_compressed, d_rope], -1).astype(jnp.bfloat16)
    d_latent_all = gather_seq(d_latent)
    inv_one = norm_forward(residual_stream, first_norm_weight)[1]
    d_first = first_back + times_transposed(d_latent, full_latent)
    d_resid, d_gain_one = norm_backward(residual_stream, inv_one, first_norm_weight, d_first)
    input_grad = (d_middle + d_resid).reshape(1, tok_rows, model_width)
    own_columns = lax.dynamic_index_in_dim(
        first_all.reshape(length, shards, groups, one_width), me, 2, keepdims=False
    ).reshape(length, shards * one_width)
    d_wlatent = inner_rows(own_columns, d_latent_all).astype(jnp.bfloat16)

    def scatter_shard(grad, axis):
        return lax.psum_scatter(grad, "shard", scatter_dimension=axis, tiled=True).astype(
            jnp.float32
        )

    devices = shards * groups
    gain_grads = lax.psum_scatter(
        jnp.concatenate(
            [
                d_gain_one.reshape(devices, one_width),
                d_gain_latent.reshape(devices, lat_width),
                d_gain_two.reshape(devices, one_width),
            ],
            1,
        ),
        ("shard", "seq"),
        scatter_dimension=0,
        tiled=True,
    ).reshape(-1)
    return (
        output,
        input_grad,
        gain_grads[:one_width],
        scatter_shard(d_wquery, 0),
        scatter_shard(d_wlatent, 0),
        gain_grads[one_width : one_width + lat_width],
        scatter_shard(d_wkvup, 0),
        scatter_shard(d_wout, 1),
        gain_grads[one_width + lat_width :],
        scatter_shard(d_wsgate, 0),
        scatter_shard(d_wsup, 0),
        scatter_shard(d_sdown, 1),
        scatter_shard(d_wegate, 0)[None],
        scatter_shard(d_weup, 0)[None],
        scatter_shard(d_edown, 1)[None],
    )


def solution(mesh):
    in_specs = (
        P("shard", "seq", None),
        P(("shard", "seq")),
        P("shard", "seq"),
        P(("shard", "seq"), None),
        P(("shard", "seq")),
        P("shard", "seq"),
        P("seq", "shard"),
        P(("shard", "seq")),
        P("shard", "seq"),
        P("shard", "seq"),
        P("seq", "shard"),
        P("seq", "shard", None),
        P("seq", "shard", None),
        P("seq", None, "shard"),
        P("shard", "seq", None),
        P("shard", "seq", None),
        P("shard", "seq", None),
        P("shard", "seq", None),
    )
    out_specs = (
        P("shard", "seq", None),
        P("shard", "seq", None),
        P(("shard", "seq")),
        P("shard", "seq"),
        P(("shard", "seq"), None),
        P(("shard", "seq")),
        P("shard", "seq"),
        P("seq", "shard"),
        P(("shard", "seq")),
        P("shard", "seq"),
        P("shard", "seq"),
        P("seq", "shard"),
        P("seq", "shard", None),
        P("seq", "shard", None),
        P("seq", None, "shard"),
    )
    return jax.shard_map(
        on_device, mesh=mesh, in_specs=in_specs, out_specs=out_specs, check_vma=False
    )
```

```python
import functools

import jax
import jax.numpy as jnp
from jax import lax
from jax.experimental import pallas as pl
from jax.experimental.pallas import tpu as pltpu
from jax.sharding import PartitionSpec as P

HEADS = 16
NOPE = 128
ROPE = 64
VDIM = 128
RANK = 512
TOPK = 6
EXP_DEV = 1


EPSILON = 1e-06
THETA = 10000.0
MASKED = -1e30


def rope_tables(positions, depth):
    half_depth = depth // 2
    frequency = THETA ** (-(2.0 * jnp.arange(half_depth, dtype=jnp.float32)) / depth)
    angles = positions.astype(jnp.float32)[:, None] * frequency[None, :]
    return (jnp.cos(angles), jnp.sin(angles))


def rotate(values, cosine, sine):
    half_depth = values.shape[-1] // 2
    first = values[..., :half_depth]
    second = values[..., half_depth:]
    return jnp.concatenate([first * cosine - second * sine, second * cosine + first * sine], -1)


def norm_forward(values, scaling):
    inverse = lax.rsqrt(jnp.mean(values * values, -1, keepdims=True) + EPSILON)
    return (values * inverse * scaling, inverse)


def norm_backward(values, inverse, scaling, upstream):
    weighted = upstream * scaling
    scaling_grad = jnp.sum(upstream * values * inverse, 0)
    centre = jnp.mean(weighted * values, -1, keepdims=True)
    return (inverse * weighted - values * inverse**3 * centre, scaling_grad)


def swish_gradient(gate_pre, upper, upstream):
    sigma = jax.nn.sigmoid(gate_pre)
    return (
        upstream * upper * sigma * (1.0 + gate_pre * (1.0 - sigma)),
        upstream * gate_pre * sigma,
    )


def inner_rows(left, right):
    return lax.dot_general(
        left, right, (((0,), (0,)), ((), ())), preferred_element_type=jnp.float32
    )


def times_transposed(left, right):
    return lax.dot_general(
        left, right, (((1,), (1,)), ((), ())), preferred_element_type=jnp.float32
    )


def masked_scores(queries, keys, offset, score_scale):
    scores = (
        jnp.einsum("qhd,khd->hqk", queries, keys, preferred_element_type=jnp.float32) * score_scale
    )
    query_pos = offset + jnp.arange(queries.shape[0])
    seen = jnp.arange(keys.shape[0])[None, :] <= query_pos[:, None]
    return jnp.where(seen[None], scores, MASKED)


MESH = pl.DeviceIdType.MESH

def ring_place(n):
    me = lax.axis_index("seq")
    core = me % 2
    place = me // 2 + core * (n - 1 - 2 * (me // 2))
    return me, place

def ring_device(place, n):
    half = n // 2
    back = place // half
    return back * (2 * (n - 1 - place) + 1) + (1 - back) * 2 * place

def meet(n, place):
    barrier = pltpu.get_barrier_semaphore()
    before = ring_device((place + n - 1) % n, n)
    pl.semaphore_signal(barrier, inc=1, device_id={"seq": before}, device_id_type=MESH)
    pl.semaphore_wait(barrier, 1)

def gather_kernel(n, parts, count, *refs):
    ins = refs[:count]; outs = refs[count:2*count]
    send, recv, local = refs[2*count:]
    me, place = ring_place(n)
    after = ring_device((place + 1) % n, n)
    rows = ins[0].shape[0] // parts
    own = [pltpu.make_async_copy(ins[a], outs[a].at[me], local.at[a]) for a in range(count)]
    meet(n, place)
    started = []
    def push(source, block, step, part, a):
        span = pl.ds(part * rows, rows)
        copy = pltpu.make_async_remote_copy(
            src_ref=source.at[span], dst_ref=outs[a].at[block, span],
            send_sem=send.at[a, step, part], recv_sem=recv.at[a, step, part],
            device_id={"seq": after}, device_id_type=MESH)
        copy.start()
        started.append(copy)
        return copy
    waits = {}
    for part in range(parts):
        for a in range(count):
            waits[a, part] = push(ins[a], me, 0, part, a)
    for copy in own: copy.start()
    for step in range(n - 1):
        block = ring_device((place + n - 1 - step) % n, n)
        for part in range(parts):
            for a in range(count):
                waits[a, part].wait_recv()
                if step < n - 2:
                    waits[a, part] = push(outs[a].at[block], block, step + 1, part, a)
    for copy in started: copy.wait_send()
    for copy in own: copy.wait()

def ring_gather(n, blocks, identity, parts=2):
    count = len(blocks)
    return pl.pallas_call(
        functools.partial(gather_kernel, n, parts, count),
        out_shape=[jax.ShapeDtypeStruct((n,) + b.shape, b.dtype) for b in blocks],
        in_specs=[pl.BlockSpec(memory_space=pltpu.VMEM)] * count,
        out_specs=[pl.BlockSpec(memory_space=pl.ANY)] * count,
        scratch_shapes=[pltpu.SemaphoreType.DMA((count, n - 1, parts)), pltpu.SemaphoreType.DMA((count, n - 1, parts)), pltpu.SemaphoreType.DMA((count,))],
        compiler_params=pltpu.CompilerParams(collective_id=identity, has_side_effects=True),
        cost_estimate=wire_cost(n, sum(b.size for b in blocks)),
        name="ring_gather",
    )(*blocks)

def scatter_kernel(n, parts, partial_ref, out_ref, own, held, send, recv, local):
    me, place = ring_place(n)
    after = ring_device((place + 1) % n, n)
    rows = out_ref.shape[0] // parts
    def block_of(step):
        return ring_device((place + 2 * n - 1 - step) % n, n)
    loads = []
    for step in range(n):
        copy = pltpu.make_async_copy(partial_ref.at[block_of(step)], own.at[step], local.at[step])
        copy.start(); loads.append(copy)
    meet(n, place)
    started = []
    def push(source, step, part):
        span = pl.ds(part * rows, rows)
        copy = pltpu.make_async_remote_copy(
            src_ref=source.at[span], dst_ref=held.at[step, span],
            send_sem=send.at[step, part], recv_sem=recv.at[step, part],
            device_id={"seq": after}, device_id_type=MESH)
        copy.start(); started.append(copy)
        return copy
    loads[0].wait()
    waits = {p: push(own.at[0], 0, p) for p in range(parts)}
    for step in range(1, n):
        loads[step].wait()
        for part in range(parts):
            span = pl.ds(part * rows, rows)
            waits[part].wait_recv()
            total = held[step - 1, span].astype(jnp.float32) + own[step, span].astype(jnp.float32)
            if step < n - 1:
                own[step, span] = total.astype(own.dtype)
                waits[part] = push(own.at[step], step, part)
            else:
                out_ref[span] = total.astype(out_ref.dtype)
    for copy in started: copy.wait_send()

def ring_scatter(n, partial, identity, parts=2, dtype=jnp.float32):
    rows, width = partial.shape[0] // n, partial.shape[1]
    return pl.pallas_call(
        functools.partial(scatter_kernel, n, parts),
        out_shape=jax.ShapeDtypeStruct((rows, width), dtype),
        in_specs=[pl.BlockSpec(memory_space=pl.ANY)],
        out_specs=pl.BlockSpec(memory_space=pltpu.VMEM),
        scratch_shapes=[
            pltpu.VMEM((n, rows, width), partial.dtype), pltpu.VMEM((n - 1, rows, width), partial.dtype),
            pltpu.SemaphoreType.DMA((n - 1, parts)), pltpu.SemaphoreType.DMA((n - 1, parts)), pltpu.SemaphoreType.DMA((n,))],
        compiler_params=pltpu.CompilerParams(collective_id=identity, has_side_effects=True),
        cost_estimate=wire_cost(n, rows * width),
        name="ring_scatter",
    )(partial.reshape(n, rows, width))


def wire_cost(n, size):
    return pl.CostEstimate(
        flops=(n - 1) * size * 2 * 9000, bytes_accessed=2 * n * size, transcendentals=0
    )


def settle_kernel(n, shards, terms_ref, out_ref, from_seq, joined, from_shard, sends, seq_recv, shard_recv):
    me = lax.axis_index("seq")
    my_shard = lax.axis_index("shard")
    barrier = pltpu.get_barrier_semaphore()
    for hop in range(1, n):
        pl.semaphore_signal(
            barrier, inc=1, device_id={"seq": (me + hop) % n}, device_id_type=MESH
        )
    for hop in range(1, shards):
        pl.semaphore_signal(
            barrier, inc=1, device_id={"shard": (my_shard + hop) % shards}, device_id_type=MESH
        )
    pl.semaphore_wait(barrier, n + shards - 2)
    first = []
    for hop in range(1, n):
        target = (me + hop) % n
        copy = pltpu.make_async_remote_copy(
            src_ref=terms_ref.at[target],
            dst_ref=from_seq.at[hop - 1],
            send_sem=sends.at[hop - 1],
            recv_sem=seq_recv.at[hop - 1],
            device_id={"seq": target},
            device_id_type=MESH,
        )
        copy.start()
        first.append(copy)
    total = terms_ref[me]
    for hop in range(1, n):
        first[hop - 1].wait_recv()
        total = total + from_seq[hop - 1]
    joined[...] = total
    second = []
    for hop in range(1, shards):
        target = (my_shard + hop) % shards
        copy = pltpu.make_async_remote_copy(
            src_ref=joined.at[target],
            dst_ref=from_shard.at[hop - 1],
            send_sem=sends.at[n - 1 + hop - 1],
            recv_sem=shard_recv.at[hop - 1],
            device_id={"shard": target},
            device_id_type=MESH,
        )
        copy.start()
        second.append(copy)
    total = joined[my_shard]
    for hop in range(1, shards):
        second[hop - 1].wait_recv()
        total = total + from_shard[hop - 1]
    out_ref[...] = total
    for copy in first + second:
        copy.wait_send()


def settle(n, shards, terms, identity):
    shape = terms.shape[2:]
    return pl.pallas_call(
        functools.partial(settle_kernel, n, shards),
        out_shape=jax.ShapeDtypeStruct(shape, jnp.float32),
        in_specs=[pl.BlockSpec(memory_space=pltpu.VMEM)],
        out_specs=pl.BlockSpec(memory_space=pltpu.VMEM),
        scratch_shapes=[
            pltpu.VMEM((n - 1, shards) + shape, jnp.float32),
            pltpu.VMEM((shards,) + shape, jnp.float32),
            pltpu.VMEM((shards - 1,) + shape, jnp.float32),
            pltpu.SemaphoreType.DMA((n + shards - 2,)),
            pltpu.SemaphoreType.DMA((n - 1,)),
            pltpu.SemaphoreType.DMA((shards - 1,)),
        ],
        compiler_params=pltpu.CompilerParams(collective_id=identity, has_side_effects=True),
        name="settle",
    )(terms)


ACROSS = ([(0, 1), (1, 0), (2, 3), (3, 2)], [(0, 2), (2, 0), (1, 3), (3, 1)])


def swap_with(block, side):
    return lax.ppermute(block, "shard", ACROSS[side])


def gather_blocks(weight, axis, side):
    if lax.axis_size("shard") != 4:
        return [lax.all_gather(weight, "shard", axis=axis, tiled=True)]
    near = [swap_with(weight, 0), swap_with(weight, 1)]
    far = swap_with(near[side], 1 - side)
    return [weight, near[0], near[1], far]


def scatter_blocks(blocks, axis, side):
    if lax.axis_size("shard") != 4:
        return lax.psum_scatter(blocks[0], "shard", scatter_dimension=axis, tiled=True).astype(
            jnp.float32
        )
    far = swap_with(blocks[3], side)
    other = 2 - side
    joined = (blocks[other].astype(jnp.float32) + far.astype(jnp.float32)).astype(jnp.bfloat16)
    second = swap_with(joined, 1 - side)
    first = swap_with(blocks[1 + side], side)
    return (
        blocks[0].astype(jnp.float32) + first.astype(jnp.float32) + second.astype(jnp.float32)
    )


def local_order(values, axis):
    if lax.axis_size("shard") != 4:
        return values
    size = values.shape[axis] // 4
    shard = lax.axis_index("shard")
    return jnp.concatenate(
        [
            lax.dynamic_slice_in_dim(values, jnp.bitwise_xor(shard, place) * size, size, axis)
            for place in range(4)
        ],
        axis,
    )


def cut(values, axis):
    if lax.axis_size("shard") != 4:
        return [values]
    size = values.shape[axis] // 4
    return [lax.slice_in_dim(values, r * size, (r + 1) * size, axis=axis) for r in range(4)]


def rows_dot(left, right):
    return jnp.dot(left, right, preferred_element_type=jnp.float32)


def on_device(
    inputs,
    attn_gain,
    query_project_weight,
    latent_project_weight,
    latent_gain,
    latent_keyval_weight,
    attention_output_weight,
    ffn_gain,
    shared_gate,
    shared_up,
    shared_down,
    expert_gate,
    expert_up,
    expert_down,
    routes,
    slots,
    gates,
    cotangent,
):
    tok_rows = inputs.shape[1]
    model_width = inputs.shape[2]
    groups = lax.axis_size("seq")
    shards = lax.axis_size("shard")
    me = lax.axis_index("seq")
    local_heads = HEADS // groups
    query_width = NOPE + ROPE
    experts = EXP_DEV * groups
    capacity = 9 * tok_rows * TOPK // (8 * experts)
    length = tok_rows * groups
    score_scale = (NOPE + ROPE) ** (-0.5)
    block_rows = min(512, length)
    starts = jnp.arange(length // block_rows) * block_rows
    own_start = me * tok_rows
    one_width = attn_gain.shape[0]
    lat_width = latent_gain.shape[0]

    own_inputs = local_order(inputs.reshape(tok_rows, model_width), 1)
    upstream = local_order(cotangent.reshape(tok_rows, model_width), 1)
    route_rows = routes.reshape(tok_rows, TOPK)
    slot_rows = slots.reshape(tok_rows, TOPK)
    kept = (route_rows[:, :, None] == jnp.arange(128)[None, None, :]) & (
        slot_rows < capacity
    )[:, :, None]
    gate_table = jnp.sum(
        jnp.where(kept, gates.reshape(tok_rows, TOPK).astype(jnp.float32)[:, :, None], 0.0), 1
    ).astype(jnp.bfloat16)

    def padded_row(gain):
        return jnp.pad(gain, (0, one_width - gain.shape[0]))[None]

    side_rows = jnp.concatenate(
        [
            padded_row(attn_gain),
            padded_row(ffn_gain),
            padded_row(latent_gain),
            jnp.zeros((one_width - 3, one_width), jnp.bfloat16),
        ],
        0,
    )
    small = lax.all_gather(
        jnp.concatenate([latent_project_weight, side_rows], 1), ("shard", "seq"), axis=0, tiled=True
    )
    latent_norm_weight = (
        small.reshape(shards * groups, one_width, -1)[:, 2, RANK + ROPE : RANK + ROPE + lat_width]
        .reshape(-1)
        .astype(jnp.float32)
    )
    small = local_order(small, 0)
    full_latent = small[:, : RANK + ROPE]
    gain_rows = small.reshape(shards * groups, one_width, -1)[:, :2, RANK + ROPE :].astype(
        jnp.float32
    )
    first_norm_weight = gain_rows[:, 0].reshape(-1)
    second_norm_weight = gain_rows[:, 1].reshape(-1)

    query_blocks = gather_blocks(query_project_weight, 0, 0)
    kvup_blocks = gather_blocks(latent_keyval_weight, 0, 1)
    out_blocks = gather_blocks(attention_output_weight, 1, 1)
    sgu_blocks = gather_blocks(jnp.concatenate([shared_gate, shared_up], 1), 0, 0)
    egate_blocks = gather_blocks(expert_gate[0], 0, 0)
    eup_blocks = gather_blocks(expert_up[0], 0, 1)
    down_blocks = gather_blocks(jnp.concatenate([expert_down[0], shared_down], 0), 1, 1)
    full_query = jnp.concatenate(query_blocks, 0)
    full_kvup = local_order(jnp.concatenate(kvup_blocks, 0), 0)
    full_out = jnp.concatenate(out_blocks, 1)
    full_sgu = jnp.concatenate(sgu_blocks, 0)
    full_egate = jnp.concatenate(egate_blocks, 0)
    full_eup = jnp.concatenate(eup_blocks, 0)
    full_down = jnp.concatenate(down_blocks, 1)
    ff = expert_gate.shape[2]
    shared_ff = shared_gate.shape[1]

    inputs_all, table_all = ring_gather(groups, [own_inputs, gate_table], 1)
    inputs_all = inputs_all.reshape(length, model_width)
    gate_column = lax.dynamic_slice_in_dim(table_all.reshape(length, -1), me, 1, 1).astype(
        jnp.float32
    )
    upstream_all = lax.all_gather(upstream, "seq", axis=0, tiled=True)

    residual_stream = own_inputs.astype(jnp.float32)
    first_all = norm_forward(inputs_all.astype(jnp.float32), first_norm_weight)[0].astype(
        jnp.bfloat16
    )
    cos_all, sin_all = rope_tables(jnp.arange(length), ROPE)
    latent = rows_dot(first_all, full_latent)
    latent_all = norm_forward(latent[:, :RANK], latent_norm_weight)[0].astype(jnp.bfloat16)
    rope_all = rotate(latent[:, RANK:], cos_all, sin_all).astype(jnp.bfloat16)
    head_query = rows_dot(first_all, full_query).reshape(length, local_heads, query_width)
    head_query = jnp.concatenate(
        [
            head_query[..., :NOPE],
            rotate(head_query[..., NOPE:], cos_all[:, None], sin_all[:, None]),
        ],
        -1,
    ).astype(jnp.bfloat16)
    keyval = (
        rows_dot(latent_all, full_kvup)
        .astype(jnp.bfloat16)
        .reshape(length, local_heads, NOPE + VDIM)
    )
    head_keys = jnp.concatenate(
        [keyval[..., :NOPE], jnp.broadcast_to(rope_all[:, None, :], (length, local_heads, ROPE))],
        -1,
    )
    head_values = keyval[..., NOPE:]

    def forward_block(offset):
        queries = lax.dynamic_slice_in_dim(head_query, offset, block_rows, 0)
        scores = masked_scores(queries, head_keys, offset, score_scale)
        top = jnp.max(scores, -1, keepdims=True)
        expo = jnp.exp(scores - top)
        total = jnp.sum(expo, -1, keepdims=True)
        probs_low = (expo / total).astype(jnp.bfloat16)
        result = jnp.einsum(
            "hqk,khd->qhd", probs_low, head_values, preferred_element_type=jnp.float32
        ).astype(jnp.bfloat16)
        return (result, (top + jnp.log(total))[..., 0])

    attended_blocks, log_totals = lax.map(forward_block, starts)
    attended = attended_blocks.reshape(length, local_heads * VDIM)
    middle = residual_stream + ring_scatter(
        groups, rows_dot(attended, full_out).astype(jnp.bfloat16), 2
    )
    normed_two, inv_two = norm_forward(middle, second_norm_weight)
    (second_all,) = ring_gather(groups, [normed_two.astype(jnp.bfloat16)], 3)
    second_all = second_all.reshape(length, model_width)

    sgu_pre = rows_dot(second_all, full_sgu)
    egate_pre = rows_dot(second_all, full_egate)
    eup_pre = rows_dot(second_all, full_eup)
    ehidden = jax.nn.silu(egate_pre) * eup_pre
    shidden = jax.nn.silu(sgu_pre[:, :shared_ff]) * sgu_pre[:, shared_ff:]
    hidden = jnp.concatenate([gate_column * ehidden, shidden], 1).astype(jnp.bfloat16)
    d_hidden = times_transposed(upstream_all, full_down)
    d_down = [inner_rows(hidden, part).astype(jnp.bfloat16) for part in cut(upstream_all, 1)]
    d_egate, d_eup = swish_gradient(egate_pre, eup_pre, gate_column * d_hidden[:, :ff])
    d_sgate, d_sup = swish_gradient(
        sgu_pre[:, :shared_ff], sgu_pre[:, shared_ff:], d_hidden[:, ff:]
    )
    d_egate = d_egate.astype(jnp.bfloat16)
    d_eup = d_eup.astype(jnp.bfloat16)
    d_sgu = jnp.concatenate([d_sgate, d_sup], 1).astype(jnp.bfloat16)
    d_second = ring_scatter(
        groups,
        (
            times_transposed(d_sgu, full_sgu)
            + times_transposed(d_egate, full_egate)
            + times_transposed(d_eup, full_eup)
        ).astype(jnp.bfloat16),
        4,
    )
    second_parts = cut(second_all, 1)
    d_wegate = [inner_rows(part, d_egate).astype(jnp.bfloat16) for part in second_parts]
    d_weup = [inner_rows(part, d_eup).astype(jnp.bfloat16) for part in second_parts]
    d_wsgu = [inner_rows(part, d_sgu).astype(jnp.bfloat16) for part in second_parts]
    added = lax.psum_scatter(
        rows_dot(hidden, full_down).astype(jnp.bfloat16), "seq", scatter_dimension=0, tiled=True
    ).astype(jnp.float32)
    output = local_order((middle + added).astype(jnp.bfloat16), 1).reshape(
        1, tok_rows, model_width
    )

    d_middle_norm, d_gain_two = norm_backward(middle, inv_two, second_norm_weight, d_second)
    d_middle = upstream.astype(jnp.float32) + d_middle_norm
    (d_branch_all,) = ring_gather(groups, [d_middle.astype(jnp.bfloat16)], 5)
    d_branch_all = d_branch_all.reshape(length, model_width)
    d_wout = [inner_rows(attended, part).astype(jnp.bfloat16) for part in cut(d_branch_all, 1)]
    d_heads = (
        times_transposed(d_branch_all, full_out)
        .astype(jnp.bfloat16)
        .reshape(length, local_heads, VDIM)
    )

    def backward_block(carry, element):
        offset, block_lse = element
        key_sum, value_sum = carry
        queries = lax.dynamic_slice_in_dim(head_query, offset, block_rows, 0)
        d_out = lax.dynamic_slice_in_dim(d_heads, offset, block_rows, 0)
        scores = masked_scores(queries, head_keys, offset, score_scale)
        probs = jnp.exp(scores - block_lse[..., None])
        probs_low = probs.astype(jnp.bfloat16)
        d_probs = jnp.einsum("qhd,khd->hqk", d_out, head_values, preferred_element_type=jnp.float32)
        centre = jnp.sum(probs * d_probs, -1, keepdims=True)
        d_scores = (probs * (d_probs - centre)).astype(jnp.bfloat16)
        d_queries = (
            jnp.einsum("hqk,khd->qhd", d_scores, head_keys, preferred_element_type=jnp.float32)
            * score_scale
        )
        key_sum = (
            key_sum
            + jnp.einsum("hqk,qhd->khd", d_scores, queries, preferred_element_type=jnp.float32)
            * score_scale
        )
        value_sum = value_sum + jnp.einsum(
            "hqk,qhd->khd", probs_low, d_out, preferred_element_type=jnp.float32
        )
        return ((key_sum, value_sum), d_queries)

    zero_keys = jnp.zeros((length, local_heads, query_width), jnp.float32)
    zero_values = jnp.zeros((length, local_heads, VDIM), jnp.float32)
    (d_keys, d_values), d_queries = lax.scan(
        backward_block, (zero_keys, zero_values), (starts, log_totals)
    )
    d_queries = d_queries.reshape(length, local_heads, query_width)
    d_queries = jnp.concatenate(
        [d_queries[..., :NOPE], rotate(d_queries[..., NOPE:], cos_all[:, None], -sin_all[:, None])],
        -1,
    )
    d_queries = d_queries.astype(jnp.bfloat16).reshape(length, local_heads * query_width)
    d_keys = d_keys.astype(jnp.bfloat16)
    d_values = d_values.astype(jnp.bfloat16)
    d_keyval = jnp.concatenate([d_keys[..., :NOPE], d_values], -1).reshape(
        length, local_heads * (NOPE + VDIM)
    )
    d_wkvup = cut(local_order(inner_rows(latent_all, d_keyval).astype(jnp.bfloat16), 0), 0)
    d_wquery = [inner_rows(part, d_queries).astype(jnp.bfloat16) for part in cut(first_all, 1)]
    first_part = times_transposed(d_queries, full_query).astype(jnp.bfloat16)
    latent_part = times_transposed(d_keyval, full_kvup)
    rope_part = jnp.sum(d_keys[..., NOPE:].astype(jnp.float32), 1)
    latent_back = ring_scatter(
        groups,
        jnp.concatenate(
            [latent_part, rope_part, jnp.zeros((length, 128 - ROPE), jnp.float32)], -1
        ).astype(jnp.bfloat16),
        6,
    )

    own_latent = lax.dynamic_slice_in_dim(latent, own_start, tok_rows, 0)[:, :RANK]
    cos_own = lax.dynamic_slice_in_dim(cos_all, own_start, tok_rows, 0)
    sin_own = lax.dynamic_slice_in_dim(sin_all, own_start, tok_rows, 0)
    inv_latent = norm_forward(own_latent, latent_norm_weight)[1]
    d_rope = rotate(latent_back[:, RANK : RANK + ROPE], cos_own, -sin_own)
    d_compressed, d_gain_latent = norm_backward(
        own_latent, inv_latent, latent_norm_weight, latent_back[:, :RANK]
    )
    d_latent = jnp.concatenate([d_compressed, d_rope], -1).astype(jnp.bfloat16)
    first_back = ring_scatter(groups, first_part, 7)
    (d_latent_all,) = ring_gather(groups, [jnp.pad(d_latent, ((0, 0), (0, 128 - ROPE)))], 8)
    d_latent_all = d_latent_all.reshape(length, -1)[:, : RANK + ROPE]
    inv_one = norm_forward(residual_stream, first_norm_weight)[1]
    d_first = first_back + times_transposed(d_latent, full_latent)
    d_resid, d_gain_one = norm_backward(residual_stream, inv_one, first_norm_weight, d_first)
    input_grad = local_order(d_middle + d_resid, 1).reshape(1, tok_rows, model_width)
    own_columns = lax.dynamic_index_in_dim(
        first_all.reshape(length, shards, groups, one_width), me, 2, keepdims=False
    ).reshape(length, shards * one_width)
    d_wlatent = cut(inner_rows(own_columns, d_latent_all).astype(jnp.bfloat16), 0)

    devices = shards * groups
    terms = jnp.concatenate(
        [
            local_order(d_gain_one, 0).reshape(devices, one_width),
            local_order(d_gain_two, 0).reshape(devices, one_width),
            d_gain_latent.reshape(devices, lat_width),
        ],
        1,
    )
    terms = jnp.pad(terms, ((0, 0), (0, 1024 - terms.shape[1]))).reshape(shards, groups, 8, 128)
    gain_grads = settle(groups, shards, terms.transpose(1, 0, 2, 3), 9).reshape(-1)
    down_grad = scatter_blocks(d_down, 1, 1)
    sgu_grad = scatter_blocks(d_wsgu, 0, 0)
    return (
        output,
        input_grad,
        gain_grads[:one_width],
        scatter_blocks(d_wquery, 0, 0),
        scatter_blocks(d_wlatent, 0, 0),
        gain_grads[2 * one_width : 2 * one_width + lat_width],
        scatter_blocks(d_wkvup, 0, 1),
        scatter_blocks(d_wout, 1, 1),
        gain_grads[one_width : 2 * one_width],
        sgu_grad[:, :shared_ff],
        sgu_grad[:, shared_ff:],
        down_grad[ff:],
        scatter_blocks(d_wegate, 0, 0)[None],
        scatter_blocks(d_weup, 0, 1)[None],
        down_grad[None, :ff],
    )


def solution(mesh):
    in_specs = (
        P("shard", "seq", None),
        P(("shard", "seq")),
        P("shard", "seq"),
        P(("shard", "seq"), None),
        P(("shard", "seq")),
        P("shard", "seq"),
        P("seq", "shard"),
        P(("shard", "seq")),
        P("shard", "seq"),
        P("shard", "seq"),
        P("seq", "shard"),
        P("seq", "shard", None),
        P("seq", "shard", None),
        P("seq", None, "shard"),
        P("shard", "seq", None),
        P("shard", "seq", None),
        P("shard", "seq", None),
        P("shard", "seq", None),
    )
    out_specs = (
        P("shard", "seq", None),
        P("shard", "seq", None),
        P(("shard", "seq")),
        P("shard", "seq"),
        P(("shard", "seq"), None),
        P(("shard", "seq")),
        P("shard", "seq"),
        P("seq", "shard"),
        P(("shard", "seq")),
        P("shard", "seq"),
        P("shard", "seq"),
        P("seq", "shard"),
        P("seq", "shard", None),
        P("seq", "shard", None),
        P("seq", None, "shard"),
    )
    return jax.shard_map(
        on_device, mesh=mesh, in_specs=in_specs, out_specs=out_specs, check_vma=False
    )
```

```python
import functools

import jax
import jax.numpy as jnp
from jax import lax
from jax.experimental import pallas as pl
from jax.experimental.pallas import tpu as pltpu
from jax.sharding import PartitionSpec as P

HEADS = 16
NOPE = 128
ROPE = 64
VDIM = 128
RANK = 512
TOPK = 6
EXP_DEV = 1
EXTRA = 16


EPSILON = 1e-06
THETA = 10000.0
MASKED = -1e30
MESH = pl.DeviceIdType.MESH


LANES = 128
STEP = 256
WIDE = 512
NARROW = 512
CHUNK = 512


def nn(left, right):
    return jnp.dot(left, right, preferred_element_type=jnp.float32)


def nt(left, right):
    return lax.dot_general(
        left, right, (((1,), (1,)), ((), ())), preferred_element_type=jnp.float32
    )


def tn(left, right):
    return lax.dot_general(
        left, right, (((0,), (0,)), ((), ())), preferred_element_type=jnp.float32
    )


def lane_index(rows):
    return lax.broadcasted_iota(jnp.int32, (rows, LANES), 1)


def turn(tile, cosine, sine):
    lane = lane_index(tile.shape[0])
    low = pltpu.roll(tile, LANES - ROPE // 2, 1)
    high = pltpu.roll(tile, ROPE // 2, 1)
    return tile * cosine + jnp.where(lane < ROPE // 2, low, high) * sine


def rope_lanes(positions):
    half = ROPE // 2
    frequency = THETA ** (-(2.0 * jnp.arange(half, dtype=jnp.float32)) / ROPE)
    angles = positions.astype(jnp.float32)[:, None] * frequency[None, :]
    cosine, sine = jnp.cos(angles), jnp.sin(angles)
    blank = jnp.zeros((positions.shape[0], LANES - ROPE), jnp.float32)
    return (
        jnp.concatenate([cosine, cosine, blank], 1),
        jnp.concatenate([-sine, sine, blank], 1),
    )


def split_heads(values, heads):
    width = NOPE + ROPE
    rows = values.shape[0]
    keep = lane_index(rows) < ROPE
    tiles = []
    for head in range(heads):
        part = values if head == 0 else pltpu.roll(values, (heads - head) * width, 1)
        if part.shape[1] >= 2 * LANES:
            turned = jnp.where(keep, part[:, NOPE : NOPE + LANES], 0.0)
        else:
            turned = jnp.concatenate(
                [part[:, NOPE:], jnp.zeros((rows, LANES - ROPE), part.dtype)], 1
            )
        tiles.append((part[:, :NOPE], turned))
    return tiles


def join_heads(tiles):
    heads = len(tiles)
    width = NOPE + ROPE
    if heads == 1:
        return jnp.concatenate([tiles[0][0], tiles[0][1][:, :ROPE]], 1)
    rows = tiles[0][0].shape[0]
    blank = jnp.zeros((rows, heads * width - 2 * LANES), jnp.float32)
    total = None
    for head, (plain, turned) in enumerate(tiles):
        part = jnp.concatenate([plain, turned, blank], 1)
        part = part if head == 0 else pltpu.roll(part, head * width, 1)
        total = part if total is None else total + part
    return total


def front_kernel(heads, count, shards, *refs):
    x_ref, gain_ref, lat_gain_ref, cos_ref, sin_ref, kvup_ref = refs[:6]
    query_refs = refs[6 : 6 + count]
    latent_refs = refs[6 + count : 6 + count + shards]
    first_ref, q_ref, k_ref, v_ref, latent_ref, low_ref = refs[6 + count + shards :]
    values = x_ref[...].astype(jnp.float32)
    inverse = lax.rsqrt(jnp.mean(values * values, -1, keepdims=True) + EPSILON)
    first = (values * inverse * gain_ref[...]).astype(jnp.bfloat16)
    first_ref[...] = first
    depth = query_refs[0].shape[0]
    query = None
    latent = None
    for r in range(count):
        term = nn(first[:, r * depth : (r + 1) * depth], query_refs[r][...])
        query = term if query is None else query + term
    depth = first.shape[1] // shards
    for r in range(shards):
        weight = latent_refs[r][...].reshape(depth, latent_refs[r].shape[2])
        term = nn(first[:, r * depth : (r + 1) * depth], weight)
        latent = term if latent is None else latent + term
    cosine, sine = cos_ref[...], sin_ref[...]
    for head, (plain, turned) in enumerate(split_heads(query, heads)):
        base = head * 2 * LANES
        q_ref[:, base : base + LANES] = plain.astype(jnp.bfloat16)
        q_ref[:, base + LANES : base + 2 * LANES] = turn(turned, cosine, sine).astype(
            jnp.bfloat16
        )
    packed = latent[:, :RANK]
    latent_ref[...] = packed
    inverse = lax.rsqrt(jnp.mean(packed * packed, -1, keepdims=True) + EPSILON)
    low = (packed * inverse * lat_gain_ref[...]).astype(jnp.bfloat16)
    low_ref[...] = low
    shared = jnp.where(
        lane_index(packed.shape[0]) < ROPE, latent[:, RANK : RANK + LANES], 0.0
    )
    shared = turn(shared, cosine, sine).astype(jnp.bfloat16)
    keyval = nn(low, kvup_ref[...]).astype(jnp.bfloat16)
    for head in range(heads):
        base = head * 2 * LANES
        k_ref[:, base : base + LANES] = keyval[:, base : base + NOPE]
        k_ref[:, base + LANES : base + 2 * LANES] = shared
        v_ref[:, head * VDIM : (head + 1) * VDIM] = keyval[:, base + NOPE : base + NOPE + VDIM]


def fixed(shape):
    return pl.BlockSpec(shape, lambda *_: (0,) * len(shape), pipeline_mode=pl.Buffered(1))


def by_rows(width, step=STEP):
    return pl.BlockSpec((step, width), lambda i: (i, 0))


def front(x, gain, lat_gain, cosine, sine, kvup, query_blocks, small, shards, heads):
    length, width = x.shape
    count = len(query_blocks)
    groups = small.shape[0]

    def latent_spec(r):
        return pl.BlockSpec(
            (groups, width // shards // groups, small.shape[2]),
            lambda *_: (0, r, 0),
            pipeline_mode=pl.Buffered(1),
        )

    shapes = [
        (width, jnp.bfloat16),
        (heads * 2 * LANES, jnp.bfloat16),
        (heads * 2 * LANES, jnp.bfloat16),
        (heads * VDIM, jnp.bfloat16),
        (RANK, jnp.float32),
        (RANK, jnp.bfloat16),
    ]
    return pl.pallas_call(
        functools.partial(front_kernel, heads, count, shards),
        grid=(length // STEP,),
        in_specs=[
            by_rows(width),
            fixed((1, width)),
            fixed((1, RANK)),
            by_rows(LANES),
            by_rows(LANES),
            fixed(kvup.shape),
        ]
        + [fixed(b.shape) for b in query_blocks]
        + [latent_spec(r) for r in range(shards)],
        out_specs=[by_rows(w) for w, _ in shapes],
        out_shape=[jax.ShapeDtypeStruct((length, w), d) for w, d in shapes],
        cost_estimate=pl.CostEstimate(
            flops=2 * length * width * 1100, bytes_accessed=20 * 2**20, transcendentals=0
        ),
        name="front",
    )(x, gain, lat_gain, cosine, sine, kvup, *query_blocks, *[small] * shards)


def causal(scores, span):
    row = lax.broadcasted_iota(jnp.int32, (STEP, STEP), 0)
    column = lax.broadcasted_iota(jnp.int32, (STEP, STEP), 1)
    edge = jnp.where(column <= row, scores[:, span - STEP :], MASKED)
    return edge if span == STEP else jnp.concatenate([scores[:, : span - STEP], edge], 1)


def attend_kernel(blocks, scale, q_ref, k_ref, v_ref, out_ref, log_ref):
    for block in range(blocks):

        @pl.when(pl.program_id(1) == block)
        def _(block=block):
            span = (block + 1) * STEP
            scores = causal(nt(q_ref[...], k_ref[:span]) * scale, span)
            top = jnp.max(scores, -1, keepdims=True)
            expo = jnp.exp(scores - top)
            total = jnp.sum(expo, -1, keepdims=True)
            low = (expo / total).astype(jnp.bfloat16)
            out_ref[...] = nn(low, v_ref[:span]).astype(jnp.bfloat16)
            log_ref[0] = top + jnp.log(total)


def attend(q, k, v, heads, scale):
    length = q.shape[0]
    blocks = length // STEP
    return pl.pallas_call(
        functools.partial(attend_kernel, blocks, scale),
        grid=(heads, blocks),
        in_specs=[
            pl.BlockSpec((STEP, 2 * LANES), lambda h, i: (i, h)),
            pl.BlockSpec((length, 2 * LANES), lambda h, i: (0, h)),
            pl.BlockSpec((length, VDIM), lambda h, i: (0, h)),
        ],
        out_specs=[
            pl.BlockSpec((STEP, VDIM), lambda h, i: (i, h)),
            pl.BlockSpec((1, STEP, 1), lambda h, i: (h, i, 0)),
        ],
        out_shape=[
            jax.ShapeDtypeStruct((length, heads * VDIM), jnp.bfloat16),
            jax.ShapeDtypeStruct((heads, length, 1), jnp.float32),
        ],
        cost_estimate=pl.CostEstimate(
            flops=2 * heads * length * length * 500,
            bytes_accessed=8 * 2**20,
            transcendentals=heads * length * length,
        ),
        name="attend",
    )(q, k, v)


def attend_back_kernel(
    heads, blocks, scale, q_ref, k_ref, v_ref, d_ref, log_ref, cos_ref, sin_ref,
    dq_ref, dkv_ref, rope_ref, key_sum, value_sum
):
    block_id = pl.program_id(0)

    @pl.when(block_id == 0)
    def _():
        key_sum[...] = jnp.zeros_like(key_sum)
        value_sum[...] = jnp.zeros_like(value_sum)

    for block in range(blocks):

        @pl.when(block_id == block)
        def _(block=block):
            span = (block + 1) * STEP
            tiles = []
            for head in range(heads):
                wide = slice(head * 2 * LANES, (head + 1) * 2 * LANES)
                thin = slice(head * VDIM, (head + 1) * VDIM)
                query = q_ref[:, wide]
                keys = k_ref[:span, wide]
                d_out = d_ref[:, thin]
                scores = causal(nt(query, keys) * scale, span)
                probs = jnp.exp(scores - log_ref[head])
                low = probs.astype(jnp.bfloat16)
                d_probs = nt(d_out, v_ref[:span, thin])
                centre = jnp.sum(probs * d_probs, -1, keepdims=True)
                d_scores = (probs * (d_probs - centre)).astype(jnp.bfloat16)
                d_query = nn(d_scores, keys) * scale
                key_sum[:span, wide] += tn(d_scores, query) * scale
                value_sum[:span, thin] += tn(low, d_out)
                tiles.append(
                    (
                        d_query[:, :NOPE],
                        turn(d_query[:, NOPE : NOPE + LANES], cos_ref[...], -sin_ref[...]),
                    )
                )
            dq_ref[...] = join_heads(tiles).astype(jnp.bfloat16)

    @pl.when(block_id == blocks - 1)
    def _():
        shared = None
        for head in range(heads):
            base = head * 2 * LANES
            dkv_ref[:, base : base + NOPE] = key_sum[:, base : base + NOPE].astype(jnp.bfloat16)
            dkv_ref[:, base + NOPE : base + NOPE + VDIM] = value_sum[
                :, head * VDIM : (head + 1) * VDIM
            ].astype(jnp.bfloat16)
            term = key_sum[:, base + LANES : base + 2 * LANES].astype(jnp.bfloat16)
            term = term.astype(jnp.float32)
            shared = term if shared is None else shared + term
        rope_ref[...] = shared.astype(jnp.bfloat16)


def attend_back(q, k, v, d_heads, logs, cosine, sine, heads, scale):
    length = q.shape[0]
    blocks = length // STEP
    query_width = heads * (NOPE + ROPE)
    return pl.pallas_call(
        functools.partial(attend_back_kernel, heads, blocks, scale),
        grid=(blocks,),
        in_specs=[
            by_rows(heads * 2 * LANES),
            fixed(k.shape),
            fixed(v.shape),
            by_rows(heads * VDIM),
            pl.BlockSpec((heads, STEP, 1), lambda i: (0, i, 0)),
            by_rows(LANES),
            by_rows(LANES),
        ],
        out_specs=[by_rows(query_width), fixed(k.shape), fixed((length, LANES))],
        out_shape=[
            jax.ShapeDtypeStruct((length, query_width), jnp.bfloat16),
            jax.ShapeDtypeStruct(k.shape, jnp.bfloat16),
            jax.ShapeDtypeStruct((length, LANES), jnp.bfloat16),
        ],
        scratch_shapes=[pltpu.VMEM(k.shape, jnp.float32), pltpu.VMEM(v.shape, jnp.float32)],
        cost_estimate=pl.CostEstimate(
            flops=2 * heads * length * length * 1100,
            bytes_accessed=12 * 2**20,
            transcendentals=heads * length * length,
        ),
        name="attend_back",
    )(q, k, v, d_heads, logs, cosine, sine)


def load_pieces(pieces, sems):
    copies = [
        pltpu.make_async_copy(source, target, sems.at[at])
        for at, (source, target) in enumerate(pieces)
    ]

    @pl.when(pl.program_id(0) == 0)
    def _():
        for copy in copies:
            copy.start()

    def take(low, high):
        @pl.when(pl.program_id(0) == 0)
        def _():
            for copy in copies[low:high]:
                copy.wait()

    return take


def stacked(refs, whole, columns):
    size = refs[0].shape[1 if columns else 0]
    pieces = []
    for r, ref in enumerate(refs):
        span = pl.ds(r * size, size)
        pieces.append((ref, whole.at[:, span] if columns else whole.at[span]))
    return pieces


def hidden_kernel(count, ff, *refs):
    x_ref, gate_ref = refs[:2]
    sources = refs[2 : 2 + 2 * count]
    hid_ref, a_ref, b_ref, gates, ups, sems = refs[2 + 2 * count :]
    pieces = stacked(sources[:count], gates, False) + stacked(sources[count:], ups, False)
    take = load_pieces(pieces, sems)
    take(0, len(pieces))
    total = gates.shape[1]
    x = x_ref[...]
    for low in range(0, total, CHUNK):
        high = min(low + CHUNK, total)
        gate = nn(x, gates[:, low:high])
        upper = nn(x, ups[:, low:high])
        sigma = jax.nn.sigmoid(gate)
        silu = gate * sigma
        slope = upper * sigma * (1.0 + gate * (1.0 - sigma))
        factor = gate_ref[...]
        if high > ff:
            column = lax.broadcasted_iota(jnp.int32, gate.shape, 1)
            factor = jnp.where(column < ff - low, factor, 1.0)
        hid_ref[:, low:high] = (silu * upper * factor).astype(jnp.bfloat16)
        a_ref[:, low:high] = (slope * factor).astype(jnp.bfloat16)
        b_ref[:, low:high] = (silu * factor).astype(jnp.bfloat16)


def hidden_pass(x, gate, gate_blocks, up_blocks, ff):
    length, width = x.shape
    count = len(gate_blocks)
    blocks = [*gate_blocks, *up_blocks]
    total = gate_blocks[0].shape[1]
    return pl.pallas_call(
        functools.partial(hidden_kernel, count, ff),
        grid=(length // WIDE,),
        in_specs=[by_rows(width, WIDE), by_rows(1, WIDE)]
        + [pl.BlockSpec(memory_space=pl.ANY)] * len(blocks),
        out_specs=[by_rows(total, WIDE)] * 3,
        out_shape=[jax.ShapeDtypeStruct((length, total), jnp.bfloat16)] * 3,
        scratch_shapes=[pltpu.VMEM((width, total), jnp.bfloat16)] * 2
        + [pltpu.SemaphoreType.DMA((2 * count,))],
        cost_estimate=pl.CostEstimate(
            flops=4 * length * width * total, bytes_accessed=32 * 2**20, transcendentals=0
        ),
        compiler_params=pltpu.CompilerParams(vmem_limit_bytes=60 * 2**20),
        name="hidden_pass",
    )(x, gate, *blocks)


def slope_kernel(count, *refs):
    g_ref, a_ref, b_ref = refs[:3]
    sources = refs[3 : 3 + 3 * count]
    dg_ref, du_ref, part_ref, downs, gates, ups, sems = refs[3 + 3 * count :]
    pieces = (
        stacked(sources[:count], downs, True)
        + stacked(sources[count : 2 * count], gates, False)
        + stacked(sources[2 * count :], ups, False)
    )
    take = load_pieces(pieces, sems)
    take(0, count)
    total = downs.shape[0]
    g = g_ref[...]
    for low in range(0, total, CHUNK):
        high = min(low + CHUNK, total)
        d_hidden = nt(g, downs[low:high])
        dg_ref[:, low:high] = (d_hidden * a_ref[:, low:high].astype(jnp.float32)).astype(
            jnp.bfloat16
        )
        du_ref[:, low:high] = (d_hidden * b_ref[:, low:high].astype(jnp.float32)).astype(
            jnp.bfloat16
        )
    take(count, len(pieces))
    d_gate, d_up = dg_ref[...], du_ref[...]
    width = g.shape[1]
    for low in range(0, width, CHUNK):
        high = min(low + CHUNK, width)
        part_ref[:, low:high] = (nt(d_gate, gates[low:high]) + nt(d_up, ups[low:high])).astype(
            jnp.bfloat16
        )


def slope_pass(g, a, b, down_blocks, gate_blocks, up_blocks):
    length, width = g.shape
    count = len(gate_blocks)
    blocks = [*down_blocks, *gate_blocks, *up_blocks]
    total = gate_blocks[0].shape[1]
    return pl.pallas_call(
        functools.partial(slope_kernel, count),
        grid=(length // NARROW,),
        in_specs=[by_rows(width, NARROW), by_rows(total, NARROW), by_rows(total, NARROW)]
        + [pl.BlockSpec(memory_space=pl.ANY)] * len(blocks),
        out_specs=[by_rows(total, NARROW), by_rows(total, NARROW), by_rows(width, NARROW)],
        out_shape=[
            jax.ShapeDtypeStruct((length, total), jnp.bfloat16),
            jax.ShapeDtypeStruct((length, total), jnp.bfloat16),
            jax.ShapeDtypeStruct((length, width), jnp.bfloat16),
        ],
        scratch_shapes=[
            pltpu.VMEM((total, width), jnp.bfloat16),
            pltpu.VMEM((width, total), jnp.bfloat16),
            pltpu.VMEM((width, total), jnp.bfloat16),
            pltpu.SemaphoreType.DMA((3 * count,)),
        ],
        cost_estimate=pl.CostEstimate(
            flops=6 * length * width * total, bytes_accessed=40 * 2**20, transcendentals=0
        ),
        compiler_params=pltpu.CompilerParams(vmem_limit_bytes=62 * 2**20),
        name="slope_pass",
    )(g, a, b, *blocks)


def rotate(values, cosine, sine):
    half_depth = values.shape[-1] // 2
    first = values[..., :half_depth]
    second = values[..., half_depth:]
    return jnp.concatenate([first * cosine - second * sine, second * cosine + first * sine], -1)


def norm_forward(values, scaling):
    inverse = lax.rsqrt(jnp.mean(values * values, -1, keepdims=True) + EPSILON)
    return (values * inverse * scaling, inverse)


def norm_backward(values, inverse, scaling, upstream):
    weighted = upstream * scaling
    scaling_grad = jnp.sum(upstream * values * inverse, 0)
    centre = jnp.mean(weighted * values, -1, keepdims=True)
    return (inverse * weighted - values * inverse**3 * centre, scaling_grad)


def gather_seq(block):
    return lax.all_gather(block, "seq", axis=0, tiled=True)


def scatter_seq(partial):
    return lax.psum_scatter(
        partial.astype(jnp.bfloat16), "seq", scatter_dimension=0, tiled=True
    ).astype(jnp.float32)


def settle_kernel(n, shards, terms_ref, out_ref, from_seq, joined, from_shard, sends, seq_recv, shard_recv):
    me = lax.axis_index("seq")
    my_shard = lax.axis_index("shard")
    barrier = pltpu.get_barrier_semaphore()
    for hop in range(1, n):
        pl.semaphore_signal(
            barrier, inc=1, device_id={"seq": (me + hop) % n}, device_id_type=MESH
        )
    for hop in range(1, shards):
        pl.semaphore_signal(
            barrier, inc=1, device_id={"shard": (my_shard + hop) % shards}, device_id_type=MESH
        )
    pl.semaphore_wait(barrier, n + shards - 2)
    first = []
    for hop in range(1, n):
        target = (me + hop) % n
        copy = pltpu.make_async_remote_copy(
            src_ref=terms_ref.at[target],
            dst_ref=from_seq.at[hop - 1],
            send_sem=sends.at[hop - 1],
            recv_sem=seq_recv.at[hop - 1],
            device_id={"seq": target},
            device_id_type=MESH,
        )
        copy.start()
        first.append(copy)
    total = terms_ref[me]
    for hop in range(1, n):
        first[hop - 1].wait_recv()
        total = total + from_seq[hop - 1]
    joined[...] = total
    second = []
    for hop in range(1, shards):
        target = (my_shard + hop) % shards
        copy = pltpu.make_async_remote_copy(
            src_ref=joined.at[target],
            dst_ref=from_shard.at[hop - 1],
            send_sem=sends.at[n - 1 + hop - 1],
            recv_sem=shard_recv.at[hop - 1],
            device_id={"shard": target},
            device_id_type=MESH,
        )
        copy.start()
        second.append(copy)
    total = joined[my_shard]
    for hop in range(1, shards):
        second[hop - 1].wait_recv()
        total = total + from_shard[hop - 1]
    out_ref[...] = total
    for copy in first + second:
        copy.wait_send()


def settle(n, shards, terms, identity):
    shape = terms.shape[2:]
    return pl.pallas_call(
        functools.partial(settle_kernel, n, shards),
        out_shape=jax.ShapeDtypeStruct(shape, jnp.float32),
        in_specs=[pl.BlockSpec(memory_space=pltpu.VMEM)],
        out_specs=pl.BlockSpec(memory_space=pltpu.VMEM),
        scratch_shapes=[
            pltpu.VMEM((n - 1, shards) + shape, jnp.float32),
            pltpu.VMEM((shards,) + shape, jnp.float32),
            pltpu.VMEM((shards - 1,) + shape, jnp.float32),
            pltpu.SemaphoreType.DMA((n + shards - 2,)),
            pltpu.SemaphoreType.DMA((n - 1,)),
            pltpu.SemaphoreType.DMA((shards - 1,)),
        ],
        compiler_params=pltpu.CompilerParams(collective_id=identity, has_side_effects=True),
        name="settle",
    )(terms)


def duplex_kernel(n, parts, x_ref, part_ref, all_ref, sum_ref, mine, other, left_in, right_in,
                  pair_send, pair_recv, line_send, line_recv, copy_send, copy_recv, local):
    half = n // 2
    me = lax.axis_index("seq")
    core = me % 2
    place = me // 2
    partner = place * 2 + 1 - core
    below, above = me - 2, me + 2
    has_below, has_above = place > 0, place < half - 1

    def remote(source, target, send, recv, device):
        return pltpu.make_async_remote_copy(
            src_ref=source,
            dst_ref=target,
            send_sem=send,
            recv_sem=recv,
            device_id={"seq": device},
            device_id_type=MESH,
        )

    def pair_copy(at):
        return remote(
            part_ref.at[at * 2 + 1 - core], other.at[at], pair_send.at[at], pair_recv.at[at], partner
        )

    piece = x_ref.shape[0] // parts

    def rows_of(part):
        return pl.ds(part * piece, piece)

    def sum_up(at, part):
        span = rows_of(part)
        return remote(
            mine.at[at, span],
            left_in.at[at, span],
            line_send.at[0, at, part],
            line_recv.at[0, at, part],
            above,
        )

    def sum_down(at, part):
        span = rows_of(part)
        return remote(
            mine.at[at, span],
            right_in.at[at, span],
            line_send.at[1, at, part],
            line_recv.at[1, at, part],
            below,
        )

    def block_copy(source, block, way, step, part, device):
        span = rows_of(part)
        return remote(
            source.at[span],
            all_ref.at[block, span],
            copy_send.at[way, step, part],
            copy_recv.at[way, step, part],
            device,
        )

    order = []
    for at in range(half):
        for item in (half - 1 - at, at):
            if item not in order:
                order.append(item)
    for at in order:
        pltpu.make_async_copy(part_ref.at[at * 2 + core], mine.at[at], local.at[at]).start()
    keep = pltpu.make_async_copy(x_ref, all_ref.at[me], local.at[half])
    keep.start()

    barrier = pltpu.get_barrier_semaphore()
    pl.semaphore_signal(barrier, inc=1, device_id={"seq": partner}, device_id_type=MESH)

    @pl.when(has_below)
    def _():
        pl.semaphore_signal(barrier, inc=1, device_id={"seq": below}, device_id_type=MESH)

    @pl.when(has_above)
    def _():
        pl.semaphore_signal(barrier, inc=1, device_id={"seq": above}, device_id_type=MESH)

    @pl.when(has_below & has_above)
    def _():
        pl.semaphore_wait(barrier, 3)

    @pl.when(jnp.logical_not(has_below & has_above))
    def _():
        pl.semaphore_wait(barrier, 2)

    for at in order:
        pair_copy(at).start()

    for part in range(parts):

        @pl.when(has_above)
        def _():
            block_copy(x_ref, me, 0, 0, part, above).start()

        @pl.when(has_below)
        def _():
            block_copy(x_ref, me, 1, 0, part, below).start()

        block_copy(x_ref, me, 2, 0, part, partner).start()

    def merge(at, part, incoming):
        span = rows_of(part)
        total = mine[at, span].astype(jnp.float32) + other[at, span].astype(jnp.float32)
        if incoming is not None:
            total = total + incoming[at, span].astype(jnp.float32)
        mine[at, span] = total.astype(mine.dtype)

    def load(at):
        return pltpu.make_async_copy(part_ref.at[at * 2 + core], mine.at[at], local.at[at])

    def ready(at):
        load(at).wait()
        pair_copy(at).wait_recv()

    def relay(slot, part):
        step = slot - 1

        @pl.when(place > step)
        def _():
            block = me - 2 * (step + 1)
            block_copy(x_ref, block, 0, step, part, above).wait_recv()

            @pl.when(has_above)
            def _():
                block_copy(all_ref.at[block], block, 0, step + 1, part, above).start()

            block_copy(all_ref.at[block], block, 2, 1 + step, part, partner).start()

        @pl.when(place < half - 1 - step)
        def _():
            block = me + 2 * (step + 1)
            block_copy(x_ref, block, 1, step, part, below).wait_recv()

            @pl.when(has_below)
            def _():
                block_copy(all_ref.at[block], block, 1, step + 1, part, below).start()

            block_copy(all_ref.at[block], block, 2, half + step, part, partner).start()

    for slot in range(2 * half - 2):
        rise = half - 1 - (slot - place)
        fall = slot - (half - 1 - place)
        if 1 <= slot <= half - 1:
            for part in range(parts):
                relay(slot, part)

        @pl.when((rise < half) & (rise > place))
        def _():
            ready(rise)
            for part in range(parts):

                @pl.when(has_below)
                def _():
                    sum_up(rise, part).wait_recv()
                    merge(rise, part, left_in)

                @pl.when(jnp.logical_not(has_below))
                def _():
                    merge(rise, part, None)

                sum_up(rise, part).start()

        @pl.when((fall >= 0) & (fall < place))
        def _():
            ready(fall)
            for part in range(parts):

                @pl.when(has_above)
                def _():
                    sum_down(fall, part).wait_recv()
                    merge(fall, part, right_in)

                @pl.when(jnp.logical_not(has_above))
                def _():
                    merge(fall, part, None)

                sum_down(fall, part).start()

    ready(place)
    for part in range(parts):

        @pl.when(has_below)
        def _():
            sum_up(place, part).wait_recv()

        @pl.when(has_above)
        def _():
            sum_down(place, part).wait_recv()

    total = mine[place].astype(jnp.float32) + other[place].astype(jnp.float32)
    low = jnp.where(has_below, left_in[place].astype(jnp.float32), 0.0)
    high = jnp.where(has_above, right_in[place].astype(jnp.float32), 0.0)
    sum_ref[...] = total + low + high

    keep.wait()
    for at in range(half):
        pair_copy(at).wait_send()
    for part in range(parts):
        block_copy(x_ref, partner, 2, 0, part, partner).wait_recv()
        block_copy(x_ref, me, 2, 0, part, partner).wait_send()

        @pl.when(has_above)
        def _():
            block_copy(x_ref, me, 0, 0, part, above).wait_send()

        @pl.when(has_below)
        def _():
            block_copy(x_ref, me, 1, 0, part, below).wait_send()

        for step in range(half - 1):
            up, down = half - 1 - step, step

            @pl.when(place < up)
            def _():
                sum_up(up, part).wait_send()

            @pl.when(place > down)
            def _():
                sum_down(down, part).wait_send()

            @pl.when(place > step)
            def _():
                block = me - 2 * (step + 1)

                @pl.when(has_above)
                def _():
                    block_copy(x_ref, block, 0, step + 1, part, above).wait_send()

                block_copy(x_ref, block, 2, 1 + step, part, partner).wait_send()
                there = partner - 2 * (step + 1)
                block_copy(x_ref, there, 2, 1 + step, part, partner).wait_recv()

            @pl.when(place < half - 1 - step)
            def _():
                block = me + 2 * (step + 1)

                @pl.when(has_below)
                def _():
                    block_copy(x_ref, block, 1, step + 1, part, below).wait_send()

                block_copy(x_ref, block, 2, half + step, part, partner).wait_send()
                there = partner + 2 * (step + 1)
                block_copy(x_ref, there, 2, half + step, part, partner).wait_recv()


def duplex(n, block, partial, identity, parts=2):
    half = n // 2
    rows, wide = partial.shape[0] // n, partial.shape[1]
    line = pltpu.VMEM((half, rows, wide), partial.dtype)
    gathered, total = pl.pallas_call(
        functools.partial(duplex_kernel, n, parts),
        out_shape=[
            jax.ShapeDtypeStruct((n,) + block.shape, block.dtype),
            jax.ShapeDtypeStruct((rows, wide), jnp.float32),
        ],
        in_specs=[
            pl.BlockSpec(memory_space=pltpu.VMEM),
            pl.BlockSpec(memory_space=pl.ANY),
        ],
        out_specs=[
            pl.BlockSpec(memory_space=pl.ANY),
            pl.BlockSpec(memory_space=pltpu.VMEM),
        ],
        scratch_shapes=[
            line,
            line,
            line,
            line,
            pltpu.SemaphoreType.DMA((half,)),
            pltpu.SemaphoreType.DMA((half,)),
            pltpu.SemaphoreType.DMA((2, half, parts)),
            pltpu.SemaphoreType.DMA((2, half, parts)),
            pltpu.SemaphoreType.DMA((3, 2 * half, parts)),
            pltpu.SemaphoreType.DMA((3, 2 * half, parts)),
            pltpu.SemaphoreType.DMA((half + 1,)),
        ],
        compiler_params=pltpu.CompilerParams(collective_id=identity, has_side_effects=True),
        cost_estimate=pl.CostEstimate(
            flops=45_000_000_000, bytes_accessed=2**24, transcendentals=0
        ),
        name="duplex",
    )(block, partial.reshape(n, rows, wide))
    return gathered.reshape(n * block.shape[0], block.shape[1]), total


ACROSS = ([(0, 1), (1, 0), (2, 3), (3, 2)], [(0, 2), (2, 0), (1, 3), (3, 1)])


def swap_with(block, side):
    return lax.ppermute(block, "shard", ACROSS[side])


def gather_blocks(weight, axis, side):
    if lax.axis_size("shard") != 4:
        return [lax.all_gather(weight, "shard", axis=axis, tiled=True)]
    near = [swap_with(weight, 0), swap_with(weight, 1)]
    far = swap_with(near[side], 1 - side)
    return [weight, near[0], near[1], far]


def after(value, token):
    return lax.optimization_barrier((value, token))[0]


def scatter_blocks(blocks, axis, side, join_token, sum_token):
    if lax.axis_size("shard") != 4:
        return (lax.psum_scatter(blocks[0], "shard", scatter_dimension=axis, tiled=True),)
    blocks = [lax.optimization_barrier(block) for block in blocks]
    far = swap_with(blocks[3], side)
    first = swap_with(blocks[1 + side], side)
    far = after(far, join_token)
    joined = (blocks[2 - side].astype(jnp.float32) + far.astype(jnp.float32)).astype(
        jnp.bfloat16
    )
    second = swap_with(joined, 1 - side)
    second = after(second, sum_token)
    return blocks[0], first, second


def add_up(terms, rows=slice(None), columns=slice(None)):
    total = None
    for term in terms:
        term = term[rows, columns].astype(jnp.float32)
        total = term if total is None else total + term
    return total


def local_order(values, axis):
    if lax.axis_size("shard") != 4:
        return values
    size = values.shape[axis] // 4
    shard = lax.axis_index("shard")
    return jnp.concatenate(
        [
            lax.dynamic_slice_in_dim(values, jnp.bitwise_xor(shard, place) * size, size, axis)
            for place in range(4)
        ],
        axis,
    )


def cut(values, axis):
    if lax.axis_size("shard") != 4:
        return [values]
    size = values.shape[axis] // 4
    return [lax.slice_in_dim(values, r * size, (r + 1) * size, axis=axis) for r in range(4)]


def on_device(
    inputs,
    attn_gain,
    query_project_weight,
    latent_project_weight,
    latent_gain,
    latent_keyval_weight,
    attention_output_weight,
    ffn_gain,
    shared_gate,
    shared_up,
    shared_down,
    expert_gate,
    expert_up,
    expert_down,
    routes,
    slots,
    gates,
    cotangent,
):
    tok_rows = inputs.shape[1]
    model_width = inputs.shape[2]
    groups = lax.axis_size("seq")
    shards = lax.axis_size("shard")
    me = lax.axis_index("seq")
    heads = HEADS // groups
    experts = EXP_DEV * groups
    capacity = 9 * tok_rows * TOPK // (8 * experts)
    length = tok_rows * groups
    score_scale = (NOPE + ROPE) ** (-0.5)
    own_start = me * tok_rows
    one_width = attn_gain.shape[0]
    lat_width = latent_gain.shape[0]
    ff = expert_gate.shape[2]
    shared_ff = shared_gate.shape[1]
    side = -(-shared_ff // LANES) * LANES

    own_inputs = local_order(inputs.reshape(tok_rows, model_width), 1)
    inputs_all = gather_seq(own_inputs)
    upstream = local_order(cotangent.reshape(tok_rows, model_width), 1)
    route_rows = routes.reshape(tok_rows, TOPK)
    slot_rows = slots.reshape(tok_rows, TOPK)
    kept = (route_rows.T[:, None, :] == jnp.arange(experts)[None, :, None]) & (
        slot_rows.T < capacity
    )[:, None, :]
    gate_table = jnp.sum(
        jnp.where(kept, gates.reshape(tok_rows, TOPK).T.astype(jnp.float32)[:, None, :], 0.0), 0
    ).astype(jnp.bfloat16)

    def padded_row(gain):
        return jnp.pad(gain, (0, LANES - ROPE - gain.shape[0]))[None]

    side_rows = jnp.concatenate(
        [
            padded_row(attn_gain),
            padded_row(ffn_gain),
            padded_row(latent_gain),
            jnp.zeros((one_width - 3, LANES - ROPE), jnp.bfloat16),
        ],
        0,
    )
    small_own = jnp.concatenate([latent_project_weight, side_rows], 1)
    small_rows = jnp.concatenate(gather_blocks(small_own, 0, 0), 0)
    small_rows = jnp.concatenate(
        [
            small_rows,
            jnp.pad(gate_table, ((0, EXTRA - experts), (0, small_rows.shape[1] - tok_rows))),
        ],
        0,
    )
    small_seq = gather_seq(small_rows).reshape(groups, shards * one_width + EXTRA, -1)
    gate_column = (
        lax.dynamic_index_in_dim(
            small_seq[:, shards * one_width :, :tok_rows], me, 1, keepdims=False
        )
        .reshape(length, 1)
        .astype(jnp.float32)
    )
    gain_rows = (
        small_seq[:, : shards * one_width, RANK + ROPE :]
        .reshape(groups, shards, one_width, -1)[:, :, :3]
        .astype(jnp.float32)
        .transpose(2, 1, 0, 3)
    )
    first_norm_weight = gain_rows[0, :, :, :one_width].reshape(-1)
    second_norm_weight = gain_rows[1, :, :, :one_width].reshape(-1)
    latent_norm_weight = local_order(gain_rows[2, :, :, :lat_width].reshape(-1), 0)

    spare = side - shared_ff
    query_blocks = gather_blocks(query_project_weight, 0, 0)
    kvup_blocks = gather_blocks(latent_keyval_weight, 0, 0)
    out_blocks = gather_blocks(attention_output_weight, 1, 0)
    gate_blocks = gather_blocks(
        jnp.pad(jnp.concatenate([expert_gate[0], shared_gate], 1), ((0, 0), (0, spare))), 0, 0
    )
    up_blocks = gather_blocks(
        jnp.pad(jnp.concatenate([expert_up[0], shared_up], 1), ((0, 0), (0, spare))), 0, 1
    )
    down_blocks = gather_blocks(
        jnp.pad(jnp.concatenate([expert_down[0], shared_down], 0), ((0, spare), (0, 0))), 1, 1
    )
    full_query = jnp.concatenate(query_blocks, 0)
    full_kvup = local_order(jnp.concatenate(kvup_blocks, 0), 0)
    full_out = jnp.concatenate(out_blocks, 1)

    residual_stream = own_inputs.astype(jnp.float32)
    cosine, sine = rope_lanes(jnp.arange(length))
    first_all, q_all, k_all, v_all, latent, latent_all = front(
        inputs_all,
        first_norm_weight[None],
        latent_norm_weight[None],
        cosine,
        sine,
        full_kvup,
        query_blocks,
        small_seq,
        shards,
        heads,
    )
    attended, logs = attend(q_all, k_all, v_all, heads, score_scale)
    attended_part = nn(attended, full_out)
    upstream_all, attended_sum = duplex(groups, upstream, attended_part.astype(jnp.bfloat16), 1)
    middle = residual_stream + attended_sum
    normed_two, inv_two = norm_forward(middle, second_norm_weight)
    second_all = gather_seq(normed_two.astype(jnp.bfloat16))

    hidden, slope_gate, slope_up = hidden_pass(second_all, gate_column, gate_blocks, up_blocks, ff)
    d_gate, d_up, second_part = slope_pass(
        upstream_all, slope_gate, slope_up, down_blocks, gate_blocks, up_blocks
    )
    d_second = scatter_seq(second_part)
    hidden_late = after(hidden, d_gate)
    d_down = [tn(hidden_late, part).astype(jnp.bfloat16) for part in cut(upstream_all, 1)]
    second_parts = cut(second_all, 1)
    d_wgate = [tn(part, d_gate).astype(jnp.bfloat16) for part in second_parts]
    d_wup = [tn(part, d_up).astype(jnp.bfloat16) for part in second_parts]
    down_part = nn(hidden, jnp.concatenate(down_blocks, 1)).astype(jnp.bfloat16)

    d_middle_norm, d_gain_two = norm_backward(middle, inv_two, second_norm_weight, d_second)
    d_middle = upstream.astype(jnp.float32) + d_middle_norm
    d_branch_all, added = duplex(groups, d_middle.astype(jnp.bfloat16), down_part, 2)
    output = local_order((middle + added).astype(jnp.bfloat16), 1).reshape(
        1, tok_rows, model_width
    )
    d_heads = nt(d_branch_all, full_out).astype(jnp.bfloat16)
    d_query, d_keyval, d_shared_key = attend_back(
        q_all, k_all, v_all, d_heads, logs, cosine, sine, heads, score_scale
    )
    latent_part = nt(d_keyval, full_kvup).astype(jnp.bfloat16)
    latent_back = scatter_seq(jnp.concatenate([latent_part, d_shared_key], 1))
    first_part = nt(d_query, full_query)
    first_back = scatter_seq(first_part)
    d_wout = [tn(attended, part).astype(jnp.bfloat16) for part in cut(d_branch_all, 1)]
    d_wquery = [tn(part, d_query).astype(jnp.bfloat16) for part in cut(first_all, 1)]
    d_wkvup = cut(local_order(tn(latent_all, d_keyval).astype(jnp.bfloat16), 0), 0)

    own_latent = lax.dynamic_slice_in_dim(latent, own_start, tok_rows, 0)
    half = ROPE // 2
    cos_own = lax.dynamic_slice_in_dim(cosine, own_start, tok_rows, 0)[:, :half]
    sin_own = lax.dynamic_slice_in_dim(sine, own_start, tok_rows, 0)[:, half:ROPE]
    inv_latent = norm_forward(own_latent, latent_norm_weight)[1]
    d_rope = rotate(latent_back[:, RANK : RANK + ROPE], cos_own, -sin_own)
    d_compressed, d_gain_latent = norm_backward(
        own_latent, inv_latent, latent_norm_weight, latent_back[:, :RANK]
    )
    d_latent = jnp.concatenate(
        [d_compressed, d_rope, jnp.zeros((tok_rows, LANES - ROPE), jnp.float32)], -1
    ).astype(jnp.bfloat16)
    d_latent_all = gather_seq(d_latent)
    inv_one = norm_forward(residual_stream, first_norm_weight)[1]
    d_first = first_back + jnp.concatenate(
        [
            nt(
                d_latent,
                small_seq[:, r * one_width : (r + 1) * one_width].reshape(groups * one_width, -1),
            )
            for r in range(shards)
        ],
        1,
    )
    d_resid, d_gain_one = norm_backward(residual_stream, inv_one, first_norm_weight, d_first)
    input_grad = local_order(d_middle + d_resid, 1).reshape(1, tok_rows, model_width)
    first_late = after(first_all, d_latent)
    own_columns = jnp.concatenate(
        [
            lax.dynamic_slice_in_dim(
                first_late, (place * groups + me) * one_width, one_width, 1
            )
            for place in range(shards)
        ],
        1,
    )
    d_wlatent = cut(tn(own_columns, d_latent_all).astype(jnp.bfloat16), 0)

    devices = shards * groups
    terms = jnp.concatenate(
        [
            local_order(d_gain_one, 0).reshape(devices, one_width),
            local_order(d_gain_two, 0).reshape(devices, one_width),
            d_gain_latent.reshape(devices, lat_width),
        ],
        1,
    )
    terms = jnp.pad(terms, ((0, 0), (0, 1024 - terms.shape[1]))).reshape(shards, groups, 8, 128)
    gain_grads = settle(groups, shards, terms.transpose(1, 0, 2, 3), 9).reshape(-1)
    gate_grad = scatter_blocks(d_wgate, 0, 0, d_keyval, gain_grads)
    up_grad = scatter_blocks(d_wup, 0, 1, d_keyval, gain_grads)
    down_grad = scatter_blocks(d_down, 1, 0, second_part, gain_grads)
    out_grad = scatter_blocks(d_wout, 1, 1, first_back, gain_grads)
    kvup_grad = scatter_blocks(d_wkvup, 0, 1, first_back, gain_grads)
    query_grad = scatter_blocks(d_wquery, 0, 1, first_back, gain_grads)
    latent_grad = scatter_blocks(d_wlatent, 0, 1, first_back, first_back)
    return (
        output,
        input_grad,
        gain_grads[:one_width],
        add_up(query_grad),
        add_up(latent_grad, columns=slice(0, RANK + ROPE)),
        gain_grads[2 * one_width : 2 * one_width + lat_width],
        add_up(kvup_grad),
        add_up(out_grad),
        gain_grads[one_width : 2 * one_width],
        add_up(gate_grad, columns=slice(ff, ff + shared_ff)),
        add_up(up_grad, columns=slice(ff, ff + shared_ff)),
        add_up(down_grad, rows=slice(ff, ff + shared_ff)),
        add_up(gate_grad, columns=slice(0, ff))[None],
        add_up(up_grad, columns=slice(0, ff))[None],
        add_up(down_grad, rows=slice(0, ff))[None],
    )


def solution(mesh):
    in_specs = (
        P("shard", "seq", None),
        P(("shard", "seq")),
        P("shard", "seq"),
        P(("shard", "seq"), None),
        P(("shard", "seq")),
        P("shard", "seq"),
        P("seq", "shard"),
        P(("shard", "seq")),
        P("shard", "seq"),
        P("shard", "seq"),
        P("seq", "shard"),
        P("seq", "shard", None),
        P("seq", "shard", None),
        P("seq", None, "shard"),
        P("shard", "seq", None),
        P("shard", "seq", None),
        P("shard", "seq", None),
        P("shard", "seq", None),
    )
    out_specs = (
        P("shard", "seq", None),
        P("shard", "seq", None),
        P(("shard", "seq")),
        P("shard", "seq"),
        P(("shard", "seq"), None),
        P(("shard", "seq")),
        P("shard", "seq"),
        P("seq", "shard"),
        P(("shard", "seq")),
        P("shard", "seq"),
        P("shard", "seq"),
        P("seq", "shard"),
        P("seq", "shard", None),
        P("seq", "shard", None),
        P("seq", None, "shard"),
    )

    return jax.shard_map(
        on_device, mesh=mesh, in_specs=in_specs, out_specs=out_specs, check_vma=False
    )
```

```python
import functools

import jax
import jax.numpy as jnp
from jax import lax
from jax.experimental import pallas as pl
from jax.experimental.pallas import tpu as pltpu
from jax.sharding import PartitionSpec as P

HEADS = 16
NOPE = 128
ROPE = 64
VDIM = 128
RANK = 512
TOPK = 6
EXP_DEV = 1
EXTRA = 32


EPSILON = 1e-06
THETA = 10000.0
MASKED = -1e30
SHARD = "shard"
SEQ = "seq"
MESH = pl.DeviceIdType.MESH


LANES = 128
STEP = 256
WIDE = 512
NARROW = 512
CHUNK = 512


def nn(left, right):
    return jnp.dot(left, right, preferred_element_type=jnp.float32)


def nt(left, right):
    return lax.dot_general(
        left, right, (((1,), (1,)), ((), ())), preferred_element_type=jnp.float32
    )


def tn(left, right):
    return lax.dot_general(
        left, right, (((0,), (0,)), ((), ())), preferred_element_type=jnp.float32
    )


def lane_index(rows):
    return lax.broadcasted_iota(jnp.int32, (rows, LANES), 1)


def turn(tile, cosine, sine):
    lane = lane_index(tile.shape[0])
    low = pltpu.roll(tile, LANES - ROPE // 2, 1)
    high = pltpu.roll(tile, ROPE // 2, 1)
    return tile * cosine + jnp.where(lane < ROPE // 2, low, high) * sine


def rope_lanes(positions):
    half = ROPE // 2
    frequency = THETA ** (-(2.0 * jnp.arange(half, dtype=jnp.float32)) / ROPE)
    angles = positions.astype(jnp.float32)[:, None] * frequency[None, :]
    cosine, sine = jnp.cos(angles), jnp.sin(angles)
    blank = jnp.zeros((positions.shape[0], LANES - ROPE), jnp.float32)
    return (
        jnp.concatenate([cosine, cosine, blank], 1),
        jnp.concatenate([-sine, sine, blank], 1),
    )


def split_heads(values, heads):
    width = NOPE + ROPE
    rows = values.shape[0]
    keep = lane_index(rows) < ROPE
    tiles = []
    for head in range(heads):
        part = values if head == 0 else pltpu.roll(values, (heads - head) * width, 1)
        if part.shape[1] >= 2 * LANES:
            turned = jnp.where(keep, part[:, NOPE : NOPE + LANES], 0.0)
        else:
            turned = jnp.concatenate(
                [part[:, NOPE:], jnp.zeros((rows, LANES - ROPE), part.dtype)], 1
            )
        tiles.append((part[:, :NOPE], turned))
    return tiles


def join_heads(tiles):
    heads = len(tiles)
    width = NOPE + ROPE
    if heads == 1:
        return jnp.concatenate([tiles[0][0], tiles[0][1][:, :ROPE]], 1)
    rows = tiles[0][0].shape[0]
    blank = jnp.zeros((rows, heads * width - 2 * LANES), jnp.float32)
    total = None
    for head, (plain, turned) in enumerate(tiles):
        part = jnp.concatenate([plain, turned, blank], 1)
        part = part if head == 0 else pltpu.roll(part, head * width, 1)
        total = part if total is None else total + part
    return total


def front_kernel(heads, count, shards, *refs):
    x_ref, gain_ref, lat_gain_ref, cos_ref, sin_ref, kvup_ref = refs[:6]
    query_refs = refs[6 : 6 + count]
    latent_refs = refs[6 + count : 6 + count + shards]
    first_ref, q_ref, k_ref, v_ref, latent_ref, low_ref = refs[6 + count + shards :]
    values = x_ref[...].astype(jnp.float32)
    inverse = lax.rsqrt(jnp.mean(values * values, -1, keepdims=True) + EPSILON)
    first = (values * inverse * gain_ref[...]).astype(jnp.bfloat16)
    first_ref[...] = first
    depth = query_refs[0].shape[0]
    query = None
    latent = None
    for r in range(count):
        term = nn(first[:, r * depth : (r + 1) * depth], query_refs[r][...])
        query = term if query is None else query + term
    depth = first.shape[1] // shards
    for r in range(shards):
        weight = latent_refs[r][...].reshape(depth, latent_refs[r].shape[2])
        term = nn(first[:, r * depth : (r + 1) * depth], weight)
        latent = term if latent is None else latent + term
    cosine, sine = cos_ref[...], sin_ref[...]
    for head, (plain, turned) in enumerate(split_heads(query, heads)):
        base = head * 2 * LANES
        q_ref[:, base : base + LANES] = plain.astype(jnp.bfloat16)
        q_ref[:, base + LANES : base + 2 * LANES] = turn(turned, cosine, sine).astype(
            jnp.bfloat16
        )
    packed = latent[:, :RANK]
    latent_ref[...] = packed
    inverse = lax.rsqrt(jnp.mean(packed * packed, -1, keepdims=True) + EPSILON)
    low = (packed * inverse * lat_gain_ref[...]).astype(jnp.bfloat16)
    low_ref[...] = low
    shared = jnp.where(
        lane_index(packed.shape[0]) < ROPE, latent[:, RANK : RANK + LANES], 0.0
    )
    shared = turn(shared, cosine, sine).astype(jnp.bfloat16)
    keyval = nn(low, kvup_ref[...]).astype(jnp.bfloat16)
    for head in range(heads):
        base = head * 2 * LANES
        k_ref[:, base : base + LANES] = keyval[:, base : base + NOPE]
        k_ref[:, base + LANES : base + 2 * LANES] = shared
        v_ref[:, head * VDIM : (head + 1) * VDIM] = keyval[:, base + NOPE : base + NOPE + VDIM]


def fixed(shape):
    return pl.BlockSpec(shape, lambda *_: (0,) * len(shape), pipeline_mode=pl.Buffered(1))


def by_rows(width, step=STEP):
    return pl.BlockSpec((step, width), lambda i: (i, 0))


def front(x, gain, lat_gain, cosine, sine, kvup, query_blocks, small, shards, heads):
    length, width = x.shape
    count = len(query_blocks)
    groups = small.shape[0]

    def latent_spec(r):
        return pl.BlockSpec(
            (groups, width // shards // groups, small.shape[2]),
            lambda *_: (0, r, 0),
            pipeline_mode=pl.Buffered(1),
        )

    shapes = [
        (width, jnp.bfloat16),
        (heads * 2 * LANES, jnp.bfloat16),
        (heads * 2 * LANES, jnp.bfloat16),
        (heads * VDIM, jnp.bfloat16),
        (RANK, jnp.float32),
        (RANK, jnp.bfloat16),
    ]
    return pl.pallas_call(
        functools.partial(front_kernel, heads, count, shards),
        grid=(length // STEP,),
        in_specs=[
            by_rows(width),
            fixed((1, width)),
            fixed((1, RANK)),
            by_rows(LANES),
            by_rows(LANES),
            fixed(kvup.shape),
        ]
        + [fixed(b.shape) for b in query_blocks]
        + [latent_spec(r) for r in range(shards)],
        out_specs=[by_rows(w) for w, _ in shapes],
        out_shape=[jax.ShapeDtypeStruct((length, w), d) for w, d in shapes],
        cost_estimate=pl.CostEstimate(
            flops=2 * length * width * 1100, bytes_accessed=20 * 2**20, transcendentals=0
        ),
        name="front",
    )(x, gain, lat_gain, cosine, sine, kvup, *query_blocks, *[small] * shards)


def causal(scores, span):
    row = lax.broadcasted_iota(jnp.int32, (STEP, STEP), 0)
    column = lax.broadcasted_iota(jnp.int32, (STEP, STEP), 1)
    edge = jnp.where(column <= row, scores[:, span - STEP :], MASKED)
    return edge if span == STEP else jnp.concatenate([scores[:, : span - STEP], edge], 1)


def attend_kernel(blocks, scale, q_ref, k_ref, v_ref, out_ref, log_ref):
    for block in range(blocks):

        @pl.when(pl.program_id(1) == block)
        def _(block=block):
            span = (block + 1) * STEP
            scores = causal(nt(q_ref[...], k_ref[:span]) * scale, span)
            top = jnp.max(scores, -1, keepdims=True)
            expo = jnp.exp(scores - top)
            total = jnp.sum(expo, -1, keepdims=True)
            low = (expo / total).astype(jnp.bfloat16)
            out_ref[...] = nn(low, v_ref[:span]).astype(jnp.bfloat16)
            log_ref[0] = top + jnp.log(total)


def attend(q, k, v, heads, scale):
    length = q.shape[0]
    blocks = length // STEP
    return pl.pallas_call(
        functools.partial(attend_kernel, blocks, scale),
        grid=(heads, blocks),
        in_specs=[
            pl.BlockSpec((STEP, 2 * LANES), lambda h, i: (i, h)),
            pl.BlockSpec((length, 2 * LANES), lambda h, i: (0, h)),
            pl.BlockSpec((length, VDIM), lambda h, i: (0, h)),
        ],
        out_specs=[
            pl.BlockSpec((STEP, VDIM), lambda h, i: (i, h)),
            pl.BlockSpec((1, STEP, 1), lambda h, i: (h, i, 0)),
        ],
        out_shape=[
            jax.ShapeDtypeStruct((length, heads * VDIM), jnp.bfloat16),
            jax.ShapeDtypeStruct((heads, length, 1), jnp.float32),
        ],
        cost_estimate=pl.CostEstimate(
            flops=2 * heads * length * length * 500,
            bytes_accessed=8 * 2**20,
            transcendentals=heads * length * length,
        ),
        name="attend",
    )(q, k, v)


def attend_back_kernel(
    heads, blocks, scale, q_ref, k_ref, v_ref, d_ref, log_ref, cos_ref, sin_ref,
    dq_ref, dkv_ref, rope_ref, key_sum, value_sum
):
    block_id = pl.program_id(0)

    @pl.when(block_id == 0)
    def _():
        key_sum[...] = jnp.zeros_like(key_sum)
        value_sum[...] = jnp.zeros_like(value_sum)

    for block in range(blocks):

        @pl.when(block_id == block)
        def _(block=block):
            span = (block + 1) * STEP
            tiles = []
            for head in range(heads):
                wide = slice(head * 2 * LANES, (head + 1) * 2 * LANES)
                thin = slice(head * VDIM, (head + 1) * VDIM)
                query = q_ref[:, wide]
                keys = k_ref[:span, wide]
                d_out = d_ref[:, thin]
                scores = causal(nt(query, keys) * scale, span)
                probs = jnp.exp(scores - log_ref[head])
                low = probs.astype(jnp.bfloat16)
                d_probs = nt(d_out, v_ref[:span, thin])
                centre = jnp.sum(probs * d_probs, -1, keepdims=True)
                d_scores = (probs * (d_probs - centre)).astype(jnp.bfloat16)
                d_query = nn(d_scores, keys) * scale
                key_sum[:span, wide] += tn(d_scores, query) * scale
                value_sum[:span, thin] += tn(low, d_out)
                tiles.append(
                    (
                        d_query[:, :NOPE],
                        turn(d_query[:, NOPE : NOPE + LANES], cos_ref[...], -sin_ref[...]),
                    )
                )
            dq_ref[...] = join_heads(tiles).astype(jnp.bfloat16)

    @pl.when(block_id == blocks - 1)
    def _():
        shared = None
        for head in range(heads):
            base = head * 2 * LANES
            dkv_ref[:, base : base + NOPE] = key_sum[:, base : base + NOPE].astype(jnp.bfloat16)
            dkv_ref[:, base + NOPE : base + NOPE + VDIM] = value_sum[
                :, head * VDIM : (head + 1) * VDIM
            ].astype(jnp.bfloat16)
            term = key_sum[:, base + LANES : base + 2 * LANES].astype(jnp.bfloat16)
            term = term.astype(jnp.float32)
            shared = term if shared is None else shared + term
        rope_ref[...] = shared.astype(jnp.bfloat16)


def attend_back(q, k, v, d_heads, logs, cosine, sine, heads, scale):
    length = q.shape[0]
    blocks = length // STEP
    query_width = heads * (NOPE + ROPE)
    return pl.pallas_call(
        functools.partial(attend_back_kernel, heads, blocks, scale),
        grid=(blocks,),
        in_specs=[
            by_rows(heads * 2 * LANES),
            fixed(k.shape),
            fixed(v.shape),
            by_rows(heads * VDIM),
            pl.BlockSpec((heads, STEP, 1), lambda i: (0, i, 0)),
            by_rows(LANES),
            by_rows(LANES),
        ],
        out_specs=[by_rows(query_width), fixed(k.shape), fixed((length, LANES))],
        out_shape=[
            jax.ShapeDtypeStruct((length, query_width), jnp.bfloat16),
            jax.ShapeDtypeStruct(k.shape, jnp.bfloat16),
            jax.ShapeDtypeStruct((length, LANES), jnp.bfloat16),
        ],
        scratch_shapes=[pltpu.VMEM(k.shape, jnp.float32), pltpu.VMEM(v.shape, jnp.float32)],
        cost_estimate=pl.CostEstimate(
            flops=2 * heads * length * length * 1100,
            bytes_accessed=12 * 2**20,
            transcendentals=heads * length * length,
        ),
        name="attend_back",
    )(q, k, v, d_heads, logs, cosine, sine)


def load_pieces(pieces, sems):
    copies = [
        pltpu.make_async_copy(source, target, sems.at[at])
        for at, (source, target) in enumerate(pieces)
    ]

    @pl.when(pl.program_id(0) == 0)
    def _():
        for copy in copies:
            copy.start()

    def take(low, high):
        @pl.when(pl.program_id(0) == 0)
        def _():
            for copy in copies[low:high]:
                copy.wait()

    return take


def stacked(refs, whole, columns):
    size = refs[0].shape[1 if columns else 0]
    pieces = []
    for r, ref in enumerate(refs):
        span = pl.ds(r * size, size)
        pieces.append((ref, whole.at[:, span] if columns else whole.at[span]))
    return pieces


def hidden_kernel(count, ff, *refs):
    x_ref, gate_ref = refs[:2]
    sources = refs[2 : 2 + 2 * count]
    hid_ref, a_ref, b_ref, gates, ups, sems = refs[2 + 2 * count :]
    pieces = stacked(sources[:count], gates, False) + stacked(sources[count:], ups, False)
    take = load_pieces(pieces, sems)
    take(0, len(pieces))
    total = gates.shape[1]
    x = x_ref[...]
    for low in range(0, total, CHUNK):
        high = min(low + CHUNK, total)
        gate = nn(x, gates[:, low:high])
        upper = nn(x, ups[:, low:high])
        sigma = jax.nn.sigmoid(gate)
        silu = gate * sigma
        slope = upper * sigma * (1.0 + gate * (1.0 - sigma))
        factor = gate_ref[...]
        if high > ff:
            column = lax.broadcasted_iota(jnp.int32, gate.shape, 1)
            factor = jnp.where(column < ff - low, factor, 1.0)
        hid_ref[:, low:high] = (silu * upper * factor).astype(jnp.bfloat16)
        a_ref[:, low:high] = (slope * factor).astype(jnp.bfloat16)
        b_ref[:, low:high] = (silu * factor).astype(jnp.bfloat16)


def hidden_pass(x, gate, gate_blocks, up_blocks, ff):
    length, width = x.shape
    count = len(gate_blocks)
    blocks = [*gate_blocks, *up_blocks]
    total = gate_blocks[0].shape[1]
    return pl.pallas_call(
        functools.partial(hidden_kernel, count, ff),
        grid=(length // WIDE,),
        in_specs=[by_rows(width, WIDE), by_rows(1, WIDE)]
        + [pl.BlockSpec(memory_space=pl.ANY)] * len(blocks),
        out_specs=[by_rows(total, WIDE)] * 3,
        out_shape=[jax.ShapeDtypeStruct((length, total), jnp.bfloat16)] * 3,
        scratch_shapes=[pltpu.VMEM((width, total), jnp.bfloat16)] * 2
        + [pltpu.SemaphoreType.DMA((2 * count,))],
        cost_estimate=pl.CostEstimate(
            flops=4 * length * width * total, bytes_accessed=32 * 2**20, transcendentals=0
        ),
        compiler_params=pltpu.CompilerParams(vmem_limit_bytes=60 * 2**20),
        name="hidden_pass",
    )(x, gate, *blocks)


def slope_kernel(count, *refs):
    g_ref, a_ref, b_ref = refs[:3]
    sources = refs[3 : 3 + 3 * count]
    dg_ref, du_ref, part_ref, downs, gates, ups, sems = refs[3 + 3 * count :]
    pieces = (
        stacked(sources[:count], downs, True)
        + stacked(sources[count : 2 * count], gates, False)
        + stacked(sources[2 * count :], ups, False)
    )
    take = load_pieces(pieces, sems)
    take(0, count)
    total = downs.shape[0]
    g = g_ref[...]
    for low in range(0, total, CHUNK):
        high = min(low + CHUNK, total)
        d_hidden = nt(g, downs[low:high])
        dg_ref[:, low:high] = (d_hidden * a_ref[:, low:high].astype(jnp.float32)).astype(
            jnp.bfloat16
        )
        du_ref[:, low:high] = (d_hidden * b_ref[:, low:high].astype(jnp.float32)).astype(
            jnp.bfloat16
        )
    take(count, len(pieces))
    d_gate, d_up = dg_ref[...], du_ref[...]
    width = g.shape[1]
    for low in range(0, width, CHUNK):
        high = min(low + CHUNK, width)
        part_ref[:, low:high] = (nt(d_gate, gates[low:high]) + nt(d_up, ups[low:high])).astype(
            jnp.bfloat16
        )


def slope_pass(g, a, b, down_blocks, gate_blocks, up_blocks):
    length, width = g.shape
    count = len(gate_blocks)
    blocks = [*down_blocks, *gate_blocks, *up_blocks]
    total = gate_blocks[0].shape[1]
    return pl.pallas_call(
        functools.partial(slope_kernel, count),
        grid=(length // NARROW,),
        in_specs=[by_rows(width, NARROW), by_rows(total, NARROW), by_rows(total, NARROW)]
        + [pl.BlockSpec(memory_space=pl.ANY)] * len(blocks),
        out_specs=[by_rows(total, NARROW), by_rows(total, NARROW), by_rows(width, NARROW)],
        out_shape=[
            jax.ShapeDtypeStruct((length, total), jnp.bfloat16),
            jax.ShapeDtypeStruct((length, total), jnp.bfloat16),
            jax.ShapeDtypeStruct((length, width), jnp.bfloat16),
        ],
        scratch_shapes=[
            pltpu.VMEM((total, width), jnp.bfloat16),
            pltpu.VMEM((width, total), jnp.bfloat16),
            pltpu.VMEM((width, total), jnp.bfloat16),
            pltpu.SemaphoreType.DMA((3 * count,)),
        ],
        cost_estimate=pl.CostEstimate(
            flops=6 * length * width * total, bytes_accessed=40 * 2**20, transcendentals=0
        ),
        compiler_params=pltpu.CompilerParams(vmem_limit_bytes=62 * 2**20),
        name="slope_pass",
    )(g, a, b, *blocks)


def rotate(values, cosine, sine):
    half_depth = values.shape[-1] // 2
    first = values[..., :half_depth]
    second = values[..., half_depth:]
    return jnp.concatenate([first * cosine - second * sine, second * cosine + first * sine], -1)


def norm_forward(values, scaling):
    inverse = lax.rsqrt(jnp.mean(values * values, -1, keepdims=True) + EPSILON)
    return (values * inverse * scaling, inverse)


def norm_backward(values, inverse, scaling, upstream):
    weighted = upstream * scaling
    scaling_grad = jnp.sum(upstream * values * inverse, 0)
    centre = jnp.mean(weighted * values, -1, keepdims=True)
    return (inverse * weighted - values * inverse**3 * centre, scaling_grad)


def gather_seq(block):
    return lax.all_gather(block, SEQ, axis=0, tiled=True)


def scatter_seq(partial):
    return lax.psum_scatter(
        partial.astype(jnp.bfloat16), SEQ, scatter_dimension=0, tiled=True
    ).astype(jnp.float32)


def settle_kernel(n, shards, terms_ref, out_ref, from_seq, joined, from_shard, sends, seq_recv, shard_recv):
    me = lax.axis_index(SEQ)
    my_shard = lax.axis_index(SHARD)
    barrier = pltpu.get_barrier_semaphore()
    for hop in range(1, n):
        pl.semaphore_signal(
            barrier, inc=1, device_id={SEQ: (me + hop) % n}, device_id_type=MESH
        )
    for hop in range(1, shards):
        pl.semaphore_signal(
            barrier, inc=1, device_id={SHARD: (my_shard + hop) % shards}, device_id_type=MESH
        )
    pl.semaphore_wait(barrier, n + shards - 2)
    first = []
    for hop in range(1, n):
        target = (me + hop) % n
        copy = pltpu.make_async_remote_copy(
            src_ref=terms_ref.at[target],
            dst_ref=from_seq.at[hop - 1],
            send_sem=sends.at[hop - 1],
            recv_sem=seq_recv.at[hop - 1],
            device_id={SEQ: target},
            device_id_type=MESH,
        )
        copy.start()
        first.append(copy)
    total = terms_ref[me]
    for hop in range(1, n):
        first[hop - 1].wait_recv()
        total = total + from_seq[hop - 1]
    joined[...] = total
    second = []
    for hop in range(1, shards):
        target = (my_shard + hop) % shards
        copy = pltpu.make_async_remote_copy(
            src_ref=joined.at[target],
            dst_ref=from_shard.at[hop - 1],
            send_sem=sends.at[n - 1 + hop - 1],
            recv_sem=shard_recv.at[hop - 1],
            device_id={SHARD: target},
            device_id_type=MESH,
        )
        copy.start()
        second.append(copy)
    total = joined[my_shard]
    for hop in range(1, shards):
        second[hop - 1].wait_recv()
        total = total + from_shard[hop - 1]
    out_ref[...] = total
    for copy in first + second:
        copy.wait_send()


def settle(n, shards, terms, identity):
    shape = terms.shape[2:]
    return pl.pallas_call(
        functools.partial(settle_kernel, n, shards),
        out_shape=jax.ShapeDtypeStruct(shape, jnp.float32),
        in_specs=[pl.BlockSpec(memory_space=pltpu.VMEM)],
        out_specs=pl.BlockSpec(memory_space=pltpu.VMEM),
        scratch_shapes=[
            pltpu.VMEM((n - 1, shards) + shape, jnp.float32),
            pltpu.VMEM((shards,) + shape, jnp.float32),
            pltpu.VMEM((shards - 1,) + shape, jnp.float32),
            pltpu.SemaphoreType.DMA((n + shards - 2,)),
            pltpu.SemaphoreType.DMA((n - 1,)),
            pltpu.SemaphoreType.DMA((shards - 1,)),
        ],
        compiler_params=pltpu.CompilerParams(collective_id=identity, has_side_effects=True),
        name="settle",
    )(terms)


def duplex_kernel(n, parts, sums, *refs):
    if sums:
        (x_ref, part_ref, all_ref, sum_ref, mine, other, left_in, right_in) = refs[:8]
        (pair_send, pair_recv, line_send, line_recv) = refs[8:12]
    else:
        x_ref, all_ref = refs[:2]
    copy_send, copy_recv, local = refs[-3:]
    half = n // 2
    me = lax.axis_index(SEQ)
    core = me % 2
    place = me // 2
    partner = place * 2 + 1 - core
    below, above = me - 2, me + 2
    has_below, has_above = place > 0, place < half - 1

    def remote(source, target, send, recv, device):
        return pltpu.make_async_remote_copy(
            src_ref=source,
            dst_ref=target,
            send_sem=send,
            recv_sem=recv,
            device_id={SEQ: device},
            device_id_type=MESH,
        )

    def pair_copy(at):
        return remote(
            part_ref.at[at * 2 + 1 - core], other.at[at], pair_send.at[at], pair_recv.at[at], partner
        )

    piece = x_ref.shape[0] // parts

    def rows_of(part):
        return pl.ds(part * piece, piece)

    def sum_up(at, part):
        span = rows_of(part)
        return remote(
            mine.at[at, span],
            left_in.at[at, span],
            line_send.at[0, at, part],
            line_recv.at[0, at, part],
            above,
        )

    def sum_down(at, part):
        span = rows_of(part)
        return remote(
            mine.at[at, span],
            right_in.at[at, span],
            line_send.at[1, at, part],
            line_recv.at[1, at, part],
            below,
        )

    def block_copy(source, block, way, step, part, device):
        span = rows_of(part)
        return remote(
            source.at[span],
            all_ref.at[block, span],
            copy_send.at[way, step, part],
            copy_recv.at[way, step, part],
            device,
        )

    order = []
    for at in range(half):
        for item in (half - 1 - at, at):
            if item not in order:
                order.append(item)
    for at in order if sums else ():
        pltpu.make_async_copy(part_ref.at[at * 2 + core], mine.at[at], local.at[at]).start()
    keep = pltpu.make_async_copy(x_ref, all_ref.at[me], local.at[half])
    keep.start()

    barrier = pltpu.get_barrier_semaphore()
    pl.semaphore_signal(barrier, inc=1, device_id={SEQ: partner}, device_id_type=MESH)

    @pl.when(has_below)
    def _():
        pl.semaphore_signal(barrier, inc=1, device_id={SEQ: below}, device_id_type=MESH)

    @pl.when(has_above)
    def _():
        pl.semaphore_signal(barrier, inc=1, device_id={SEQ: above}, device_id_type=MESH)

    @pl.when(has_below & has_above)
    def _():
        pl.semaphore_wait(barrier, 3)

    @pl.when(jnp.logical_not(has_below & has_above))
    def _():
        pl.semaphore_wait(barrier, 2)

    for at in order if sums else ():
        pair_copy(at).start()

    for part in range(parts):

        @pl.when(has_above)
        def _():
            block_copy(x_ref, me, 0, 0, part, above).start()

        @pl.when(has_below)
        def _():
            block_copy(x_ref, me, 1, 0, part, below).start()

        block_copy(x_ref, me, 2, 0, part, partner).start()

    def merge(at, part, incoming):
        span = rows_of(part)
        total = mine[at, span].astype(jnp.float32) + other[at, span].astype(jnp.float32)
        if incoming is not None:
            total = total + incoming[at, span].astype(jnp.float32)
        mine[at, span] = total.astype(mine.dtype)

    def load(at):
        return pltpu.make_async_copy(part_ref.at[at * 2 + core], mine.at[at], local.at[at])

    def ready(at):
        load(at).wait()
        pair_copy(at).wait_recv()

    def relay(slot, part):
        step = slot - 1

        @pl.when(place > step)
        def _():
            block = me - 2 * (step + 1)
            block_copy(x_ref, block, 0, step, part, above).wait_recv()

            @pl.when(has_above)
            def _():
                block_copy(all_ref.at[block], block, 0, step + 1, part, above).start()

            block_copy(all_ref.at[block], block, 2, 1 + step, part, partner).start()

        @pl.when(place < half - 1 - step)
        def _():
            block = me + 2 * (step + 1)
            block_copy(x_ref, block, 1, step, part, below).wait_recv()

            @pl.when(has_below)
            def _():
                block_copy(all_ref.at[block], block, 1, step + 1, part, below).start()

            block_copy(all_ref.at[block], block, 2, half + step, part, partner).start()

    for slot in range(2 * half - 2):
        rise = half - 1 - (slot - place)
        fall = slot - (half - 1 - place)
        if 1 <= slot <= half - 1:
            for part in range(parts):
                relay(slot, part)
        if not sums:
            continue

        @pl.when((rise < half) & (rise > place))
        def _():
            ready(rise)
            for part in range(parts):

                @pl.when(has_below)
                def _():
                    sum_up(rise, part).wait_recv()
                    merge(rise, part, left_in)

                @pl.when(jnp.logical_not(has_below))
                def _():
                    merge(rise, part, None)

                sum_up(rise, part).start()

        @pl.when((fall >= 0) & (fall < place))
        def _():
            ready(fall)
            for part in range(parts):

                @pl.when(has_above)
                def _():
                    sum_down(fall, part).wait_recv()
                    merge(fall, part, right_in)

                @pl.when(jnp.logical_not(has_above))
                def _():
                    merge(fall, part, None)

                sum_down(fall, part).start()

    if sums:
        ready(place)
        for part in range(parts):

            @pl.when(has_below)
            def _():
                sum_up(place, part).wait_recv()

            @pl.when(has_above)
            def _():
                sum_down(place, part).wait_recv()

        total = mine[place].astype(jnp.float32) + other[place].astype(jnp.float32)
        low = jnp.where(has_below, left_in[place].astype(jnp.float32), 0.0)
        high = jnp.where(has_above, right_in[place].astype(jnp.float32), 0.0)
        sum_ref[...] = total + low + high

    keep.wait()
    for at in range(half if sums else 0):
        pair_copy(at).wait_send()
    for part in range(parts):
        block_copy(x_ref, partner, 2, 0, part, partner).wait_recv()
        block_copy(x_ref, me, 2, 0, part, partner).wait_send()

        @pl.when(has_above)
        def _():
            block_copy(x_ref, me, 0, 0, part, above).wait_send()

        @pl.when(has_below)
        def _():
            block_copy(x_ref, me, 1, 0, part, below).wait_send()

        for step in range(half - 1):
            up, down = half - 1 - step, step
            if sums:

                @pl.when(place < up)
                def _():
                    sum_up(up, part).wait_send()

                @pl.when(place > down)
                def _():
                    sum_down(down, part).wait_send()

            @pl.when(place > step)
            def _():
                block = me - 2 * (step + 1)

                @pl.when(has_above)
                def _():
                    block_copy(x_ref, block, 0, step + 1, part, above).wait_send()

                block_copy(x_ref, block, 2, 1 + step, part, partner).wait_send()
                there = partner - 2 * (step + 1)
                block_copy(x_ref, there, 2, 1 + step, part, partner).wait_recv()

            @pl.when(place < half - 1 - step)
            def _():
                block = me + 2 * (step + 1)

                @pl.when(has_below)
                def _():
                    block_copy(x_ref, block, 1, step + 1, part, below).wait_send()

                block_copy(x_ref, block, 2, half + step, part, partner).wait_send()
                there = partner + 2 * (step + 1)
                block_copy(x_ref, there, 2, half + step, part, partner).wait_recv()


def duplex(n, block, partial, identity, parts=2):
    half = n // 2
    rows, wide = partial.shape[0] // n, partial.shape[1]
    line = pltpu.VMEM((half, rows, wide), partial.dtype)
    gathered, total = pl.pallas_call(
        functools.partial(duplex_kernel, n, parts, True),
        out_shape=[
            jax.ShapeDtypeStruct((n,) + block.shape, block.dtype),
            jax.ShapeDtypeStruct((rows, wide), jnp.float32),
        ],
        in_specs=[
            pl.BlockSpec(memory_space=pltpu.VMEM),
            pl.BlockSpec(memory_space=pl.ANY),
        ],
        out_specs=[
            pl.BlockSpec(memory_space=pl.ANY),
            pl.BlockSpec(memory_space=pltpu.VMEM),
        ],
        scratch_shapes=[
            line,
            line,
            line,
            line,
            pltpu.SemaphoreType.DMA((half,)),
            pltpu.SemaphoreType.DMA((half,)),
            pltpu.SemaphoreType.DMA((2, half, parts)),
            pltpu.SemaphoreType.DMA((2, half, parts)),
            pltpu.SemaphoreType.DMA((3, 2 * half, parts)),
            pltpu.SemaphoreType.DMA((3, 2 * half, parts)),
            pltpu.SemaphoreType.DMA((half + 1,)),
        ],
        compiler_params=pltpu.CompilerParams(collective_id=identity, has_side_effects=True),
        cost_estimate=pl.CostEstimate(
            flops=45_000_000_000, bytes_accessed=2**24, transcendentals=0
        ),
        name="duplex",
    )(block, partial.reshape(n, rows, wide))
    return gathered.reshape(n * block.shape[0], block.shape[1]), total


def chain_gather(n, block, identity, parts=2):
    half = n // 2
    return pl.pallas_call(
        functools.partial(duplex_kernel, n, parts, False),
        out_shape=jax.ShapeDtypeStruct((n,) + block.shape, block.dtype),
        in_specs=[pl.BlockSpec(memory_space=pltpu.VMEM)],
        out_specs=pl.BlockSpec(memory_space=pl.ANY),
        scratch_shapes=[
            pltpu.SemaphoreType.DMA((3, 2 * half, parts)),
            pltpu.SemaphoreType.DMA((3, 2 * half, parts)),
            pltpu.SemaphoreType.DMA((half + 1,)),
        ],
        compiler_params=pltpu.CompilerParams(collective_id=identity, has_side_effects=True),
        cost_estimate=pl.CostEstimate(
            flops=25_000_000_000, bytes_accessed=2**22, transcendentals=0
        ),
        name="chain",
    )(block)


ACROSS = ([(0, 1), (1, 0), (2, 3), (3, 2)], [(0, 2), (2, 0), (1, 3), (3, 1)])


def swap_with(block, side):
    return lax.ppermute(block, SHARD, ACROSS[side])


def gather_blocks(weight, axis, side):
    if lax.axis_size(SHARD) != 4:
        return [lax.all_gather(weight, SHARD, axis=axis, tiled=True)]
    near = [swap_with(weight, 0), swap_with(weight, 1)]
    far = swap_with(near[side], 1 - side)
    return [weight, near[0], near[1], far]


def after(value, token):
    return lax.optimization_barrier((value, token))[0]


def scatter_blocks(blocks, axis, side, join_token, sum_token):
    if lax.axis_size(SHARD) != 4:
        blocks = [block.astype(jnp.bfloat16) for block in blocks]
        return (lax.psum_scatter(blocks[0], SHARD, scatter_dimension=axis, tiled=True),)
    blocks = [lax.optimization_barrier(block.astype(jnp.bfloat16)) for block in blocks]
    far = swap_with(blocks[3], side)
    first = swap_with(blocks[1 + side], side)
    far = after(far, join_token)
    joined = (blocks[2 - side].astype(jnp.float32) + far.astype(jnp.float32)).astype(
        jnp.bfloat16
    )
    second = swap_with(joined, 1 - side)
    second = after(second, sum_token)
    return blocks[0], first, second


def add_up(terms, rows=slice(None), columns=slice(None)):
    total = None
    for term in terms:
        term = term[rows, columns].astype(jnp.float32)
        total = term if total is None else total + term
    return total


def local_order(values, axis):
    if lax.axis_size(SHARD) != 4:
        return values
    size = values.shape[axis] // 4
    shard = lax.axis_index(SHARD)
    return jnp.concatenate(
        [
            lax.dynamic_slice_in_dim(values, jnp.bitwise_xor(shard, place) * size, size, axis)
            for place in range(4)
        ],
        axis,
    )


def cut(values, axis):
    if lax.axis_size(SHARD) != 4:
        return [values]
    size = values.shape[axis] // 4
    return [lax.slice_in_dim(values, r * size, (r + 1) * size, axis=axis) for r in range(4)]


def on_device(
    inputs,
    attn_gain,
    query_project_weight,
    latent_project_weight,
    latent_gain,
    latent_keyval_weight,
    attention_output_weight,
    ffn_gain,
    shared_gate,
    shared_up,
    shared_down,
    expert_gate,
    expert_up,
    expert_down,
    routes,
    slots,
    gates,
    cotangent,
):
    tok_rows = inputs.shape[1]
    model_width = inputs.shape[2]
    groups = lax.axis_size(SEQ)
    shards = lax.axis_size(SHARD)
    me = lax.axis_index(SEQ)
    heads = HEADS // groups
    experts = EXP_DEV * groups
    capacity = 9 * tok_rows * TOPK // (8 * experts)
    length = tok_rows * groups
    score_scale = (NOPE + ROPE) ** (-0.5)
    own_start = me * tok_rows
    one_width = attn_gain.shape[0]
    lat_width = latent_gain.shape[0]
    ff = expert_gate.shape[2]
    shared_ff = shared_gate.shape[1]
    side = -(-shared_ff // LANES) * LANES

    own_inputs = local_order(inputs.reshape(tok_rows, model_width), 1)
    inputs_all = gather_seq(own_inputs)
    upstream = local_order(cotangent.reshape(tok_rows, model_width), 1)
    route_rows = routes.reshape(tok_rows, TOPK)
    slot_rows = slots.reshape(tok_rows, TOPK)
    kept = (route_rows.T[:, None, :] == jnp.arange(experts)[None, :, None]) & (
        slot_rows.T < capacity
    )[:, None, :]
    gate_table = jnp.sum(
        jnp.where(kept, gates.reshape(tok_rows, TOPK).T.astype(jnp.float32)[:, None, :], 0.0), 0
    ).astype(jnp.bfloat16)

    def padded_row(gain):
        return jnp.pad(gain, (0, LANES - ROPE - gain.shape[0]))[None]

    side_rows = jnp.concatenate(
        [
            padded_row(attn_gain),
            padded_row(ffn_gain),
            padded_row(latent_gain),
            jnp.zeros((one_width - 3, LANES - ROPE), jnp.bfloat16),
        ],
        0,
    )
    small_own = jnp.concatenate([latent_project_weight, side_rows], 1)
    small_rows = jnp.concatenate(gather_blocks(small_own, 0, 0), 0)
    small_rows = jnp.concatenate(
        [
            small_rows,
            jnp.pad(gate_table, ((0, EXTRA - experts), (0, small_rows.shape[1] - tok_rows))),
        ],
        0,
    )
    small_seq = chain_gather(groups, small_rows, 4)
    gate_column = (
        lax.dynamic_index_in_dim(
            small_seq[:, shards * one_width :, :tok_rows], me, 1, keepdims=False
        )
        .reshape(length, 1)
        .astype(jnp.float32)
    )
    gain_rows = (
        small_seq[:, : shards * one_width, RANK + ROPE :]
        .reshape(groups, shards, one_width, -1)[:, :, :3]
        .astype(jnp.float32)
        .transpose(2, 1, 0, 3)
    )
    first_norm_weight = gain_rows[0, :, :, :one_width].reshape(-1)
    second_norm_weight = gain_rows[1, :, :, :one_width].reshape(-1)
    latent_norm_weight = local_order(gain_rows[2, :, :, :lat_width].reshape(-1), 0)

    spare = side - shared_ff
    gate_own = jnp.pad(
        jnp.concatenate([expert_gate[0], shared_gate], 1), ((0, 0), (0, spare))
    )
    up_own = jnp.pad(jnp.concatenate([expert_up[0], shared_up], 1), ((0, 0), (0, spare)))
    down_own = jnp.pad(jnp.concatenate([expert_down[0], shared_down], 0), ((0, spare), (0, 0)))
    query_blocks = gather_blocks(query_project_weight, 0, 0)
    kvup_blocks = gather_blocks(latent_keyval_weight, 0, 0)
    out_blocks = gather_blocks(attention_output_weight, 1, 0)
    gate_blocks = gather_blocks(gate_own, 0, 0)
    up_blocks = gather_blocks(up_own, 0, 1)
    down_blocks = gather_blocks(down_own, 1, 1)
    full_query = jnp.concatenate(query_blocks, 0)
    full_kvup = local_order(jnp.concatenate(kvup_blocks, 0), 0)
    full_out = jnp.concatenate(out_blocks, 1)

    residual_stream = own_inputs.astype(jnp.float32)
    cosine, sine = rope_lanes(jnp.arange(length))
    first_all, q_all, k_all, v_all, latent, latent_all = front(
        inputs_all,
        first_norm_weight[None],
        latent_norm_weight[None],
        cosine,
        sine,
        full_kvup,
        query_blocks,
        small_seq,
        shards,
        heads,
    )
    attended, logs = attend(q_all, k_all, v_all, heads, score_scale)
    attended_part = nn(attended, full_out)
    upstream_all, attended_sum = duplex(groups, upstream, attended_part.astype(jnp.bfloat16), 1)
    middle = residual_stream + attended_sum
    normed_two, inv_two = norm_forward(middle, second_norm_weight)
    second_all = gather_seq(normed_two.astype(jnp.bfloat16))

    hidden, slope_gate, slope_up = hidden_pass(second_all, gate_column, gate_blocks, up_blocks, ff)
    d_gate, d_up, second_part = slope_pass(
        upstream_all, slope_gate, slope_up, down_blocks, gate_blocks, up_blocks
    )
    d_second = scatter_seq(second_part)
    hidden_late = after(hidden, d_gate)
    d_down = [tn(hidden_late, part) for part in cut(upstream_all, 1)[1:]]
    second_parts = cut(second_all, 1)
    d_wgate = [tn(part, d_gate) for part in second_parts[1:]]
    d_wup = [tn(part, d_up) for part in second_parts[1:]]
    down_part = nn(hidden, jnp.concatenate(down_blocks, 1)).astype(jnp.bfloat16)

    d_middle_norm, d_gain_two = norm_backward(middle, inv_two, second_norm_weight, d_second)
    d_middle = upstream.astype(jnp.float32) + d_middle_norm
    d_branch_all, added = duplex(groups, d_middle.astype(jnp.bfloat16), down_part, 2)
    output = local_order((middle + added).astype(jnp.bfloat16), 1).reshape(
        1, tok_rows, model_width
    )
    d_heads = nt(d_branch_all, full_out).astype(jnp.bfloat16)
    d_query, d_keyval, d_shared_key = attend_back(
        q_all, k_all, v_all, d_heads, logs, cosine, sine, heads, score_scale
    )
    latent_part = nt(d_keyval, full_kvup).astype(jnp.bfloat16)
    latent_back = scatter_seq(jnp.concatenate([latent_part, d_shared_key], 1))
    first_part = nt(d_query, full_query)
    first_back = scatter_seq(first_part)
    d_wout = [tn(attended, part).astype(jnp.bfloat16) for part in cut(d_branch_all, 1)]
    d_wquery = [tn(part, d_query).astype(jnp.bfloat16) for part in cut(first_all, 1)]
    d_wkvup = cut(local_order(tn(latent_all, d_keyval).astype(jnp.bfloat16), 0), 0)

    own_latent = lax.dynamic_slice_in_dim(latent, own_start, tok_rows, 0)
    half = ROPE // 2
    cos_own = lax.dynamic_slice_in_dim(cosine, own_start, tok_rows, 0)[:, :half]
    sin_own = lax.dynamic_slice_in_dim(sine, own_start, tok_rows, 0)[:, half:ROPE]
    inv_latent = norm_forward(own_latent, latent_norm_weight)[1]
    d_rope = rotate(latent_back[:, RANK : RANK + ROPE], cos_own, -sin_own)
    d_compressed, d_gain_latent = norm_backward(
        own_latent, inv_latent, latent_norm_weight, latent_back[:, :RANK]
    )
    d_latent = jnp.concatenate(
        [d_compressed, d_rope, jnp.zeros((tok_rows, LANES - ROPE), jnp.float32)], -1
    ).astype(jnp.bfloat16)
    d_latent_all = gather_seq(d_latent)
    inv_one = norm_forward(residual_stream, first_norm_weight)[1]
    d_first = first_back + jnp.concatenate(
        [
            nt(
                d_latent,
                small_seq[:, r * one_width : (r + 1) * one_width].reshape(groups * one_width, -1),
            )
            for r in range(shards)
        ],
        1,
    )
    d_resid, d_gain_one = norm_backward(residual_stream, inv_one, first_norm_weight, d_first)
    input_grad = local_order(d_middle + d_resid, 1).reshape(1, tok_rows, model_width)
    first_late = after(first_all, d_latent)
    own_columns = jnp.concatenate(
        [
            lax.dynamic_slice_in_dim(
                first_late, (place * groups + me) * one_width, one_width, 1
            )
            for place in range(shards)
        ],
        1,
    )
    d_wlatent = cut(tn(own_columns, d_latent_all).astype(jnp.bfloat16), 0)

    devices = shards * groups
    terms = jnp.concatenate(
        [
            local_order(d_gain_one, 0).reshape(devices, one_width),
            local_order(d_gain_two, 0).reshape(devices, one_width),
            d_gain_latent.reshape(devices, lat_width),
        ],
        1,
    )
    terms = jnp.pad(terms, ((0, 0), (0, 1024 - terms.shape[1]))).reshape(shards, groups, 8, 128)
    gain_grads = settle(groups, shards, terms.transpose(1, 0, 2, 3), 9).reshape(-1)
    d_down.insert(0, tn(hidden, cut(after(upstream_all, d_latent), 1)[0]))
    second_own = cut(after(second_all, d_latent), 1)[0]
    d_wgate.insert(0, tn(second_own, d_gate))
    d_wup.insert(0, tn(second_own, d_up))
    gate_grad = scatter_blocks(d_wgate, 0, 0, d_keyval, d_wlatent[0])
    up_grad = scatter_blocks(d_wup, 0, 1, d_keyval, d_wlatent[0])
    down_grad = scatter_blocks(d_down, 1, 0, second_part, d_latent)
    out_grad = scatter_blocks(d_wout, 1, 1, d_latent, d_wlatent[0])
    kvup_grad = scatter_blocks(d_wkvup, 0, 1, d_latent, d_wlatent[0])
    query_grad = scatter_blocks(d_wquery, 0, 1, d_latent, d_wlatent[0])
    latent_grad = scatter_blocks(d_wlatent, 0, 1, first_back, first_back)
    return (
        output,
        input_grad,
        gain_grads[:one_width],
        add_up(query_grad),
        add_up(latent_grad, columns=slice(0, RANK + ROPE)),
        gain_grads[2 * one_width : 2 * one_width + lat_width],
        add_up(kvup_grad),
        add_up(out_grad),
        gain_grads[one_width : 2 * one_width],
        add_up(gate_grad, columns=slice(ff, ff + shared_ff)),
        add_up(up_grad, columns=slice(ff, ff + shared_ff)),
        add_up(down_grad, rows=slice(ff, ff + shared_ff)),
        add_up(gate_grad, columns=slice(0, ff))[None],
        add_up(up_grad, columns=slice(0, ff))[None],
        add_up(down_grad, rows=slice(0, ff))[None],
    )


def solution(mesh):
    in_specs = (
        P(SHARD, SEQ, None),
        P((SHARD, SEQ)),
        P(SHARD, SEQ),
        P((SHARD, SEQ), None),
        P((SHARD, SEQ)),
        P(SHARD, SEQ),
        P(SEQ, SHARD),
        P((SHARD, SEQ)),
        P(SHARD, SEQ),
        P(SHARD, SEQ),
        P(SEQ, SHARD),
        P(SEQ, SHARD, None),
        P(SEQ, SHARD, None),
        P(SEQ, None, SHARD),
        P(SHARD, SEQ, None),
        P(SHARD, SEQ, None),
        P(SHARD, SEQ, None),
        P(SHARD, SEQ, None),
    )
    out_specs = (
        P(SHARD, SEQ, None),
        P(SHARD, SEQ, None),
        P((SHARD, SEQ)),
        P(SHARD, SEQ),
        P((SHARD, SEQ), None),
        P((SHARD, SEQ)),
        P(SHARD, SEQ),
        P(SEQ, SHARD),
        P((SHARD, SEQ)),
        P(SHARD, SEQ),
        P(SHARD, SEQ),
        P(SEQ, SHARD),
        P(SEQ, SHARD, None),
        P(SEQ, SHARD, None),
        P(SEQ, None, SHARD),
    )

    return jax.shard_map(
        on_device, mesh=mesh, in_specs=in_specs, out_specs=out_specs, check_vma=False
    )
```

```python
import functools

import jax
import jax.numpy as jnp
from jax import lax
from jax.experimental import pallas as pl
from jax.experimental.pallas import tpu as pltpu
from jax.sharding import PartitionSpec as P

HEADS = 16
NOPE = 128
ROPE = 64
VDIM = 128
RANK = 512
TOPK = 6
EXP_DEV = 1
EXTRA = 32


EPSILON = 1e-06
THETA = 10000.0
MASKED = -1e30
SHARD = "shard"
SEQ = "seq"
MESH = pl.DeviceIdType.MESH


LANES = 128
STEP = 256
WIDE = 512
NARROW = 512
CHUNK = 512


def nn(left, right):
    return jnp.dot(left, right, preferred_element_type=jnp.float32)


def nt(left, right):
    return lax.dot_general(
        left, right, (((1,), (1,)), ((), ())), preferred_element_type=jnp.float32
    )


def tn(left, right):
    return lax.dot_general(
        left, right, (((0,), (0,)), ((), ())), preferred_element_type=jnp.float32
    )


def lane_index(rows):
    return lax.broadcasted_iota(jnp.int32, (rows, LANES), 1)


def turn(tile, cosine, sine):
    lane = lane_index(tile.shape[0])
    low = pltpu.roll(tile, LANES - ROPE // 2, 1)
    high = pltpu.roll(tile, ROPE // 2, 1)
    return tile * cosine + jnp.where(lane < ROPE // 2, low, high) * sine


def rope_lanes(positions):
    half = ROPE // 2
    frequency = THETA ** (-(2.0 * jnp.arange(half, dtype=jnp.float32)) / ROPE)
    angles = positions.astype(jnp.float32)[:, None] * frequency[None, :]
    cosine, sine = jnp.cos(angles), jnp.sin(angles)
    blank = jnp.zeros((positions.shape[0], LANES - ROPE), jnp.float32)
    return (
        jnp.concatenate([cosine, cosine, blank], 1),
        jnp.concatenate([-sine, sine, blank], 1),
    )


def split_heads(values, heads):
    width = NOPE + ROPE
    rows = values.shape[0]
    keep = lane_index(rows) < ROPE
    tiles = []
    for head in range(heads):
        part = values if head == 0 else pltpu.roll(values, (heads - head) * width, 1)
        if part.shape[1] >= 2 * LANES:
            turned = jnp.where(keep, part[:, NOPE : NOPE + LANES], 0.0)
        else:
            turned = jnp.concatenate(
                [part[:, NOPE:], jnp.zeros((rows, LANES - ROPE), part.dtype)], 1
            )
        tiles.append((part[:, :NOPE], turned))
    return tiles


def join_heads(tiles):
    heads = len(tiles)
    width = NOPE + ROPE
    if heads == 1:
        return jnp.concatenate([tiles[0][0], tiles[0][1][:, :ROPE]], 1)
    rows = tiles[0][0].shape[0]
    blank = jnp.zeros((rows, heads * width - 2 * LANES), jnp.float32)
    total = None
    for head, (plain, turned) in enumerate(tiles):
        part = jnp.concatenate([plain, turned, blank], 1)
        part = part if head == 0 else pltpu.roll(part, head * width, 1)
        total = part if total is None else total + part
    return total


def front_kernel(heads, count, shards, *refs):
    x_ref, gain_ref, lat_gain_ref, cos_ref, sin_ref, kvup_ref = refs[:6]
    query_refs = refs[6 : 6 + count]
    latent_refs = refs[6 + count : 6 + count + shards]
    first_ref, q_ref, k_ref, v_ref, latent_ref, low_ref = refs[6 + count + shards :]
    values = x_ref[...].astype(jnp.float32)
    inverse = lax.rsqrt(jnp.mean(values * values, -1, keepdims=True) + EPSILON)
    first = (values * inverse * gain_ref[...]).astype(jnp.bfloat16)
    first_ref[...] = first
    depth = query_refs[0].shape[0]
    query = None
    latent = None
    for r in range(count):
        term = nn(first[:, r * depth : (r + 1) * depth], query_refs[r][...])
        query = term if query is None else query + term
    depth = first.shape[1] // shards
    for r in range(shards):
        weight = latent_refs[r][...].reshape(depth, latent_refs[r].shape[2])
        term = nn(first[:, r * depth : (r + 1) * depth], weight)
        latent = term if latent is None else latent + term
    cosine, sine = cos_ref[...], sin_ref[...]
    for head, (plain, turned) in enumerate(split_heads(query, heads)):
        base = head * 2 * LANES
        q_ref[:, base : base + LANES] = plain.astype(jnp.bfloat16)
        q_ref[:, base + LANES : base + 2 * LANES] = turn(turned, cosine, sine).astype(
            jnp.bfloat16
        )
    packed = latent[:, :RANK]
    latent_ref[...] = packed
    inverse = lax.rsqrt(jnp.mean(packed * packed, -1, keepdims=True) + EPSILON)
    low = (packed * inverse * lat_gain_ref[...]).astype(jnp.bfloat16)
    low_ref[...] = low
    shared = jnp.where(
        lane_index(packed.shape[0]) < ROPE, latent[:, RANK : RANK + LANES], 0.0
    )
    shared = turn(shared, cosine, sine).astype(jnp.bfloat16)
    keyval = nn(low, kvup_ref[...]).astype(jnp.bfloat16)
    for head in range(heads):
        base = head * 2 * LANES
        k_ref[:, base : base + LANES] = keyval[:, base : base + NOPE]
        k_ref[:, base + LANES : base + 2 * LANES] = shared
        v_ref[:, head * VDIM : (head + 1) * VDIM] = keyval[:, base + NOPE : base + NOPE + VDIM]


def fixed(shape):
    return pl.BlockSpec(shape, lambda *_: (0,) * len(shape), pipeline_mode=pl.Buffered(1))


def by_rows(width, step=STEP):
    return pl.BlockSpec((step, width), lambda i: (i, 0))


def front(x, gain, lat_gain, cosine, sine, kvup, query_blocks, small, shards, heads):
    length, width = x.shape
    count = len(query_blocks)
    groups = small.shape[0]

    def latent_spec(r):
        return pl.BlockSpec(
            (groups, width // shards // groups, small.shape[2]),
            lambda *_: (0, r, 0),
            pipeline_mode=pl.Buffered(1),
        )

    shapes = [
        (width, jnp.bfloat16),
        (heads * 2 * LANES, jnp.bfloat16),
        (heads * 2 * LANES, jnp.bfloat16),
        (heads * VDIM, jnp.bfloat16),
        (RANK, jnp.float32),
        (RANK, jnp.bfloat16),
    ]
    return pl.pallas_call(
        functools.partial(front_kernel, heads, count, shards),
        grid=(length // STEP,),
        in_specs=[
            by_rows(width),
            fixed((1, width)),
            fixed((1, RANK)),
            by_rows(LANES),
            by_rows(LANES),
            fixed(kvup.shape),
        ]
        + [fixed(b.shape) for b in query_blocks]
        + [latent_spec(r) for r in range(shards)],
        out_specs=[by_rows(w) for w, _ in shapes],
        out_shape=[jax.ShapeDtypeStruct((length, w), d) for w, d in shapes],
        cost_estimate=pl.CostEstimate(
            flops=2 * length * width * 1100, bytes_accessed=20 * 2**20, transcendentals=0
        ),
        name="front",
    )(x, gain, lat_gain, cosine, sine, kvup, *query_blocks, *[small] * shards)


def causal(scores, span):
    row = lax.broadcasted_iota(jnp.int32, (STEP, STEP), 0)
    column = lax.broadcasted_iota(jnp.int32, (STEP, STEP), 1)
    edge = jnp.where(column <= row, scores[:, span - STEP :], MASKED)
    return edge if span == STEP else jnp.concatenate([scores[:, : span - STEP], edge], 1)


def attend_kernel(blocks, scale, q_ref, k_ref, v_ref, out_ref, log_ref):
    for block in range(blocks):

        @pl.when(pl.program_id(1) == block)
        def _(block=block):
            span = (block + 1) * STEP
            scores = causal(nt(q_ref[...], k_ref[:span]) * scale, span)
            top = jnp.max(scores, -1, keepdims=True)
            expo = jnp.exp(scores - top)
            total = jnp.sum(expo, -1, keepdims=True)
            low = (expo / total).astype(jnp.bfloat16)
            out_ref[...] = nn(low, v_ref[:span]).astype(jnp.bfloat16)
            log_ref[0] = top + jnp.log(total)


def attend(q, k, v, heads, scale):
    length = q.shape[0]
    blocks = length // STEP
    return pl.pallas_call(
        functools.partial(attend_kernel, blocks, scale),
        grid=(heads, blocks),
        in_specs=[
            pl.BlockSpec((STEP, 2 * LANES), lambda h, i: (i, h)),
            pl.BlockSpec((length, 2 * LANES), lambda h, i: (0, h)),
            pl.BlockSpec((length, VDIM), lambda h, i: (0, h)),
        ],
        out_specs=[
            pl.BlockSpec((STEP, VDIM), lambda h, i: (i, h)),
            pl.BlockSpec((1, STEP, 1), lambda h, i: (h, i, 0)),
        ],
        out_shape=[
            jax.ShapeDtypeStruct((length, heads * VDIM), jnp.bfloat16),
            jax.ShapeDtypeStruct((heads, length, 1), jnp.float32),
        ],
        cost_estimate=pl.CostEstimate(
            flops=2 * heads * length * length * 500,
            bytes_accessed=8 * 2**20,
            transcendentals=heads * length * length,
        ),
        name="attend",
    )(q, k, v)


def attend_back_kernel(heads, blocks, scale, *refs):
    q_ref, k_ref, v_ref, d_ref, log_ref, cos_ref, sin_ref, kvup_ref = refs[:8]
    query_refs = refs[8:-5]
    dq_ref, dkv_ref, part_ref, key_sum, value_sum = refs[-5:]
    block_id = pl.program_id(0)
    depth = query_refs[0].shape[0]
    width = depth * len(query_refs)

    @pl.when(block_id == 0)
    def _():
        key_sum[...] = jnp.zeros_like(key_sum)
        value_sum[...] = jnp.zeros_like(value_sum)

    for block in range(blocks):

        @pl.when(block_id == block)
        def _(block=block):
            span = (block + 1) * STEP
            tiles = []
            for head in range(heads):
                wide = slice(head * 2 * LANES, (head + 1) * 2 * LANES)
                thin = slice(head * VDIM, (head + 1) * VDIM)
                query = q_ref[:, wide]
                keys = k_ref[:span, wide]
                d_out = d_ref[:, thin]
                scores = causal(nt(query, keys) * scale, span)
                probs = jnp.exp(scores - log_ref[head])
                low = probs.astype(jnp.bfloat16)
                d_probs = nt(d_out, v_ref[:span, thin])
                centre = jnp.sum(probs * d_probs, -1, keepdims=True)
                d_scores = (probs * (d_probs - centre)).astype(jnp.bfloat16)
                d_query = nn(d_scores, keys) * scale
                key_sum[:span, wide] += tn(d_scores, query) * scale
                value_sum[:span, thin] += tn(low, d_out)
                tiles.append(
                    (
                        d_query[:, :NOPE],
                        turn(d_query[:, NOPE : NOPE + LANES], cos_ref[...], -sin_ref[...]),
                    )
                )
            dq_ref[...] = join_heads(tiles).astype(jnp.bfloat16)

    rows = pl.ds(pl.multiple_of(block_id * STEP, STEP), STEP)
    for r, query_ref in enumerate(query_refs):
        part_ref[rows, r * depth : (r + 1) * depth] = nt(dq_ref[...], query_ref[...]).astype(
            jnp.bfloat16
        )

    @pl.when(block_id == blocks - 1)
    def _():
        shared = None
        for head in range(heads):
            base = head * 2 * LANES
            dkv_ref[:, base : base + NOPE] = key_sum[:, base : base + NOPE].astype(jnp.bfloat16)
            dkv_ref[:, base + NOPE : base + NOPE + VDIM] = value_sum[
                :, head * VDIM : (head + 1) * VDIM
            ].astype(jnp.bfloat16)
            term = key_sum[:, base + LANES : base + 2 * LANES].astype(jnp.bfloat16)
            term = term.astype(jnp.float32)
            shared = term if shared is None else shared + term
        part_ref[:, width + RANK :] = shared.astype(jnp.bfloat16)
        part_ref[:, width : width + RANK] = nt(dkv_ref[...], kvup_ref[...]).astype(jnp.bfloat16)


def attend_back(q, k, v, d_heads, logs, cosine, sine, kvup, query_blocks, heads, scale):
    length = q.shape[0]
    part_width = query_blocks[0].shape[0] * len(query_blocks) + RANK + LANES
    blocks = length // STEP
    query_width = heads * (NOPE + ROPE)
    return pl.pallas_call(
        functools.partial(attend_back_kernel, heads, blocks, scale),
        grid=(blocks,),
        in_specs=[
            by_rows(heads * 2 * LANES),
            fixed(k.shape),
            fixed(v.shape),
            by_rows(heads * VDIM),
            pl.BlockSpec((heads, STEP, 1), lambda i: (0, i, 0)),
            by_rows(LANES),
            by_rows(LANES),
            fixed(kvup.shape),
        ]
        + [fixed(b.shape) for b in query_blocks],
        out_specs=[by_rows(query_width), fixed(k.shape), fixed((length, part_width))],
        out_shape=[
            jax.ShapeDtypeStruct((length, query_width), jnp.bfloat16),
            jax.ShapeDtypeStruct(k.shape, jnp.bfloat16),
            jax.ShapeDtypeStruct((length, part_width), jnp.bfloat16),
        ],
        scratch_shapes=[pltpu.VMEM(k.shape, jnp.float32), pltpu.VMEM(v.shape, jnp.float32)],
        cost_estimate=pl.CostEstimate(
            flops=2 * heads * length * length * 1100,
            bytes_accessed=12 * 2**20,
            transcendentals=heads * length * length,
        ),
        name="attend_back",
    )(q, k, v, d_heads, logs, cosine, sine, kvup, *query_blocks)


def load_pieces(pieces, sems):
    copies = [
        pltpu.make_async_copy(source, target, sems.at[at])
        for at, (source, target) in enumerate(pieces)
    ]

    @pl.when(pl.program_id(0) == 0)
    def _():
        for copy in copies:
            copy.start()

    def take(low, high):
        @pl.when(pl.program_id(0) == 0)
        def _():
            for copy in copies[low:high]:
                copy.wait()

    return take


def stacked(refs, whole, columns):
    size = refs[0].shape[1 if columns else 0]
    pieces = []
    for r, ref in enumerate(refs):
        span = pl.ds(r * size, size)
        pieces.append((ref, whole.at[:, span] if columns else whole.at[span]))
    return pieces


def minor_kernel(att_ref, branch_ref, low_ref, keyval_ref, query_ref, first_ref, *out_refs):
    shard = lax.axis_index(SHARD)
    depth = out_refs[0].shape[1]
    narrow = low_ref.shape[1] // len(out_refs)
    for r, out_ref in enumerate(out_refs):
        wide = slice(r * depth, (r + 1) * depth)
        place = pl.multiple_of(jnp.bitwise_xor(shard, r) * narrow, narrow)
        top = att_ref.shape[1]
        out_ref[:top] = tn(att_ref[...], branch_ref[:, wide]).astype(jnp.bfloat16)
        out_ref[top : top + narrow] = tn(
            low_ref[:, pl.ds(place, narrow)], keyval_ref[...]
        ).astype(jnp.bfloat16)
        out_ref[top + narrow :] = tn(query_ref[...], first_ref[:, wide]).astype(jnp.bfloat16)


def minor_grads(attended, branch, low, keyval, query, first, shards):
    depth = first.shape[1] // shards
    rows = attended.shape[1] + low.shape[1] // shards + query.shape[1]
    return pl.pallas_call(
        minor_kernel,
        in_specs=[pl.BlockSpec(memory_space=pltpu.VMEM)] * 6,
        out_specs=[pl.BlockSpec(memory_space=pltpu.VMEM)] * shards,
        out_shape=[jax.ShapeDtypeStruct((rows, depth), jnp.bfloat16)] * shards,
        cost_estimate=pl.CostEstimate(
            flops=2 * first.shape[0] * rows * first.shape[1],
            bytes_accessed=16 * 2**20,
            transcendentals=0,
        ),
        name="minor",
    )(attended, branch, low, keyval, query, first)


def hidden_kernel(count, ff, *refs):
    x_ref, gate_ref = refs[:2]
    sources = refs[2 : 2 + 2 * count]
    hid_ref, a_ref, b_ref, gates, ups, sems = refs[2 + 2 * count :]
    pieces = stacked(sources[:count], gates, False) + stacked(sources[count:], ups, False)
    take = load_pieces(pieces, sems)
    take(0, len(pieces))
    total = gates.shape[1]
    x = x_ref[...]
    for low in range(0, total, CHUNK):
        high = min(low + CHUNK, total)
        gate = nn(x, gates[:, low:high])
        upper = nn(x, ups[:, low:high])
        sigma = jax.nn.sigmoid(gate)
        silu = gate * sigma
        slope = upper * sigma * (1.0 + gate * (1.0 - sigma))
        factor = gate_ref[...]
        if high > ff:
            column = lax.broadcasted_iota(jnp.int32, gate.shape, 1)
            factor = jnp.where(column < ff - low, factor, 1.0)
        hid_ref[:, low:high] = (silu * upper * factor).astype(jnp.bfloat16)
        a_ref[:, low:high] = (slope * factor).astype(jnp.bfloat16)
        b_ref[:, low:high] = (silu * factor).astype(jnp.bfloat16)


def hidden_pass(x, gate, gate_blocks, up_blocks, ff):
    length, width = x.shape
    count = len(gate_blocks)
    blocks = [*gate_blocks, *up_blocks]
    total = gate_blocks[0].shape[1]
    return pl.pallas_call(
        functools.partial(hidden_kernel, count, ff),
        grid=(length // WIDE,),
        in_specs=[by_rows(width, WIDE), by_rows(1, WIDE)]
        + [pl.BlockSpec(memory_space=pl.ANY)] * len(blocks),
        out_specs=[by_rows(total, WIDE)] * 3,
        out_shape=[jax.ShapeDtypeStruct((length, total), jnp.bfloat16)] * 3,
        scratch_shapes=[pltpu.VMEM((width, total), jnp.bfloat16)] * 2
        + [pltpu.SemaphoreType.DMA((2 * count,))],
        cost_estimate=pl.CostEstimate(
            flops=4 * length * width * total, bytes_accessed=32 * 2**20, transcendentals=0
        ),
        compiler_params=pltpu.CompilerParams(vmem_limit_bytes=60 * 2**20),
        name="hidden_pass",
    )(x, gate, *blocks)


def slope_kernel(count, *refs):
    g_ref, a_ref, b_ref = refs[:3]
    sources = refs[3 : 3 + 3 * count]
    dg_ref, du_ref, part_ref, downs, gates, ups, sems = refs[3 + 3 * count :]
    pieces = (
        stacked(sources[:count], downs, True)
        + stacked(sources[count : 2 * count], gates, False)
        + stacked(sources[2 * count :], ups, False)
    )
    take = load_pieces(pieces, sems)
    take(0, count)
    total = downs.shape[0]
    g = g_ref[...]
    for low in range(0, total, CHUNK):
        high = min(low + CHUNK, total)
        d_hidden = nt(g, downs[low:high])
        dg_ref[:, low:high] = (d_hidden * a_ref[:, low:high].astype(jnp.float32)).astype(
            jnp.bfloat16
        )
        du_ref[:, low:high] = (d_hidden * b_ref[:, low:high].astype(jnp.float32)).astype(
            jnp.bfloat16
        )
    take(count, len(pieces))
    d_gate, d_up = dg_ref[...], du_ref[...]
    width = g.shape[1]
    for low in range(0, width, CHUNK):
        high = min(low + CHUNK, width)
        part_ref[:, low:high] = (nt(d_gate, gates[low:high]) + nt(d_up, ups[low:high])).astype(
            jnp.bfloat16
        )


def slope_pass(g, a, b, down_blocks, gate_blocks, up_blocks):
    length, width = g.shape
    count = len(gate_blocks)
    blocks = [*down_blocks, *gate_blocks, *up_blocks]
    total = gate_blocks[0].shape[1]
    return pl.pallas_call(
        functools.partial(slope_kernel, count),
        grid=(length // NARROW,),
        in_specs=[by_rows(width, NARROW), by_rows(total, NARROW), by_rows(total, NARROW)]
        + [pl.BlockSpec(memory_space=pl.ANY)] * len(blocks),
        out_specs=[by_rows(total, NARROW), by_rows(total, NARROW), by_rows(width, NARROW)],
        out_shape=[
            jax.ShapeDtypeStruct((length, total), jnp.bfloat16),
            jax.ShapeDtypeStruct((length, total), jnp.bfloat16),
            jax.ShapeDtypeStruct((length, width), jnp.bfloat16),
        ],
        scratch_shapes=[
            pltpu.VMEM((total, width), jnp.bfloat16),
            pltpu.VMEM((width, total), jnp.bfloat16),
            pltpu.VMEM((width, total), jnp.bfloat16),
            pltpu.SemaphoreType.DMA((3 * count,)),
        ],
        cost_estimate=pl.CostEstimate(
            flops=6 * length * width * total, bytes_accessed=40 * 2**20, transcendentals=0
        ),
        compiler_params=pltpu.CompilerParams(vmem_limit_bytes=62 * 2**20),
        name="slope_pass",
    )(g, a, b, *blocks)


def rotate(values, cosine, sine):
    half_depth = values.shape[-1] // 2
    first = values[..., :half_depth]
    second = values[..., half_depth:]
    return jnp.concatenate([first * cosine - second * sine, second * cosine + first * sine], -1)


def norm_forward(values, scaling):
    inverse = lax.rsqrt(jnp.mean(values * values, -1, keepdims=True) + EPSILON)
    return (values * inverse * scaling, inverse)


def norm_backward(values, inverse, scaling, upstream):
    weighted = upstream * scaling
    scaling_grad = jnp.sum(upstream * values * inverse, 0)
    centre = jnp.mean(weighted * values, -1, keepdims=True)
    return (inverse * weighted - values * inverse**3 * centre, scaling_grad)


def gather_seq(block):
    return lax.all_gather(block, SEQ, axis=0, tiled=True)


def scatter_seq(partial):
    return lax.psum_scatter(
        partial.astype(jnp.bfloat16), SEQ, scatter_dimension=0, tiled=True
    ).astype(jnp.float32)


def settle_kernel(n, shards, terms_ref, out_ref, from_seq, joined, from_shard, sends, seq_recv, shard_recv):
    me = lax.axis_index(SEQ)
    my_shard = lax.axis_index(SHARD)
    barrier = pltpu.get_barrier_semaphore()
    for hop in range(1, n):
        pl.semaphore_signal(
            barrier, inc=1, device_id={SEQ: (me + hop) % n}, device_id_type=MESH
        )
    for hop in range(1, shards):
        pl.semaphore_signal(
            barrier, inc=1, device_id={SHARD: (my_shard + hop) % shards}, device_id_type=MESH
        )
    pl.semaphore_wait(barrier, n + shards - 2)
    first = []
    for hop in range(1, n):
        target = (me + hop) % n
        copy = pltpu.make_async_remote_copy(
            src_ref=terms_ref.at[:, target],
            dst_ref=from_seq.at[hop - 1],
            send_sem=sends.at[hop - 1],
            recv_sem=seq_recv.at[hop - 1],
            device_id={SEQ: target},
            device_id_type=MESH,
        )
        copy.start()
        first.append(copy)
    total = terms_ref[:, me]
    for hop in range(1, n):
        first[hop - 1].wait_recv()
        total = total + from_seq[hop - 1]
    joined[...] = total
    second = []
    for hop in range(1, shards):
        target = (my_shard + hop) % shards
        place = target
        if shards == 4:
            low, high = my_shard % 2, my_shard // 2
            low = low + hop % 2 - 2 * low * (hop % 2)
            high = high + hop // 2 - 2 * high * (hop // 2)
            target, place = 2 * high + low, hop
        copy = pltpu.make_async_remote_copy(
            src_ref=joined.at[place],
            dst_ref=from_shard.at[hop - 1],
            send_sem=sends.at[n - 1 + hop - 1],
            recv_sem=shard_recv.at[hop - 1],
            device_id={SHARD: target},
            device_id_type=MESH,
        )
        copy.start()
        second.append(copy)
    total = joined[0 if shards == 4 else my_shard]
    for hop in range(1, shards):
        second[hop - 1].wait_recv()
        total = total + from_shard[hop - 1]
    out_ref[...] = total
    for copy in first + second:
        copy.wait_send()


def settle(n, shards, terms, identity):
    shape = terms.shape[2:]
    return pl.pallas_call(
        functools.partial(settle_kernel, n, shards),
        out_shape=jax.ShapeDtypeStruct(shape, jnp.float32),
        in_specs=[pl.BlockSpec(memory_space=pltpu.VMEM)],
        out_specs=pl.BlockSpec(memory_space=pltpu.VMEM),
        scratch_shapes=[
            pltpu.VMEM((n - 1, shards) + shape, jnp.float32),
            pltpu.VMEM((shards,) + shape, jnp.float32),
            pltpu.VMEM((shards - 1,) + shape, jnp.float32),
            pltpu.SemaphoreType.DMA((n + shards - 2,)),
            pltpu.SemaphoreType.DMA((n - 1,)),
            pltpu.SemaphoreType.DMA((shards - 1,)),
        ],
        compiler_params=pltpu.CompilerParams(collective_id=identity, has_side_effects=True),
        name="settle",
    )(terms)


def duplex_kernel(n, parts, sums, *refs):
    if sums:
        (x_ref, part_ref, all_ref, sum_ref, mine, other, left_in, right_in) = refs[:8]
        (pair_send, pair_recv, line_send, line_recv) = refs[8:12]
    else:
        x_ref, all_ref = refs[:2]
    copy_send, copy_recv, local = refs[-3:]
    half = n // 2
    me = lax.axis_index(SEQ)
    core = me % 2
    place = me // 2
    partner = place * 2 + 1 - core
    below, above = me - 2, me + 2
    has_below, has_above = place > 0, place < half - 1

    def remote(source, target, send, recv, device):
        return pltpu.make_async_remote_copy(
            src_ref=source,
            dst_ref=target,
            send_sem=send,
            recv_sem=recv,
            device_id={SEQ: device},
            device_id_type=MESH,
        )

    def pair_copy(at):
        return remote(
            part_ref.at[at * 2 + 1 - core], other.at[at], pair_send.at[at], pair_recv.at[at], partner
        )

    piece = x_ref.shape[0] // parts

    def rows_of(part):
        return pl.ds(part * piece, piece)

    def sum_up(at, part):
        span = rows_of(part)
        return remote(
            mine.at[at, span],
            left_in.at[at, span],
            line_send.at[0, at, part],
            line_recv.at[0, at, part],
            above,
        )

    def sum_down(at, part):
        span = rows_of(part)
        return remote(
            mine.at[at, span],
            right_in.at[at, span],
            line_send.at[1, at, part],
            line_recv.at[1, at, part],
            below,
        )

    def block_copy(source, block, way, step, part, device):
        span = rows_of(part)
        return remote(
            source.at[span],
            all_ref.at[block, span],
            copy_send.at[way, step, part],
            copy_recv.at[way, step, part],
            device,
        )

    order = []
    for at in range(half):
        for item in (half - 1 - at, at):
            if item not in order:
                order.append(item)
    for at in order if sums else ():
        pltpu.make_async_copy(part_ref.at[at * 2 + core], mine.at[at], local.at[at]).start()
    keep = pltpu.make_async_copy(x_ref, all_ref.at[me], local.at[half])
    keep.start()

    barrier = pltpu.get_barrier_semaphore()
    pl.semaphore_signal(barrier, inc=1, device_id={SEQ: partner}, device_id_type=MESH)

    @pl.when(has_below)
    def _():
        pl.semaphore_signal(barrier, inc=1, device_id={SEQ: below}, device_id_type=MESH)

    @pl.when(has_above)
    def _():
        pl.semaphore_signal(barrier, inc=1, device_id={SEQ: above}, device_id_type=MESH)

    @pl.when(has_below & has_above)
    def _():
        pl.semaphore_wait(barrier, 3)

    @pl.when(jnp.logical_not(has_below & has_above))
    def _():
        pl.semaphore_wait(barrier, 2)

    for at in order if sums else ():
        pair_copy(at).start()

    for part in range(parts):

        @pl.when(has_above)
        def _():
            block_copy(x_ref, me, 0, 0, part, above).start()

        @pl.when(has_below)
        def _():
            block_copy(x_ref, me, 1, 0, part, below).start()

        block_copy(x_ref, me, 2, 0, part, partner).start()

    def merge(at, part, incoming):
        span = rows_of(part)
        total = mine[at, span].astype(jnp.float32) + other[at, span].astype(jnp.float32)
        if incoming is not None:
            total = total + incoming[at, span].astype(jnp.float32)
        mine[at, span] = total.astype(mine.dtype)

    def load(at):
        return pltpu.make_async_copy(part_ref.at[at * 2 + core], mine.at[at], local.at[at])

    def ready(at):
        load(at).wait()
        pair_copy(at).wait_recv()

    def relay(slot, part):
        step = slot - 1

        @pl.when(place > step)
        def _():
            block = me - 2 * (step + 1)
            block_copy(x_ref, block, 0, step, part, above).wait_recv()

            @pl.when(has_above)
            def _():
                block_copy(all_ref.at[block], block, 0, step + 1, part, above).start()

            block_copy(all_ref.at[block], block, 2, 1 + step, part, partner).start()

        @pl.when(place < half - 1 - step)
        def _():
            block = me + 2 * (step + 1)
            block_copy(x_ref, block, 1, step, part, below).wait_recv()

            @pl.when(has_below)
            def _():
                block_copy(all_ref.at[block], block, 1, step + 1, part, below).start()

            block_copy(all_ref.at[block], block, 2, half + step, part, partner).start()

    for slot in range(2 * half - 2):
        rise = half - 1 - (slot - place)
        fall = slot - (half - 1 - place)
        if 1 <= slot <= half - 1:
            for part in range(parts):
                relay(slot, part)
        if not sums:
            continue

        @pl.when((rise < half) & (rise > place))
        def _():
            ready(rise)
            for part in range(parts):

                @pl.when(has_below)
                def _():
                    sum_up(rise, part).wait_recv()
                    merge(rise, part, left_in)

                @pl.when(jnp.logical_not(has_below))
                def _():
                    merge(rise, part, None)

                sum_up(rise, part).start()

        @pl.when((fall >= 0) & (fall < place))
        def _():
            ready(fall)
            for part in range(parts):

                @pl.when(has_above)
                def _():
                    sum_down(fall, part).wait_recv()
                    merge(fall, part, right_in)

                @pl.when(jnp.logical_not(has_above))
                def _():
                    merge(fall, part, None)

                sum_down(fall, part).start()

    if sums:
        ready(place)
        for part in range(parts):

            @pl.when(has_below)
            def _():
                sum_up(place, part).wait_recv()

            @pl.when(has_above)
            def _():
                sum_down(place, part).wait_recv()

        total = mine[place].astype(jnp.float32) + other[place].astype(jnp.float32)
        low = jnp.where(has_below, left_in[place].astype(jnp.float32), 0.0)
        high = jnp.where(has_above, right_in[place].astype(jnp.float32), 0.0)
        sum_ref[...] = total + low + high

    keep.wait()
    for at in range(half if sums else 0):
        pair_copy(at).wait_send()
    for part in range(parts):
        block_copy(x_ref, partner, 2, 0, part, partner).wait_recv()
        block_copy(x_ref, me, 2, 0, part, partner).wait_send()

        @pl.when(has_above)
        def _():
            block_copy(x_ref, me, 0, 0, part, above).wait_send()

        @pl.when(has_below)
        def _():
            block_copy(x_ref, me, 1, 0, part, below).wait_send()

        for step in range(half - 1):
            up, down = half - 1 - step, step
            if sums:

                @pl.when(place < up)
                def _():
                    sum_up(up, part).wait_send()

                @pl.when(place > down)
                def _():
                    sum_down(down, part).wait_send()

            @pl.when(place > step)
            def _():
                block = me - 2 * (step + 1)

                @pl.when(has_above)
                def _():
                    block_copy(x_ref, block, 0, step + 1, part, above).wait_send()

                block_copy(x_ref, block, 2, 1 + step, part, partner).wait_send()
                there = partner - 2 * (step + 1)
                block_copy(x_ref, there, 2, 1 + step, part, partner).wait_recv()

            @pl.when(place < half - 1 - step)
            def _():
                block = me + 2 * (step + 1)

                @pl.when(has_below)
                def _():
                    block_copy(x_ref, block, 1, step + 1, part, below).wait_send()

                block_copy(x_ref, block, 2, half + step, part, partner).wait_send()
                there = partner + 2 * (step + 1)
                block_copy(x_ref, there, 2, half + step, part, partner).wait_recv()


def duplex(n, block, partial, identity, parts=2):
    half = n // 2
    rows, wide = partial.shape[0] // n, partial.shape[1]
    line = pltpu.VMEM((half, rows, wide), partial.dtype)
    gathered, total = pl.pallas_call(
        functools.partial(duplex_kernel, n, parts, True),
        out_shape=[
            jax.ShapeDtypeStruct((n,) + block.shape, block.dtype),
            jax.ShapeDtypeStruct((rows, wide), jnp.float32),
        ],
        in_specs=[
            pl.BlockSpec(memory_space=pltpu.VMEM),
            pl.BlockSpec(memory_space=pl.ANY),
        ],
        out_specs=[
            pl.BlockSpec(memory_space=pl.ANY),
            pl.BlockSpec(memory_space=pltpu.VMEM),
        ],
        scratch_shapes=[
            line,
            line,
            line,
            line,
            pltpu.SemaphoreType.DMA((half,)),
            pltpu.SemaphoreType.DMA((half,)),
            pltpu.SemaphoreType.DMA((2, half, parts)),
            pltpu.SemaphoreType.DMA((2, half, parts)),
            pltpu.SemaphoreType.DMA((3, 2 * half, parts)),
            pltpu.SemaphoreType.DMA((3, 2 * half, parts)),
            pltpu.SemaphoreType.DMA((half + 1,)),
        ],
        compiler_params=pltpu.CompilerParams(collective_id=identity, has_side_effects=True),
        cost_estimate=pl.CostEstimate(
            flops=45_000_000_000, bytes_accessed=2**24, transcendentals=0
        ),
        name="duplex",
    )(block, partial.reshape(n, rows, wide))
    return gathered.reshape(n * block.shape[0], block.shape[1]), total


def chain_gather(n, block, identity, parts=2):
    half = n // 2
    return pl.pallas_call(
        functools.partial(duplex_kernel, n, parts, False),
        out_shape=jax.ShapeDtypeStruct((n,) + block.shape, block.dtype),
        in_specs=[pl.BlockSpec(memory_space=pltpu.VMEM)],
        out_specs=pl.BlockSpec(memory_space=pl.ANY),
        scratch_shapes=[
            pltpu.SemaphoreType.DMA((3, 2 * half, parts)),
            pltpu.SemaphoreType.DMA((3, 2 * half, parts)),
            pltpu.SemaphoreType.DMA((half + 1,)),
        ],
        compiler_params=pltpu.CompilerParams(collective_id=identity, has_side_effects=True),
        cost_estimate=pl.CostEstimate(
            flops=25_000_000_000, bytes_accessed=2**22, transcendentals=0
        ),
        name="chain",
    )(block)


ACROSS = ([(0, 1), (1, 0), (2, 3), (3, 2)], [(0, 2), (2, 0), (1, 3), (3, 1)])


def swap_with(block, side):
    return lax.ppermute(block, SHARD, ACROSS[side])


def gather_blocks(weight, axis, side):
    if lax.axis_size(SHARD) != 4:
        return [lax.all_gather(weight, SHARD, axis=axis, tiled=True)]
    return gather_far(gather_near(weight, axis), side)


def gather_near(weight, axis):
    if lax.axis_size(SHARD) != 4:
        return [lax.all_gather(weight, SHARD, axis=axis, tiled=True)]
    return [weight, swap_with(weight, 0), swap_with(weight, 1)]


def gather_far(blocks, side, token=None):
    if len(blocks) == 1:
        return blocks
    relay = blocks[1 + side]
    relay = relay if token is None else after(relay, token)
    return [*blocks, swap_with(relay, 1 - side)]


def after(value, token):
    return lax.optimization_barrier((value, token))[0]


def scatter_blocks(blocks, axis, side, join_token, sum_token, one_token=None):
    if lax.axis_size(SHARD) != 4:
        blocks = [block.astype(jnp.bfloat16) for block in blocks]
        return (lax.psum_scatter(blocks[0], SHARD, scatter_dimension=axis, tiled=True),)
    blocks = [lax.optimization_barrier(block.astype(jnp.bfloat16)) for block in blocks]
    far = swap_with(blocks[3], side)
    one = blocks[1 + side] if one_token is None else after(blocks[1 + side], one_token)
    first = swap_with(one, side)
    far = after(far, join_token)
    joined = (blocks[2 - side].astype(jnp.float32) + far.astype(jnp.float32)).astype(
        jnp.bfloat16
    )
    second = swap_with(joined, 1 - side)
    second = after(second, sum_token)
    return blocks[0], first, second


def add_up(terms, rows=slice(None), columns=slice(None)):
    total = None
    for term in terms:
        term = term[rows, columns].astype(jnp.float32)
        total = term if total is None else total + term
    return total


def local_order(values, axis):
    if lax.axis_size(SHARD) != 4:
        return values
    size = values.shape[axis] // 4
    shard = lax.axis_index(SHARD)
    return jnp.concatenate(
        [
            lax.dynamic_slice_in_dim(values, jnp.bitwise_xor(shard, place) * size, size, axis)
            for place in range(4)
        ],
        axis,
    )


def cut(values, axis):
    if lax.axis_size(SHARD) != 4:
        return [values]
    size = values.shape[axis] // 4
    return [lax.slice_in_dim(values, r * size, (r + 1) * size, axis=axis) for r in range(4)]


def on_device(
    inputs,
    attn_gain,
    query_project_weight,
    latent_project_weight,
    latent_gain,
    latent_keyval_weight,
    attention_output_weight,
    ffn_gain,
    shared_gate,
    shared_up,
    shared_down,
    expert_gate,
    expert_up,
    expert_down,
    routes,
    slots,
    gates,
    cotangent,
):
    tok_rows = inputs.shape[1]
    model_width = inputs.shape[2]
    groups = lax.axis_size(SEQ)
    shards = lax.axis_size(SHARD)
    me = lax.axis_index(SEQ)
    heads = HEADS // groups
    experts = EXP_DEV * groups
    capacity = 9 * tok_rows * TOPK // (8 * experts)
    length = tok_rows * groups
    score_scale = (NOPE + ROPE) ** (-0.5)
    own_start = me * tok_rows
    one_width = attn_gain.shape[0]
    lat_width = latent_gain.shape[0]
    ff = expert_gate.shape[2]
    shared_ff = shared_gate.shape[1]
    side = -(-shared_ff // LANES) * LANES

    own_inputs = local_order(inputs.reshape(tok_rows, model_width), 1)
    inputs_all = gather_seq(own_inputs)
    upstream = local_order(cotangent.reshape(tok_rows, model_width), 1)
    route_rows = routes.reshape(tok_rows, TOPK)
    slot_rows = slots.reshape(tok_rows, TOPK)
    kept = (route_rows.T[:, None, :] == jnp.arange(experts)[None, :, None]) & (
        slot_rows.T < capacity
    )[:, None, :]
    gate_table = jnp.sum(
        jnp.where(kept, gates.reshape(tok_rows, TOPK).T.astype(jnp.float32)[:, None, :], 0.0), 0
    ).astype(jnp.bfloat16)

    def padded_row(gain):
        return jnp.pad(gain, (0, LANES - ROPE - gain.shape[0]))[None]

    side_rows = jnp.concatenate(
        [
            padded_row(attn_gain),
            padded_row(ffn_gain),
            padded_row(latent_gain),
            jnp.zeros((one_width - 3, LANES - ROPE), jnp.bfloat16),
        ],
        0,
    )
    small_own = jnp.concatenate([latent_project_weight, side_rows], 1)
    small_rows = jnp.concatenate(gather_blocks(small_own, 0, 0), 0)
    small_rows = jnp.concatenate(
        [
            small_rows,
            jnp.pad(gate_table, ((0, EXTRA - experts), (0, small_rows.shape[1] - tok_rows))),
        ],
        0,
    )
    small_seq = chain_gather(groups, small_rows, 4)
    gate_column = (
        lax.dynamic_index_in_dim(
            small_seq[:, shards * one_width :, :tok_rows], me, 1, keepdims=False
        )
        .reshape(length, 1)
        .astype(jnp.float32)
    )
    gain_rows = (
        small_seq[:, : shards * one_width, RANK + ROPE :]
        .reshape(groups, shards, one_width, -1)[:, :, :3]
        .astype(jnp.float32)
        .transpose(2, 1, 0, 3)
    )
    first_norm_weight = gain_rows[0, :, :, :one_width].reshape(-1)
    second_norm_weight = gain_rows[1, :, :, :one_width].reshape(-1)
    latent_norm_weight = local_order(gain_rows[2, :, :, :lat_width].reshape(-1), 0)

    spare = side - shared_ff
    gate_own = jnp.pad(
        jnp.concatenate([expert_gate[0], shared_gate], 1), ((0, 0), (0, spare))
    )
    up_own = jnp.pad(jnp.concatenate([expert_up[0], shared_up], 1), ((0, 0), (0, spare)))
    down_own = jnp.pad(jnp.concatenate([expert_down[0], shared_down], 0), ((0, spare), (0, 0)))
    query_blocks = gather_blocks(query_project_weight, 0, 0)
    kvup_blocks = gather_blocks(latent_keyval_weight, 0, 0)
    out_blocks = gather_blocks(attention_output_weight, 1, 0)
    gate_near = gather_near(gate_own, 0)
    up_near = gather_near(up_own, 0)
    down_near = gather_near(down_own, 1)
    full_kvup = local_order(jnp.concatenate(kvup_blocks, 0), 0)
    full_out = jnp.concatenate(out_blocks, 1)

    residual_stream = own_inputs.astype(jnp.float32)
    cosine, sine = rope_lanes(jnp.arange(length))
    first_all, q_all, k_all, v_all, latent, latent_all = front(
        inputs_all,
        first_norm_weight[None],
        latent_norm_weight[None],
        cosine,
        sine,
        full_kvup,
        query_blocks,
        small_seq,
        shards,
        heads,
    )
    gate_blocks = gather_far(gate_near, 0, q_all)
    up_blocks = gather_far(up_near, 1, q_all)
    down_blocks = gather_far(down_near, 1)
    attended, logs = attend(q_all, k_all, v_all, heads, score_scale)
    attended_part = nn(attended, full_out)
    upstream_all, attended_sum = duplex(groups, upstream, attended_part.astype(jnp.bfloat16), 1)
    middle = residual_stream + attended_sum
    normed_two, inv_two = norm_forward(middle, second_norm_weight)
    second_all = chain_gather(groups, normed_two.astype(jnp.bfloat16), 5)
    second_all = second_all.reshape(length, model_width)

    hidden, slope_gate, slope_up = hidden_pass(second_all, gate_column, gate_blocks, up_blocks, ff)
    d_gate, d_up, second_part = slope_pass(
        upstream_all, slope_gate, slope_up, down_blocks, gate_blocks, up_blocks
    )
    d_second = scatter_seq(second_part)
    hidden_late = after(hidden, d_gate)
    d_down = [tn(hidden_late, part) for part in cut(upstream_all, 1)[1:]]
    second_parts = cut(second_all, 1)
    count = len(second_parts)
    d_wgate = [tn(part, d_gate) for part in second_parts[1:]]
    d_wup = [tn(part, d_up) for part in second_parts[2:]]
    down_part = nn(hidden, jnp.concatenate(down_blocks, 1)).astype(jnp.bfloat16)

    d_middle_norm, d_gain_two = norm_backward(middle, inv_two, second_norm_weight, d_second)
    d_middle = upstream.astype(jnp.float32) + d_middle_norm
    d_branch_all, added = duplex(groups, d_middle.astype(jnp.bfloat16), down_part, 2)
    output = local_order((middle + added).astype(jnp.bfloat16), 1).reshape(1, tok_rows, model_width)
    d_heads = nt(d_branch_all, full_out).astype(jnp.bfloat16)
    d_query, d_keyval, back_part = attend_back(
        q_all,
        k_all,
        v_all,
        d_heads,
        logs,
        cosine,
        sine,
        full_kvup,
        query_blocks,
        heads,
        score_scale,
    )
    back_sum = scatter_seq(back_part)
    first_back, latent_back = back_sum[:, :model_width], back_sum[:, model_width:]
    if shards == 4:
        d_minor = minor_grads(
            attended, d_branch_all, latent_all, d_keyval, d_query, first_all, shards
        )
    else:
        d_wout = [tn(attended, part).astype(jnp.bfloat16) for part in cut(d_branch_all, 1)]
        d_wquery = [tn(part, d_query).astype(jnp.bfloat16) for part in cut(first_all, 1)]
        d_wkvup = cut(local_order(tn(latent_all, d_keyval).astype(jnp.bfloat16), 0), 0)

    own_latent = lax.dynamic_slice_in_dim(latent, own_start, tok_rows, 0)
    half = ROPE // 2
    cos_own = lax.dynamic_slice_in_dim(cosine, own_start, tok_rows, 0)[:, :half]
    sin_own = lax.dynamic_slice_in_dim(sine, own_start, tok_rows, 0)[:, half:ROPE]
    inv_latent = norm_forward(own_latent, latent_norm_weight)[1]
    d_rope = rotate(latent_back[:, RANK : RANK + ROPE], cos_own, -sin_own)
    d_compressed, d_gain_latent = norm_backward(
        own_latent, inv_latent, latent_norm_weight, latent_back[:, :RANK]
    )
    d_latent = jnp.concatenate(
        [d_compressed, d_rope, jnp.zeros((tok_rows, LANES - ROPE), jnp.float32)], -1
    ).astype(jnp.bfloat16)
    d_latent_all = gather_seq(d_latent)
    inv_one = norm_forward(residual_stream, first_norm_weight)[1]
    wide_latent = jnp.concatenate(
        [
            small_seq[:, r * one_width : (r + 1) * one_width].reshape(groups * one_width, -1)
            for r in range(shards)
        ],
        0,
    )
    d_first = first_back + nt(d_latent, wide_latent)
    d_resid, d_gain_one = norm_backward(residual_stream, inv_one, first_norm_weight, d_first)
    input_grad = local_order(d_middle + d_resid, 1).reshape(1, tok_rows, model_width)
    first_late = after(first_all, d_latent)
    own_columns = jnp.concatenate(
        [
            lax.dynamic_slice_in_dim(
                first_late, (place * groups + me) * one_width, one_width, 1
            )
            for place in range(shards)
        ],
        1,
    )
    d_wlatent = cut(tn(own_columns, d_latent_all).astype(jnp.bfloat16), 0)

    terms = jnp.concatenate(
        [
            d_gain_one.reshape(shards, groups, one_width),
            d_gain_two.reshape(shards, groups, one_width),
            local_order(d_gain_latent, 0).reshape(shards, groups, lat_width),
        ],
        2,
    )
    terms = jnp.pad(terms, ((0, 0), (0, 0), (0, 1024 - terms.shape[2])))
    terms = terms.reshape(shards, groups, 8, 128)
    gain_grads = settle(groups, shards, terms, 9).reshape(-1)
    d_down.insert(0, tn(hidden, cut(after(upstream_all, d_keyval), 1)[0]))
    second_late = cut(after(second_all, d_keyval), 1)
    d_wgate.insert(0, tn(second_late[0], d_gate))
    d_wup = [tn(part, d_up) for part in second_late[: count - len(d_wup)]] + d_wup
    gate_grad = scatter_blocks(d_wgate, 0, 0, d_keyval, d_wlatent[0])
    up_grad = scatter_blocks(d_wup, 0, 1, d_keyval, d_wlatent[0])
    down_grad = scatter_blocks(d_down, 1, 0, second_part, d_wgate[0])
    if shards == 4:
        minor = scatter_blocks(d_minor, 0, 1, gain_grads, d_wlatent[0], gain_grads)
        top, narrow = attended.shape[1], RANK // shards
        out_grad = add_up(minor, rows=slice(0, top))
        kvup_grad = add_up(minor, rows=slice(top, top + narrow))
        query_grad = add_up(minor, rows=slice(top + narrow, None)).T
    else:
        out_grad = add_up(scatter_blocks(d_wout, 1, 1, gain_grads, d_wlatent[0]))
        kvup_grad = add_up(scatter_blocks(d_wkvup, 0, 1, gain_grads, d_wlatent[0]))
        query_grad = add_up(scatter_blocks(d_wquery, 0, 1, gain_grads, d_wlatent[0]))
    latent_grad = scatter_blocks(d_wlatent, 0, 1, first_back, first_back)
    return (
        output,
        input_grad,
        gain_grads[:one_width],
        query_grad,
        add_up(latent_grad, columns=slice(0, RANK + ROPE)),
        gain_grads[2 * one_width : 2 * one_width + lat_width],
        kvup_grad,
        out_grad,
        gain_grads[one_width : 2 * one_width],
        add_up(gate_grad, columns=slice(ff, ff + shared_ff)),
        add_up(up_grad, columns=slice(ff, ff + shared_ff)),
        add_up(down_grad, rows=slice(ff, ff + shared_ff)),
        add_up(gate_grad, columns=slice(0, ff))[None],
        add_up(up_grad, columns=slice(0, ff))[None],
        add_up(down_grad, rows=slice(0, ff))[None],
    )


def solution(mesh):
    in_specs = (
        P(SHARD, SEQ, None),
        P((SHARD, SEQ)),
        P(SHARD, SEQ),
        P((SHARD, SEQ), None),
        P((SHARD, SEQ)),
        P(SHARD, SEQ),
        P(SEQ, SHARD),
        P((SHARD, SEQ)),
        P(SHARD, SEQ),
        P(SHARD, SEQ),
        P(SEQ, SHARD),
        P(SEQ, SHARD, None),
        P(SEQ, SHARD, None),
        P(SEQ, None, SHARD),
        P(SHARD, SEQ, None),
        P(SHARD, SEQ, None),
        P(SHARD, SEQ, None),
        P(SHARD, SEQ, None),
    )
    out_specs = (
        P(SHARD, SEQ, None),
        P(SHARD, SEQ, None),
        P((SHARD, SEQ)),
        P(SHARD, SEQ),
        P((SHARD, SEQ), None),
        P((SHARD, SEQ)),
        P(SHARD, SEQ),
        P(SEQ, SHARD),
        P((SHARD, SEQ)),
        P(SHARD, SEQ),
        P(SHARD, SEQ),
        P(SEQ, SHARD),
        P(SEQ, SHARD, None),
        P(SEQ, SHARD, None),
        P(SEQ, None, SHARD),
    )

    return jax.shard_map(
        on_device, mesh=mesh, in_specs=in_specs, out_specs=out_specs, check_vma=False
    )
```

```python
import functools

import jax
import jax.numpy as jnp
from jax import lax
from jax.experimental import pallas as pl
from jax.experimental.pallas import tpu as pltpu
from jax.sharding import PartitionSpec as P

HEADS = 16
NOPE = 128
ROPE = 64
VDIM = 128
RANK = 512
TOPK = 6
EXP_DEV = 1
EXTRA = 32


EPSILON = 1e-06
THETA = 10000.0
MASKED = -1e30
SHARD = "shard"
SEQ = "seq"
MESH = pl.DeviceIdType.MESH


LANES = 128
STEP = 256
WIDE = 512
NARROW = 512
CHUNK = 512


def nn(left, right):
    return jnp.dot(left, right, preferred_element_type=jnp.float32)


def nt(left, right):
    return lax.dot_general(
        left, right, (((1,), (1,)), ((), ())), preferred_element_type=jnp.float32
    )


def tn(left, right):
    return lax.dot_general(
        left, right, (((0,), (0,)), ((), ())), preferred_element_type=jnp.float32
    )


def lane_index(rows):
    return lax.broadcasted_iota(jnp.int32, (rows, LANES), 1)


def turn(tile, cosine, sine):
    lane = lane_index(tile.shape[0])
    low = pltpu.roll(tile, LANES - ROPE // 2, 1)
    high = pltpu.roll(tile, ROPE // 2, 1)
    return tile * cosine + jnp.where(lane < ROPE // 2, low, high) * sine


def rope_lanes(positions):
    half = ROPE // 2
    frequency = THETA ** (-(2.0 * jnp.arange(half, dtype=jnp.float32)) / ROPE)
    angles = positions.astype(jnp.float32)[:, None] * frequency[None, :]
    cosine, sine = jnp.cos(angles), jnp.sin(angles)
    blank = jnp.zeros((positions.shape[0], LANES - ROPE), jnp.float32)
    return (
        jnp.concatenate([cosine, cosine, blank], 1),
        jnp.concatenate([-sine, sine, blank], 1),
    )


def split_heads(values, heads):
    width = NOPE + ROPE
    rows = values.shape[0]
    keep = lane_index(rows) < ROPE
    tiles = []
    for head in range(heads):
        part = values if head == 0 else pltpu.roll(values, (heads - head) * width, 1)
        if part.shape[1] >= 2 * LANES:
            turned = jnp.where(keep, part[:, NOPE : NOPE + LANES], 0.0)
        else:
            turned = jnp.concatenate(
                [part[:, NOPE:], jnp.zeros((rows, LANES - ROPE), part.dtype)], 1
            )
        tiles.append((part[:, :NOPE], turned))
    return tiles


def join_heads(tiles):
    heads = len(tiles)
    width = NOPE + ROPE
    if heads == 1:
        return jnp.concatenate([tiles[0][0], tiles[0][1][:, :ROPE]], 1)
    rows = tiles[0][0].shape[0]
    blank = jnp.zeros((rows, heads * width - 2 * LANES), jnp.float32)
    total = None
    for head, (plain, turned) in enumerate(tiles):
        part = jnp.concatenate([plain, turned, blank], 1)
        part = part if head == 0 else pltpu.roll(part, head * width, 1)
        total = part if total is None else total + part
    return total


def front_kernel(heads, count, shards, *refs):
    x_ref, gain_ref, lat_gain_ref, cos_ref, sin_ref, kvup_ref = refs[:6]
    query_refs = refs[6 : 6 + count]
    latent_refs = refs[6 + count : 6 + count + shards]
    first_ref, q_ref, k_ref, v_ref, latent_ref, low_ref = refs[6 + count + shards :]
    values = x_ref[...].astype(jnp.float32)
    inverse = lax.rsqrt(jnp.mean(values * values, -1, keepdims=True) + EPSILON)
    first = (values * inverse * gain_ref[...]).astype(jnp.bfloat16)
    first_ref[...] = first
    depth = query_refs[0].shape[0]
    query = None
    latent = None
    for r in range(count):
        term = nn(first[:, r * depth : (r + 1) * depth], query_refs[r][...])
        query = term if query is None else query + term
    depth = first.shape[1] // shards
    for r in range(shards):
        weight = latent_refs[r][...].reshape(depth, latent_refs[r].shape[2])
        term = nn(first[:, r * depth : (r + 1) * depth], weight)
        latent = term if latent is None else latent + term
    cosine, sine = cos_ref[...], sin_ref[...]
    for head, (plain, turned) in enumerate(split_heads(query, heads)):
        base = head * 2 * LANES
        q_ref[:, base : base + LANES] = plain.astype(jnp.bfloat16)
        q_ref[:, base + LANES : base + 2 * LANES] = turn(turned, cosine, sine).astype(
            jnp.bfloat16
        )
    packed = latent[:, :RANK]
    latent_ref[...] = packed
    inverse = lax.rsqrt(jnp.mean(packed * packed, -1, keepdims=True) + EPSILON)
    low = (packed * inverse * lat_gain_ref[...]).astype(jnp.bfloat16)
    low_ref[...] = low
    shared = jnp.where(
        lane_index(packed.shape[0]) < ROPE, latent[:, RANK : RANK + LANES], 0.0
    )
    shared = turn(shared, cosine, sine).astype(jnp.bfloat16)
    keyval = nn(low, kvup_ref[...]).astype(jnp.bfloat16)
    for head in range(heads):
        base = head * 2 * LANES
        k_ref[:, base : base + LANES] = keyval[:, base : base + NOPE]
        k_ref[:, base + LANES : base + 2 * LANES] = shared
        v_ref[:, head * VDIM : (head + 1) * VDIM] = keyval[:, base + NOPE : base + NOPE + VDIM]


def fixed(shape):
    return pl.BlockSpec(shape, lambda *_: (0,) * len(shape), pipeline_mode=pl.Buffered(1))


def by_rows(width, step=STEP):
    return pl.BlockSpec((step, width), lambda i: (i, 0))


def front(x, gain, lat_gain, cosine, sine, kvup, query_blocks, small, shards, heads):
    length, width = x.shape
    count = len(query_blocks)
    groups = small.shape[0]

    def latent_spec(r):
        return pl.BlockSpec(
            (groups, width // shards // groups, small.shape[2]),
            lambda *_: (0, r, 0),
            pipeline_mode=pl.Buffered(1),
        )

    shapes = [
        (width, jnp.bfloat16),
        (heads * 2 * LANES, jnp.bfloat16),
        (heads * 2 * LANES, jnp.bfloat16),
        (heads * VDIM, jnp.bfloat16),
        (RANK, jnp.float32),
        (RANK, jnp.bfloat16),
    ]
    return pl.pallas_call(
        functools.partial(front_kernel, heads, count, shards),
        grid=(length // STEP,),
        in_specs=[
            by_rows(width),
            fixed((1, width)),
            fixed((1, RANK)),
            by_rows(LANES),
            by_rows(LANES),
            fixed(kvup.shape),
        ]
        + [fixed(b.shape) for b in query_blocks]
        + [latent_spec(r) for r in range(shards)],
        out_specs=[by_rows(w) for w, _ in shapes],
        out_shape=[jax.ShapeDtypeStruct((length, w), d) for w, d in shapes],
        cost_estimate=pl.CostEstimate(
            flops=2 * length * width * 1100, bytes_accessed=20 * 2**20, transcendentals=0
        ),
        name="front",
    )(x, gain, lat_gain, cosine, sine, kvup, *query_blocks, *[small] * shards)


def causal(scores, span):
    row = lax.broadcasted_iota(jnp.int32, (STEP, STEP), 0)
    column = lax.broadcasted_iota(jnp.int32, (STEP, STEP), 1)
    edge = jnp.where(column <= row, scores[:, span - STEP :], MASKED)
    return edge if span == STEP else jnp.concatenate([scores[:, : span - STEP], edge], 1)


def attend_kernel(blocks, scale, q_ref, k_ref, v_ref, out_ref, log_ref):
    for block in range(blocks):

        @pl.when(pl.program_id(1) == block)
        def _(block=block):
            span = (block + 1) * STEP
            scores = causal(nt(q_ref[...], k_ref[:span]) * scale, span)
            top = jnp.max(scores, -1, keepdims=True)
            expo = jnp.exp(scores - top)
            total = jnp.sum(expo, -1, keepdims=True)
            low = (expo / total).astype(jnp.bfloat16)
            out_ref[...] = nn(low, v_ref[:span]).astype(jnp.bfloat16)
            log_ref[0] = top + jnp.log(total)


def attend(q, k, v, heads, scale):
    length = q.shape[0]
    blocks = length // STEP
    return pl.pallas_call(
        functools.partial(attend_kernel, blocks, scale),
        grid=(heads, blocks),
        in_specs=[
            pl.BlockSpec((STEP, 2 * LANES), lambda h, i: (i, h)),
            pl.BlockSpec((length, 2 * LANES), lambda h, i: (0, h)),
            pl.BlockSpec((length, VDIM), lambda h, i: (0, h)),
        ],
        out_specs=[
            pl.BlockSpec((STEP, VDIM), lambda h, i: (i, h)),
            pl.BlockSpec((1, STEP, 1), lambda h, i: (h, i, 0)),
        ],
        out_shape=[
            jax.ShapeDtypeStruct((length, heads * VDIM), jnp.bfloat16),
            jax.ShapeDtypeStruct((heads, length, 1), jnp.float32),
        ],
        cost_estimate=pl.CostEstimate(
            flops=2 * heads * length * length * 500,
            bytes_accessed=8 * 2**20,
            transcendentals=heads * length * length,
        ),
        name="attend",
    )(q, k, v)


def attend_back_kernel(heads, blocks, scale, *refs):
    q_ref, k_ref, v_ref, d_ref, log_ref, cos_ref, sin_ref, kvup_ref = refs[:8]
    query_refs = refs[8:-5]
    dq_ref, dkv_ref, part_ref, key_sum, value_sum = refs[-5:]
    block_id = pl.program_id(0)
    depth = query_refs[0].shape[0]
    width = depth * len(query_refs)

    @pl.when(block_id == 0)
    def _():
        key_sum[...] = jnp.zeros_like(key_sum)
        value_sum[...] = jnp.zeros_like(value_sum)

    for block in range(blocks):

        @pl.when(block_id == block)
        def _(block=block):
            span = (block + 1) * STEP
            tiles = []
            for head in range(heads):
                wide = slice(head * 2 * LANES, (head + 1) * 2 * LANES)
                thin = slice(head * VDIM, (head + 1) * VDIM)
                query = q_ref[:, wide]
                keys = k_ref[:span, wide]
                d_out = d_ref[:, thin]
                scores = causal(nt(query, keys) * scale, span)
                probs = jnp.exp(scores - log_ref[head])
                low = probs.astype(jnp.bfloat16)
                d_probs = nt(d_out, v_ref[:span, thin])
                centre = jnp.sum(probs * d_probs, -1, keepdims=True)
                d_scores = (probs * (d_probs - centre)).astype(jnp.bfloat16)
                d_query = nn(d_scores, keys) * scale
                key_sum[:span, wide] += tn(d_scores, query) * scale
                value_sum[:span, thin] += tn(low, d_out)
                tiles.append(
                    (
                        d_query[:, :NOPE],
                        turn(d_query[:, NOPE : NOPE + LANES], cos_ref[...], -sin_ref[...]),
                    )
                )
            dq_ref[...] = join_heads(tiles).astype(jnp.bfloat16)

    rows = pl.ds(pl.multiple_of(block_id * STEP, STEP), STEP)
    for r, query_ref in enumerate(query_refs):
        part_ref[rows, r * depth : (r + 1) * depth] = nt(dq_ref[...], query_ref[...]).astype(
            jnp.bfloat16
        )

    @pl.when(block_id == blocks - 1)
    def _():
        shared = None
        for head in range(heads):
            base = head * 2 * LANES
            dkv_ref[:, base : base + NOPE] = key_sum[:, base : base + NOPE].astype(jnp.bfloat16)
            dkv_ref[:, base + NOPE : base + NOPE + VDIM] = value_sum[
                :, head * VDIM : (head + 1) * VDIM
            ].astype(jnp.bfloat16)
            term = key_sum[:, base + LANES : base + 2 * LANES].astype(jnp.bfloat16)
            term = term.astype(jnp.float32)
            shared = term if shared is None else shared + term
        part_ref[:, width + RANK :] = shared.astype(jnp.bfloat16)
        part_ref[:, width : width + RANK] = nt(dkv_ref[...], kvup_ref[...]).astype(jnp.bfloat16)


def attend_back(q, k, v, d_heads, logs, cosine, sine, kvup, query_blocks, heads, scale):
    length = q.shape[0]
    part_width = query_blocks[0].shape[0] * len(query_blocks) + RANK + LANES
    blocks = length // STEP
    query_width = heads * (NOPE + ROPE)
    return pl.pallas_call(
        functools.partial(attend_back_kernel, heads, blocks, scale),
        grid=(blocks,),
        in_specs=[
            by_rows(heads * 2 * LANES),
            fixed(k.shape),
            fixed(v.shape),
            by_rows(heads * VDIM),
            pl.BlockSpec((heads, STEP, 1), lambda i: (0, i, 0)),
            by_rows(LANES),
            by_rows(LANES),
            fixed(kvup.shape),
        ]
        + [fixed(b.shape) for b in query_blocks],
        out_specs=[by_rows(query_width), fixed(k.shape), fixed((length, part_width))],
        out_shape=[
            jax.ShapeDtypeStruct((length, query_width), jnp.bfloat16),
            jax.ShapeDtypeStruct(k.shape, jnp.bfloat16),
            jax.ShapeDtypeStruct((length, part_width), jnp.bfloat16),
        ],
        scratch_shapes=[pltpu.VMEM(k.shape, jnp.float32), pltpu.VMEM(v.shape, jnp.float32)],
        cost_estimate=pl.CostEstimate(
            flops=2 * heads * length * length * 1100,
            bytes_accessed=12 * 2**20,
            transcendentals=heads * length * length,
        ),
        name="attend_back",
    )(q, k, v, d_heads, logs, cosine, sine, kvup, *query_blocks)


def load_pieces(pieces, sems):
    copies = [
        pltpu.make_async_copy(source, target, sems.at[at])
        for at, (source, target) in enumerate(pieces)
    ]

    @pl.when(pl.program_id(0) == 0)
    def _():
        for copy in copies:
            copy.start()

    def take(low, high):
        @pl.when(pl.program_id(0) == 0)
        def _():
            for copy in copies[low:high]:
                copy.wait()

    return take


def stacked(refs, whole, columns):
    size = refs[0].shape[1 if columns else 0]
    pieces = []
    for r, ref in enumerate(refs):
        span = pl.ds(r * size, size)
        pieces.append((ref, whole.at[:, span] if columns else whole.at[span]))
    return pieces


def minor_kernel(att_ref, branch_ref, low_ref, keyval_ref, query_ref, first_ref, *out_refs):
    shard = lax.axis_index(SHARD)
    depth = out_refs[0].shape[1]
    narrow = low_ref.shape[1] // len(out_refs)
    for r, out_ref in enumerate(out_refs):
        wide = slice(r * depth, (r + 1) * depth)
        place = pl.multiple_of(jnp.bitwise_xor(shard, r) * narrow, narrow)
        top = att_ref.shape[1]
        out_ref[:top] = tn(att_ref[...], branch_ref[:, wide]).astype(jnp.bfloat16)
        out_ref[top : top + narrow] = tn(
            low_ref[:, pl.ds(place, narrow)], keyval_ref[...]
        ).astype(jnp.bfloat16)
        out_ref[top + narrow :] = tn(query_ref[...], first_ref[:, wide]).astype(jnp.bfloat16)


def minor_grads(attended, branch, low, keyval, query, first, shards):
    depth = first.shape[1] // shards
    rows = attended.shape[1] + low.shape[1] // shards + query.shape[1]
    return pl.pallas_call(
        minor_kernel,
        in_specs=[pl.BlockSpec(memory_space=pltpu.VMEM)] * 6,
        out_specs=[pl.BlockSpec(memory_space=pltpu.VMEM)] * shards,
        out_shape=[jax.ShapeDtypeStruct((rows, depth), jnp.bfloat16)] * shards,
        cost_estimate=pl.CostEstimate(
            flops=2 * first.shape[0] * rows * first.shape[1],
            bytes_accessed=16 * 2**20,
            transcendentals=0,
        ),
        name="minor",
    )(attended, branch, low, keyval, query, first)


def hidden_kernel(count, ff, *refs):
    x_ref, gate_ref = refs[:2]
    sources = refs[2 : 2 + 2 * count]
    hid_ref, a_ref, b_ref, gates, ups, sems = refs[2 + 2 * count :]
    total = gates.shape[1]
    pieces = []
    for low in range(0, total, CHUNK):
        span = (slice(None), pl.ds(low, min(CHUNK, total - low)))
        for refs_in, whole in ((sources[:count], gates), (sources[count:], ups)):
            for source, target in stacked(refs_in, whole, False):
                pieces.append((source.at[span], target.at[span]))
    take = load_pieces(pieces, sems)
    x = x_ref[...]
    for low in range(0, total, CHUNK):
        high = min(low + CHUNK, total)
        take(low // CHUNK * 2 * count, (low // CHUNK + 1) * 2 * count)
        gate = nn(x, gates[:, low:high])
        upper = nn(x, ups[:, low:high])
        sigma = jax.nn.sigmoid(gate)
        silu = gate * sigma
        slope = upper * sigma * (1.0 + gate * (1.0 - sigma))
        factor = gate_ref[...]
        if high > ff:
            column = lax.broadcasted_iota(jnp.int32, gate.shape, 1)
            factor = jnp.where(column < ff - low, factor, 1.0)
        hid_ref[:, low:high] = (silu * upper * factor).astype(jnp.bfloat16)
        a_ref[:, low:high] = (slope * factor).astype(jnp.bfloat16)
        b_ref[:, low:high] = (silu * factor).astype(jnp.bfloat16)


def hidden_pass(x, gate, gate_blocks, up_blocks, ff):
    length, width = x.shape
    count = len(gate_blocks)
    blocks = [*gate_blocks, *up_blocks]
    total = gate_blocks[0].shape[1]
    return pl.pallas_call(
        functools.partial(hidden_kernel, count, ff),
        grid=(length // WIDE,),
        in_specs=[by_rows(width, WIDE), by_rows(1, WIDE)]
        + [pl.BlockSpec(memory_space=pl.ANY)] * len(blocks),
        out_specs=[by_rows(total, WIDE)] * 3,
        out_shape=[jax.ShapeDtypeStruct((length, total), jnp.bfloat16)] * 3,
        scratch_shapes=[pltpu.VMEM((width, total), jnp.bfloat16)] * 2
        + [pltpu.SemaphoreType.DMA((2 * count * -(-total // CHUNK),))],
        cost_estimate=pl.CostEstimate(
            flops=4 * length * width * total, bytes_accessed=32 * 2**20, transcendentals=0
        ),
        compiler_params=pltpu.CompilerParams(vmem_limit_bytes=60 * 2**20),
        name="hidden_pass",
    )(x, gate, *blocks)


def slope_kernel(count, *refs):
    g_ref, a_ref, b_ref = refs[:3]
    sources = refs[3 : 3 + 3 * count]
    dg_ref, du_ref, part_ref, downs, gates, ups, sems = refs[3 + 3 * count :]
    total = downs.shape[0]
    pieces = stacked(sources[:count], downs, True)
    first = len(pieces)
    pieces += stacked(sources[count : 2 * count], gates, False)
    pieces += stacked(sources[2 * count :], ups, False)
    take = load_pieces(pieces, sems)
    take(0, first)
    g = g_ref[...]
    for low in range(0, total, CHUNK):
        high = min(low + CHUNK, total)
        d_hidden = nt(g, downs[low:high])
        dg_ref[:, low:high] = (d_hidden * a_ref[:, low:high].astype(jnp.float32)).astype(
            jnp.bfloat16
        )
        du_ref[:, low:high] = (d_hidden * b_ref[:, low:high].astype(jnp.float32)).astype(
            jnp.bfloat16
        )
    take(first, len(pieces))
    d_gate, d_up = dg_ref[...], du_ref[...]
    width = g.shape[1]
    for low in range(0, width, CHUNK):
        high = min(low + CHUNK, width)
        part_ref[:, low:high] = (nt(d_gate, gates[low:high]) + nt(d_up, ups[low:high])).astype(
            jnp.bfloat16
        )


def slope_pass(g, a, b, down_blocks, gate_blocks, up_blocks):
    length, width = g.shape
    count = len(gate_blocks)
    blocks = [*down_blocks, *gate_blocks, *up_blocks]
    total = gate_blocks[0].shape[1]
    return pl.pallas_call(
        functools.partial(slope_kernel, count),
        grid=(length // NARROW,),
        in_specs=[by_rows(width, NARROW), by_rows(total, NARROW), by_rows(total, NARROW)]
        + [pl.BlockSpec(memory_space=pl.ANY)] * len(blocks),
        out_specs=[by_rows(total, NARROW), by_rows(total, NARROW), by_rows(width, NARROW)],
        out_shape=[
            jax.ShapeDtypeStruct((length, total), jnp.bfloat16),
            jax.ShapeDtypeStruct((length, total), jnp.bfloat16),
            jax.ShapeDtypeStruct((length, width), jnp.bfloat16),
        ],
        scratch_shapes=[
            pltpu.VMEM((total, width), jnp.bfloat16),
            pltpu.VMEM((width, total), jnp.bfloat16),
            pltpu.VMEM((width, total), jnp.bfloat16),
            pltpu.SemaphoreType.DMA((3 * count,)),
        ],
        cost_estimate=pl.CostEstimate(
            flops=6 * length * width * total, bytes_accessed=40 * 2**20, transcendentals=0
        ),
        compiler_params=pltpu.CompilerParams(vmem_limit_bytes=62 * 2**20),
        name="slope_pass",
    )(g, a, b, *blocks)


def rotate(values, cosine, sine):
    half_depth = values.shape[-1] // 2
    first = values[..., :half_depth]
    second = values[..., half_depth:]
    return jnp.concatenate([first * cosine - second * sine, second * cosine + first * sine], -1)


def norm_forward(values, scaling):
    inverse = lax.rsqrt(jnp.mean(values * values, -1, keepdims=True) + EPSILON)
    return (values * inverse * scaling, inverse)


def norm_backward(values, inverse, scaling, upstream):
    weighted = upstream * scaling
    scaling_grad = jnp.sum(upstream * values * inverse, 0)
    centre = jnp.mean(weighted * values, -1, keepdims=True)
    return (inverse * weighted - values * inverse**3 * centre, scaling_grad)


def gather_seq(block):
    return lax.all_gather(block, SEQ, axis=0, tiled=True)


def scatter_seq(partial):
    return lax.psum_scatter(
        partial.astype(jnp.bfloat16), SEQ, scatter_dimension=0, tiled=True
    ).astype(jnp.float32)


def settle_kernel(n, shards, terms_ref, out_ref, from_seq, joined, from_shard, sends, seq_recv, shard_recv):
    me = lax.axis_index(SEQ)
    my_shard = lax.axis_index(SHARD)
    barrier = pltpu.get_barrier_semaphore()
    for hop in range(1, n):
        pl.semaphore_signal(
            barrier, inc=1, device_id={SEQ: (me + hop) % n}, device_id_type=MESH
        )
    for hop in range(1, shards):
        pl.semaphore_signal(
            barrier, inc=1, device_id={SHARD: (my_shard + hop) % shards}, device_id_type=MESH
        )
    pl.semaphore_wait(barrier, n + shards - 2)
    first = []
    for hop in range(1, n):
        target = (me + hop) % n
        copy = pltpu.make_async_remote_copy(
            src_ref=terms_ref.at[:, target],
            dst_ref=from_seq.at[hop - 1],
            send_sem=sends.at[hop - 1],
            recv_sem=seq_recv.at[hop - 1],
            device_id={SEQ: target},
            device_id_type=MESH,
        )
        copy.start()
        first.append(copy)
    total = terms_ref[:, me]
    for hop in range(1, n):
        first[hop - 1].wait_recv()
        total = total + from_seq[hop - 1]
    joined[...] = total
    second = []
    for hop in range(1, shards):
        target = (my_shard + hop) % shards
        place = target
        if shards == 4:
            low, high = my_shard % 2, my_shard // 2
            low = low + hop % 2 - 2 * low * (hop % 2)
            high = high + hop // 2 - 2 * high * (hop // 2)
            target, place = 2 * high + low, hop
        copy = pltpu.make_async_remote_copy(
            src_ref=joined.at[place],
            dst_ref=from_shard.at[hop - 1],
            send_sem=sends.at[n - 1 + hop - 1],
            recv_sem=shard_recv.at[hop - 1],
            device_id={SHARD: target},
            device_id_type=MESH,
        )
        copy.start()
        second.append(copy)
    total = joined[0 if shards == 4 else my_shard]
    for hop in range(1, shards):
        second[hop - 1].wait_recv()
        total = total + from_shard[hop - 1]
    out_ref[...] = total
    for copy in first + second:
        copy.wait_send()


def settle(n, shards, terms, identity):
    shape = terms.shape[2:]
    return pl.pallas_call(
        functools.partial(settle_kernel, n, shards),
        out_shape=jax.ShapeDtypeStruct(shape, jnp.float32),
        in_specs=[pl.BlockSpec(memory_space=pltpu.VMEM)],
        out_specs=pl.BlockSpec(memory_space=pltpu.VMEM),
        scratch_shapes=[
            pltpu.VMEM((n - 1, shards) + shape, jnp.float32),
            pltpu.VMEM((shards,) + shape, jnp.float32),
            pltpu.VMEM((shards - 1,) + shape, jnp.float32),
            pltpu.SemaphoreType.DMA((n + shards - 2,)),
            pltpu.SemaphoreType.DMA((n - 1,)),
            pltpu.SemaphoreType.DMA((shards - 1,)),
        ],
        compiler_params=pltpu.CompilerParams(collective_id=identity, has_side_effects=True),
        name="settle",
    )(terms)


def duplex_kernel(n, parts, sums, *refs):
    if sums:
        (x_ref, part_ref, all_ref, sum_ref, mine, other, left_in, right_in) = refs[:8]
        (pair_send, pair_recv, line_send, line_recv) = refs[8:12]
    else:
        x_ref, all_ref = refs[:2]
    copy_send, copy_recv, local = refs[-3:]
    half = n // 2
    me = lax.axis_index(SEQ)
    core = me % 2
    place = me // 2
    partner = place * 2 + 1 - core
    below, above = me - 2, me + 2
    has_below, has_above = place > 0, place < half - 1

    def remote(source, target, send, recv, device):
        return pltpu.make_async_remote_copy(
            src_ref=source,
            dst_ref=target,
            send_sem=send,
            recv_sem=recv,
            device_id={SEQ: device},
            device_id_type=MESH,
        )

    def pair_copy(at):
        return remote(
            part_ref.at[at * 2 + 1 - core], other.at[at], pair_send.at[at], pair_recv.at[at], partner
        )

    piece = x_ref.shape[0] // parts

    def rows_of(part):
        return pl.ds(part * piece, piece)

    def sum_up(at, part):
        span = rows_of(part)
        return remote(
            mine.at[at, span],
            left_in.at[at, span],
            line_send.at[0, at, part],
            line_recv.at[0, at, part],
            above,
        )

    def sum_down(at, part):
        span = rows_of(part)
        return remote(
            mine.at[at, span],
            right_in.at[at, span],
            line_send.at[1, at, part],
            line_recv.at[1, at, part],
            below,
        )

    def block_copy(source, block, way, step, part, device):
        span = rows_of(part)
        return remote(
            source.at[span],
            all_ref.at[block, span],
            copy_send.at[way, step, part],
            copy_recv.at[way, step, part],
            device,
        )

    order = []
    for at in range(half):
        for item in (half - 1 - at, at):
            if item not in order:
                order.append(item)
    for at in order if sums else ():
        pltpu.make_async_copy(part_ref.at[at * 2 + core], mine.at[at], local.at[at]).start()
    keep = pltpu.make_async_copy(x_ref, all_ref.at[me], local.at[half])
    keep.start()

    barrier = pltpu.get_barrier_semaphore()
    pl.semaphore_signal(barrier, inc=1, device_id={SEQ: partner}, device_id_type=MESH)

    @pl.when(has_below)
    def _():
        pl.semaphore_signal(barrier, inc=1, device_id={SEQ: below}, device_id_type=MESH)

    @pl.when(has_above)
    def _():
        pl.semaphore_signal(barrier, inc=1, device_id={SEQ: above}, device_id_type=MESH)

    @pl.when(has_below & has_above)
    def _():
        pl.semaphore_wait(barrier, 3)

    @pl.when(jnp.logical_not(has_below & has_above))
    def _():
        pl.semaphore_wait(barrier, 2)

    for at in order if sums else ():
        pair_copy(at).start()

    for part in range(parts):

        @pl.when(has_above)
        def _():
            block_copy(x_ref, me, 0, 0, part, above).start()

        @pl.when(has_below)
        def _():
            block_copy(x_ref, me, 1, 0, part, below).start()

        block_copy(x_ref, me, 2, 0, part, partner).start()

    def merge(at, part, incoming):
        span = rows_of(part)
        total = mine[at, span].astype(jnp.float32) + other[at, span].astype(jnp.float32)
        if incoming is not None:
            total = total + incoming[at, span].astype(jnp.float32)
        mine[at, span] = total.astype(mine.dtype)

    def load(at):
        return pltpu.make_async_copy(part_ref.at[at * 2 + core], mine.at[at], local.at[at])

    def ready(at):
        load(at).wait()
        pair_copy(at).wait_recv()

    def relay(slot, part):
        step = slot - 1

        @pl.when(place > step)
        def _():
            block = me - 2 * (step + 1)
            block_copy(x_ref, block, 0, step, part, above).wait_recv()

            @pl.when(has_above)
            def _():
                block_copy(all_ref.at[block], block, 0, step + 1, part, above).start()

            block_copy(all_ref.at[block], block, 2, 1 + step, part, partner).start()

        @pl.when(place < half - 1 - step)
        def _():
            block = me + 2 * (step + 1)
            block_copy(x_ref, block, 1, step, part, below).wait_recv()

            @pl.when(has_below)
            def _():
                block_copy(all_ref.at[block], block, 1, step + 1, part, below).start()

            block_copy(all_ref.at[block], block, 2, half + step, part, partner).start()

    for slot in range(2 * half - 2):
        rise = half - 1 - (slot - place)
        fall = slot - (half - 1 - place)
        if 1 <= slot <= half - 1:
            for part in range(parts):
                relay(slot, part)
        if not sums:
            continue

        @pl.when((rise < half) & (rise > place))
        def _():
            ready(rise)
            for part in range(parts):

                @pl.when(has_below)
                def _():
                    sum_up(rise, part).wait_recv()
                    merge(rise, part, left_in)

                @pl.when(jnp.logical_not(has_below))
                def _():
                    merge(rise, part, None)

                sum_up(rise, part).start()

        @pl.when((fall >= 0) & (fall < place))
        def _():
            ready(fall)
            for part in range(parts):

                @pl.when(has_above)
                def _():
                    sum_down(fall, part).wait_recv()
                    merge(fall, part, right_in)

                @pl.when(jnp.logical_not(has_above))
                def _():
                    merge(fall, part, None)

                sum_down(fall, part).start()

    if sums:
        ready(place)
        for part in range(parts):

            @pl.when(has_below)
            def _():
                sum_up(place, part).wait_recv()

            @pl.when(has_above)
            def _():
                sum_down(place, part).wait_recv()

        total = mine[place].astype(jnp.float32) + other[place].astype(jnp.float32)
        low = jnp.where(has_below, left_in[place].astype(jnp.float32), 0.0)
        high = jnp.where(has_above, right_in[place].astype(jnp.float32), 0.0)
        sum_ref[...] = total + low + high

    keep.wait()
    for at in range(half if sums else 0):
        pair_copy(at).wait_send()
    for part in range(parts):
        block_copy(x_ref, partner, 2, 0, part, partner).wait_recv()
        block_copy(x_ref, me, 2, 0, part, partner).wait_send()

        @pl.when(has_above)
        def _():
            block_copy(x_ref, me, 0, 0, part, above).wait_send()

        @pl.when(has_below)
        def _():
            block_copy(x_ref, me, 1, 0, part, below).wait_send()

        for step in range(half - 1):
            up, down = half - 1 - step, step
            if sums:

                @pl.when(place < up)
                def _():
                    sum_up(up, part).wait_send()

                @pl.when(place > down)
                def _():
                    sum_down(down, part).wait_send()

            @pl.when(place > step)
            def _():
                block = me - 2 * (step + 1)

                @pl.when(has_above)
                def _():
                    block_copy(x_ref, block, 0, step + 1, part, above).wait_send()

                block_copy(x_ref, block, 2, 1 + step, part, partner).wait_send()
                there = partner - 2 * (step + 1)
                block_copy(x_ref, there, 2, 1 + step, part, partner).wait_recv()

            @pl.when(place < half - 1 - step)
            def _():
                block = me + 2 * (step + 1)

                @pl.when(has_below)
                def _():
                    block_copy(x_ref, block, 1, step + 1, part, below).wait_send()

                block_copy(x_ref, block, 2, half + step, part, partner).wait_send()
                there = partner + 2 * (step + 1)
                block_copy(x_ref, there, 2, half + step, part, partner).wait_recv()


def duplex(n, block, partial, identity, parts=2):
    half = n // 2
    rows, wide = partial.shape[0] // n, partial.shape[1]
    line = pltpu.VMEM((half, rows, wide), partial.dtype)
    gathered, total = pl.pallas_call(
        functools.partial(duplex_kernel, n, parts, True),
        out_shape=[
            jax.ShapeDtypeStruct((n,) + block.shape, block.dtype),
            jax.ShapeDtypeStruct((rows, wide), jnp.float32),
        ],
        in_specs=[
            pl.BlockSpec(memory_space=pltpu.VMEM),
            pl.BlockSpec(memory_space=pl.ANY),
        ],
        out_specs=[
            pl.BlockSpec(memory_space=pl.ANY),
            pl.BlockSpec(memory_space=pltpu.VMEM),
        ],
        scratch_shapes=[
            line,
            line,
            line,
            line,
            pltpu.SemaphoreType.DMA((half,)),
            pltpu.SemaphoreType.DMA((half,)),
            pltpu.SemaphoreType.DMA((2, half, parts)),
            pltpu.SemaphoreType.DMA((2, half, parts)),
            pltpu.SemaphoreType.DMA((3, 2 * half, parts)),
            pltpu.SemaphoreType.DMA((3, 2 * half, parts)),
            pltpu.SemaphoreType.DMA((half + 1,)),
        ],
        compiler_params=pltpu.CompilerParams(collective_id=identity, has_side_effects=True),
        cost_estimate=pl.CostEstimate(
            flops=45_000_000_000, bytes_accessed=2**24, transcendentals=0
        ),
        name="duplex",
    )(block, partial.reshape(n, rows, wide))
    return gathered.reshape(n * block.shape[0], block.shape[1]), total


def chain_gather(n, block, identity, parts=2):
    half = n // 2
    return pl.pallas_call(
        functools.partial(duplex_kernel, n, parts, False),
        out_shape=jax.ShapeDtypeStruct((n,) + block.shape, block.dtype),
        in_specs=[pl.BlockSpec(memory_space=pltpu.VMEM)],
        out_specs=pl.BlockSpec(memory_space=pl.ANY),
        scratch_shapes=[
            pltpu.SemaphoreType.DMA((3, 2 * half, parts)),
            pltpu.SemaphoreType.DMA((3, 2 * half, parts)),
            pltpu.SemaphoreType.DMA((half + 1,)),
        ],
        compiler_params=pltpu.CompilerParams(collective_id=identity, has_side_effects=True),
        cost_estimate=pl.CostEstimate(
            flops=25_000_000_000, bytes_accessed=2**22, transcendentals=0
        ),
        name="chain",
    )(block)


ACROSS = ([(0, 1), (1, 0), (2, 3), (3, 2)], [(0, 2), (2, 0), (1, 3), (3, 1)])


def swap_with(block, side):
    return lax.ppermute(block, SHARD, ACROSS[side])


def gather_blocks(weight, axis, side):
    if lax.axis_size(SHARD) != 4:
        return [lax.all_gather(weight, SHARD, axis=axis, tiled=True)]
    return gather_far(gather_near(weight, axis), side)


def gather_near(weight, axis):
    if lax.axis_size(SHARD) != 4:
        return [lax.all_gather(weight, SHARD, axis=axis, tiled=True)]
    return [weight, swap_with(weight, 0), swap_with(weight, 1)]


def gather_far(blocks, side, token=None):
    if len(blocks) == 1:
        return blocks
    relay = blocks[1 + side]
    relay = relay if token is None else after(relay, token)
    return [*blocks, swap_with(relay, 1 - side)]


def after(value, token):
    return lax.optimization_barrier((value, token))[0]


def scatter_blocks(blocks, axis, side, join_token, sum_token, one_token=None):
    if lax.axis_size(SHARD) != 4:
        blocks = [block.astype(jnp.bfloat16) for block in blocks]
        return (lax.psum_scatter(blocks[0], SHARD, scatter_dimension=axis, tiled=True),)
    blocks = [lax.optimization_barrier(block.astype(jnp.bfloat16)) for block in blocks]
    far = swap_with(blocks[3], side)
    one = blocks[1 + side] if one_token is None else after(blocks[1 + side], one_token)
    first = swap_with(one, side)
    far = after(far, join_token)
    joined = (blocks[2 - side].astype(jnp.float32) + far.astype(jnp.float32)).astype(
        jnp.bfloat16
    )
    second = swap_with(joined, 1 - side)
    second = after(second, sum_token)
    return blocks[0], first, second


def add_up(terms, rows=slice(None), columns=slice(None)):
    total = None
    for term in terms:
        term = term[rows, columns].astype(jnp.float32)
        total = term if total is None else total + term
    return total


def local_order(values, axis):
    if lax.axis_size(SHARD) != 4:
        return values
    size = values.shape[axis] // 4
    shard = lax.axis_index(SHARD)
    return jnp.concatenate(
        [
            lax.dynamic_slice_in_dim(values, jnp.bitwise_xor(shard, place) * size, size, axis)
            for place in range(4)
        ],
        axis,
    )


def cut(values, axis):
    if lax.axis_size(SHARD) != 4:
        return [values]
    size = values.shape[axis] // 4
    return [lax.slice_in_dim(values, r * size, (r + 1) * size, axis=axis) for r in range(4)]


def on_device(
    inputs,
    attn_gain,
    query_project_weight,
    latent_project_weight,
    latent_gain,
    latent_keyval_weight,
    attention_output_weight,
    ffn_gain,
    shared_gate,
    shared_up,
    shared_down,
    expert_gate,
    expert_up,
    expert_down,
    routes,
    slots,
    gates,
    cotangent,
):
    tok_rows = inputs.shape[1]
    model_width = inputs.shape[2]
    groups = lax.axis_size(SEQ)
    shards = lax.axis_size(SHARD)
    me = lax.axis_index(SEQ)
    heads = HEADS // groups
    experts = EXP_DEV * groups
    capacity = 9 * tok_rows * TOPK // (8 * experts)
    length = tok_rows * groups
    score_scale = (NOPE + ROPE) ** (-0.5)
    own_start = me * tok_rows
    one_width = attn_gain.shape[0]
    lat_width = latent_gain.shape[0]
    ff = expert_gate.shape[2]
    shared_ff = shared_gate.shape[1]
    side = -(-shared_ff // LANES) * LANES

    own_inputs = local_order(inputs.reshape(tok_rows, model_width), 1)
    inputs_all = gather_seq(own_inputs)
    upstream = local_order(cotangent.reshape(tok_rows, model_width), 1)
    route_rows = routes.reshape(tok_rows, TOPK)
    slot_rows = slots.reshape(tok_rows, TOPK)
    kept = (route_rows.T[:, None, :] == jnp.arange(experts)[None, :, None]) & (
        slot_rows.T < capacity
    )[:, None, :]
    gate_table = jnp.sum(
        jnp.where(kept, gates.reshape(tok_rows, TOPK).T.astype(jnp.float32)[:, None, :], 0.0), 0
    ).astype(jnp.bfloat16)

    def padded_row(gain):
        return jnp.pad(gain, (0, LANES - ROPE - gain.shape[0]))[None]

    side_rows = jnp.concatenate(
        [
            padded_row(attn_gain),
            padded_row(ffn_gain),
            padded_row(latent_gain),
            jnp.zeros((one_width - 3, LANES - ROPE), jnp.bfloat16),
        ],
        0,
    )
    small_own = jnp.concatenate([latent_project_weight, side_rows], 1)
    small_rows = jnp.concatenate(gather_blocks(small_own, 0, 0), 0)
    small_rows = jnp.concatenate(
        [
            small_rows,
            jnp.pad(gate_table, ((0, EXTRA - experts), (0, small_rows.shape[1] - tok_rows))),
        ],
        0,
    )
    small_seq = chain_gather(groups, small_rows, 4)
    gate_column = (
        lax.dynamic_index_in_dim(
            small_seq[:, shards * one_width :, :tok_rows], me, 1, keepdims=False
        )
        .reshape(length, 1)
        .astype(jnp.float32)
    )
    gain_rows = (
        small_seq[:, : shards * one_width, RANK + ROPE :]
        .reshape(groups, shards, one_width, -1)[:, :, :3]
        .astype(jnp.float32)
        .transpose(2, 1, 0, 3)
    )
    first_norm_weight = gain_rows[0, :, :, :one_width].reshape(-1)
    second_norm_weight = gain_rows[1, :, :, :one_width].reshape(-1)
    latent_norm_weight = local_order(gain_rows[2, :, :, :lat_width].reshape(-1), 0)

    spare = side - shared_ff
    gate_own = jnp.pad(
        jnp.concatenate([expert_gate[0], shared_gate], 1), ((0, 0), (0, spare))
    )
    up_own = jnp.pad(jnp.concatenate([expert_up[0], shared_up], 1), ((0, 0), (0, spare)))
    down_own = jnp.pad(jnp.concatenate([expert_down[0], shared_down], 0), ((0, spare), (0, 0)))
    query_blocks = gather_blocks(query_project_weight, 0, 0)
    kvup_blocks = gather_blocks(latent_keyval_weight, 0, 0)
    out_blocks = gather_blocks(attention_output_weight, 1, 0)
    gate_near = gather_near(gate_own, 0)
    up_near = gather_near(up_own, 0)
    down_near = gather_near(down_own, 1)
    full_kvup = local_order(jnp.concatenate(kvup_blocks, 0), 0)
    full_out = jnp.concatenate(out_blocks, 1)

    residual_stream = own_inputs.astype(jnp.float32)
    cosine, sine = rope_lanes(jnp.arange(length))
    first_all, q_all, k_all, v_all, latent, latent_all = front(
        inputs_all,
        first_norm_weight[None],
        latent_norm_weight[None],
        cosine,
        sine,
        full_kvup,
        query_blocks,
        small_seq,
        shards,
        heads,
    )
    gate_blocks = gather_far(gate_near, 0, q_all)
    up_blocks = gather_far(up_near, 1, q_all)
    down_blocks = gather_far(down_near, 1)
    attended, logs = attend(q_all, k_all, v_all, heads, score_scale)
    attended_part = nn(attended, full_out)
    upstream_all, attended_sum = duplex(groups, upstream, attended_part.astype(jnp.bfloat16), 1)
    middle = residual_stream + attended_sum
    normed_two, inv_two = norm_forward(middle, second_norm_weight)
    second_all = chain_gather(groups, normed_two.astype(jnp.bfloat16), 5)
    second_all = second_all.reshape(length, model_width)

    hidden, slope_gate, slope_up = hidden_pass(second_all, gate_column, gate_blocks, up_blocks, ff)
    d_gate, d_up, second_part = slope_pass(
        upstream_all, slope_gate, slope_up, down_blocks, gate_blocks, up_blocks
    )
    d_second = scatter_seq(second_part)
    hidden_late = after(hidden, d_gate)
    d_down = [tn(hidden_late, part) for part in cut(upstream_all, 1)[1:]]
    second_parts = cut(second_all, 1)
    count = len(second_parts)
    d_wgate = [tn(part, d_gate) for part in second_parts[1:]]
    d_wup = [tn(part, d_up) for part in second_parts[2:]]
    down_part = nn(hidden, jnp.concatenate(down_blocks, 1)).astype(jnp.bfloat16)

    d_middle_norm, d_gain_two = norm_backward(middle, inv_two, second_norm_weight, d_second)
    d_middle = upstream.astype(jnp.float32) + d_middle_norm
    d_branch_all, added = duplex(groups, d_middle.astype(jnp.bfloat16), down_part, 2)
    output = local_order((middle + added).astype(jnp.bfloat16), 1).reshape(1, tok_rows, model_width)
    d_heads = nt(d_branch_all, full_out).astype(jnp.bfloat16)
    d_query, d_keyval, back_part = attend_back(
        q_all,
        k_all,
        v_all,
        d_heads,
        logs,
        cosine,
        sine,
        full_kvup,
        query_blocks,
        heads,
        score_scale,
    )
    back_sum = scatter_seq(back_part)
    first_back, latent_back = back_sum[:, :model_width], back_sum[:, model_width:]
    if shards == 4:
        d_minor = minor_grads(
            attended, d_branch_all, latent_all, d_keyval, d_query, first_all, shards
        )
    else:
        d_wout = [tn(attended, part).astype(jnp.bfloat16) for part in cut(d_branch_all, 1)]
        d_wquery = [tn(part, d_query).astype(jnp.bfloat16) for part in cut(first_all, 1)]
        d_wkvup = cut(local_order(tn(latent_all, d_keyval).astype(jnp.bfloat16), 0), 0)

    own_latent = lax.dynamic_slice_in_dim(latent, own_start, tok_rows, 0)
    half = ROPE // 2
    cos_own = lax.dynamic_slice_in_dim(cosine, own_start, tok_rows, 0)[:, :half]
    sin_own = lax.dynamic_slice_in_dim(sine, own_start, tok_rows, 0)[:, half:ROPE]
    inv_latent = norm_forward(own_latent, latent_norm_weight)[1]
    d_rope = rotate(latent_back[:, RANK : RANK + ROPE], cos_own, -sin_own)
    d_compressed, d_gain_latent = norm_backward(
        own_latent, inv_latent, latent_norm_weight, latent_back[:, :RANK]
    )
    d_latent = jnp.concatenate(
        [d_compressed, d_rope, jnp.zeros((tok_rows, LANES - ROPE), jnp.float32)], -1
    ).astype(jnp.bfloat16)
    d_latent_all = gather_seq(d_latent)
    inv_one = norm_forward(residual_stream, first_norm_weight)[1]
    wide_latent = jnp.concatenate(
        [
            small_seq[:, r * one_width : (r + 1) * one_width].reshape(groups * one_width, -1)
            for r in range(shards)
        ],
        0,
    )
    d_first = first_back + nt(d_latent, wide_latent)
    d_resid, d_gain_one = norm_backward(residual_stream, inv_one, first_norm_weight, d_first)
    input_grad = local_order(after(d_middle, output) + d_resid, 1).reshape(1, tok_rows, model_width)
    first_late = after(first_all, d_latent)
    own_columns = jnp.concatenate(
        [
            lax.dynamic_slice_in_dim(
                first_late, (place * groups + me) * one_width, one_width, 1
            )
            for place in range(shards)
        ],
        1,
    )
    d_wlatent = cut(tn(own_columns, d_latent_all).astype(jnp.bfloat16), 0)

    terms = jnp.concatenate(
        [
            d_gain_one.reshape(shards, groups, one_width),
            d_gain_two.reshape(shards, groups, one_width),
            local_order(d_gain_latent, 0).reshape(shards, groups, lat_width),
        ],
        2,
    )
    terms = jnp.pad(terms, ((0, 0), (0, 0), (0, 1024 - terms.shape[2])))
    terms = terms.reshape(shards, groups, 8, 128)
    gain_grads = settle(groups, shards, terms, 9).reshape(-1)
    d_down.insert(0, tn(hidden, cut(after(upstream_all, d_keyval), 1)[0]))
    second_late = cut(after(second_all, d_keyval), 1)
    d_wgate.insert(0, tn(second_late[0], d_gate))
    d_wup = [tn(part, d_up) for part in second_late[: count - len(d_wup)]] + d_wup
    gate_grad = scatter_blocks(d_wgate, 0, 0, d_keyval, d_wlatent[0])
    up_grad = scatter_blocks(d_wup, 0, 1, d_keyval, d_wlatent[0])
    down_grad = scatter_blocks(d_down, 1, 0, second_part, d_wgate[0])
    if shards == 4:
        minor = scatter_blocks(d_minor, 0, 1, gain_grads, d_wlatent[0], gain_grads)
        top, narrow = attended.shape[1], RANK // shards
        out_grad = add_up(minor, rows=slice(0, top))
        kvup_grad = add_up(minor, rows=slice(top, top + narrow))
        query_grad = add_up(minor, rows=slice(top + narrow, None)).T
    else:
        out_grad = add_up(scatter_blocks(d_wout, 1, 1, gain_grads, d_wlatent[0]))
        kvup_grad = add_up(scatter_blocks(d_wkvup, 0, 1, gain_grads, d_wlatent[0]))
        query_grad = add_up(scatter_blocks(d_wquery, 0, 1, gain_grads, d_wlatent[0]))
    latent_grad = scatter_blocks(d_wlatent, 0, 1, first_back, first_back)
    return (
        output,
        input_grad,
        gain_grads[:one_width],
        query_grad,
        add_up(latent_grad, columns=slice(0, RANK + ROPE)),
        gain_grads[2 * one_width : 2 * one_width + lat_width],
        kvup_grad,
        out_grad,
        gain_grads[one_width : 2 * one_width],
        add_up(gate_grad, columns=slice(ff, ff + shared_ff)),
        add_up(up_grad, columns=slice(ff, ff + shared_ff)),
        add_up(down_grad, rows=slice(ff, ff + shared_ff)),
        add_up(gate_grad, columns=slice(0, ff))[None],
        add_up(up_grad, columns=slice(0, ff))[None],
        add_up(down_grad, rows=slice(0, ff))[None],
    )


def solution(mesh):
    in_specs = (
        P(SHARD, SEQ, None),
        P((SHARD, SEQ)),
        P(SHARD, SEQ),
        P((SHARD, SEQ), None),
        P((SHARD, SEQ)),
        P(SHARD, SEQ),
        P(SEQ, SHARD),
        P((SHARD, SEQ)),
        P(SHARD, SEQ),
        P(SHARD, SEQ),
        P(SEQ, SHARD),
        P(SEQ, SHARD, None),
        P(SEQ, SHARD, None),
        P(SEQ, None, SHARD),
        P(SHARD, SEQ, None),
        P(SHARD, SEQ, None),
        P(SHARD, SEQ, None),
        P(SHARD, SEQ, None),
    )
    out_specs = (
        P(SHARD, SEQ, None),
        P(SHARD, SEQ, None),
        P((SHARD, SEQ)),
        P(SHARD, SEQ),
        P((SHARD, SEQ), None),
        P((SHARD, SEQ)),
        P(SHARD, SEQ),
        P(SEQ, SHARD),
        P((SHARD, SEQ)),
        P(SHARD, SEQ),
        P(SHARD, SEQ),
        P(SEQ, SHARD),
        P(SEQ, SHARD, None),
        P(SEQ, SHARD, None),
        P(SEQ, None, SHARD),
    )

    return jax.shard_map(
        on_device, mesh=mesh, in_specs=in_specs, out_specs=out_specs, check_vma=False
    )
```
